32 devices in a mesh: tm: 16 (over z, x, core), space: 2 (over y).
Axes of the slice: x: 2, y: 2, z: 4, core: 2. Of those that a mesh axis runs over, the one named last changes fastest.
Arguments:
- fine_nodes: float32 [16, 3, 3, 32, 4096], P('tm', None, None, 'space'), may hold values from -6 to 6
- init_state: float32 [3, 32, 4096], P(None, 'space'), may hold values from -6 to 6
- mean_depth: float32 [32, 4096], P('space'), may hold values from 0.5 to 2
Outputs:
- new_nodes: float32 [16, 3, 3, 32, 4096], P('tm', None, None, 'space')
The draws below stay inside these ranges and needn't reach their ends.
All inputs are finite; a program needn't handle non-finite values.
Results may differ from the reference program's by a relative error of at most 0.00002.
Values sent between devices are 32-bit elements; how exact they have to be, the bound alone decides.
No kernel may reach another device: no remote copies, remote signals or barrier semaphores. Data moves between devices by JAX's collectives and lax.ppermute only.
A program may use at most 64 MiB of HBM per device.

```python
import math
import jax
import jax.numpy as jnp
from jax import lax

NX = 4096
NODES = 3
FIELDS = 3
NY = 32
SLICES = 16


def steps_of(rng, shape, pieces, least, largest):
    level, own = 1.0, jax.random.fold_in(rng, 6)
    for position, parts in pieces:
        heights = jnp.exp(jax.random.uniform(jax.random.fold_in(own, position), (parts,), jnp.float32, least / len(pieces), largest / len(pieces)))
        level = level * jnp.repeat(heights, shape[position] // parts).reshape([-1 if axis == position else 1 for axis in range(len(shape))])
    return level


def noise(key, extent, scale, limit, split=(), held_as=jnp.bfloat16):
    array = scale * jax.random.normal(key, extent, jnp.float32)
    if split:
        array = array * steps_of(key, extent, split, -0.22, 0.18)
    return jnp.clip(array, -limit, limit).astype(held_as)


def setup_inputs(seed: int = 0) -> dict:
    seeds = jax.random.split(jax.random.key(seed), 4)
    return {
        "fine_nodes": noise(seeds[0], (SLICES, NODES, FIELDS, NY, NX), 1.0, 6.0, ((0, 16), (3, 2)), jnp.float32),
        "init_state": noise(seeds[1], (FIELDS, NY, NX), 1.0, 6.0, ((1, 2),), jnp.float32),
        "mean_depth": jnp.clip(jnp.exp(math.log(2.0) - 1.3862944 * jax.random.uniform(seeds[2], (NY, NX), jnp.float32) ** steps_of(seeds[2], (NY, NX), ((0, 2),), -0.2, 0.2)), 0.5, 2.0),
    }


step_size = 0.3
viscosity = 1.0 / 3.0
coriolis = 0.5
quad_near = 5.0 / 24.0
quad_mid = 1.0 / 3.0
quad_far = -1.0 / 24.0


def column_slope(values):
    return (jnp.roll(values, -1, -1) - jnp.roll(values, 1, -1)) * 0.5


def row_slope(values):
    return (values[..., 2:, :] - values[..., :-2, :]) * 0.5


def diffuse(values, centre):
    return values[..., 2:, :] + values[..., :-2, :] + jnp.roll(centre, -1, -1) + jnp.roll(centre, 1, -1) - 4.0 * centre


def tendency(padded, depth_rows):
    height = padded[..., 0, :, :]
    east_flow = padded[..., 1, :, :]
    north_flow = padded[..., 2, :, :]
    centre = padded[..., 1:-1, :]
    height_c = centre[..., 0, :, :]
    east_c = centre[..., 1, :, :]
    north_c = centre[..., 2, :, :]
    depth_c = depth_rows[1:-1]
    height_rate = -column_slope(depth_c * east_c) - row_slope(depth_rows * north_flow) + viscosity * diffuse(height, height_c)
    east_rate = -column_slope(height_c) + coriolis * north_c + viscosity * diffuse(east_flow, east_c)
    north_rate = -row_slope(height) - coriolis * east_c + viscosity * diffuse(north_flow, north_c)
    return jnp.stack([height_rate, east_rate, north_rate], axis=-3)


def padded_rows(values):
    return jnp.concatenate([values[..., -1:, :], values, values[..., :1, :]], axis=-2)


def full_rate(values, mean_depth):
    return tendency(padded_rows(values), padded_rows(mean_depth))


def reference(fine_nodes, init_state, mean_depth):
    half_step = step_size * 0.5
    starts = jnp.concatenate([init_state[None], fine_nodes[:-1, 2]], axis=0)
    first_flags = jnp.arange(fine_nodes.shape[0], dtype=jnp.int32) == 0

    def slice_work(slice_items):
        points, section_zero, is_first = slice_items
        old_rates = full_rate(points, mean_depth)
        rate_zero = full_rate(section_zero, mean_depth)
        section_one = section_zero + half_step * (rate_zero - old_rates[0]) + step_size * (quad_near * old_rates[0] + quad_mid * old_rates[1] + quad_far * old_rates[2])
        rate_one = full_rate(section_one, mean_depth)
        section_two = section_one + half_step * (rate_one - old_rates[1]) + step_size * (quad_far * old_rates[0] + quad_mid * old_rates[1] + quad_near * old_rates[2])
        rate_two = full_rate(section_two, mean_depth)
        fas_term = -(step_size / 3.0) * (rate_zero - 2.0 * rate_one + rate_two)
        drift_total = half_step * (rate_two - rate_zero) + fas_term
        boosted = drift_total + jnp.where(is_first, section_zero + step_size * rate_zero, 0.0)
        return section_one, section_two, boosted

    section_ones, section_twos, boosts = lax.map(slice_work, (fine_nodes, starts, first_flags))

    def chain_turn(current, boosted):
        updated = boosted + (current + step_size * full_rate(current, mean_depth))
        return updated, updated

    _, coarse_end = lax.scan(chain_turn, jnp.zeros_like(init_state), boosts)
    coarse_begin = jnp.concatenate([init_state[None], coarse_end[:-1]], axis=0)
    middle = section_ones + 0.5 * ((coarse_begin - starts) + (coarse_end - section_twos))
    return jnp.stack([coarse_begin, middle, coarse_end], axis=1)
```

```python
import functools

import jax
import jax.numpy as jnp
from jax import lax
from jax.experimental import pallas as pl
from jax.experimental.pallas import tpu as pltpu
from jax.sharding import Mesh
from jax.sharding import PartitionSpec as P

DT = 0.3
HALF = 0.5 * DT
NU = 1.0 / 3.0
FC = 0.5
DEEP = 3
TILE = 8
LANES = 128


def rolled(x, by, axis):
    return pltpu.roll(x, by % x.shape[axis], axis)


def tendency(q, depth):
    height, east, north = q

    def near(x):
        up, down = rolled(x, 1, 0), rolled(x, -1, 0)
        left, right = rolled(x, 1, 1), rolled(x, -1, 1)
        lap = ((up + down) + (left + right)) - 4.0 * x
        return up, down, left, right, NU * lap

    h_up, h_down, h_left, h_right, h_lap = near(height)
    _, _, _, _, e_lap = near(east)
    _, _, _, _, n_lap = near(north)
    flux_e = depth * east
    flux_n = depth * north
    dh = (
        (rolled(flux_e, 1, 1) - rolled(flux_e, -1, 1))
        + (rolled(flux_n, 1, 0) - rolled(flux_n, -1, 0))
    ) * 0.5 + h_lap
    de = (h_left - h_right) * 0.5 + FC * north + e_lap
    dn = (h_up - h_down) * 0.5 - FC * east + n_lap
    return dh, de, dn


def stepped(q, depth):
    return tuple(x + DT * r for x, r in zip(q, tendency(q, depth)))


def combine_body(first_ref, nodes, prev, init, g_out, k_out, edge_out):
    rows = g_out.shape[1]
    first = first_ref[0] == 1
    edge_out[:, 15:, :] = jnp.zeros((2, 1, edge_out.shape[2]), jnp.float32)
    for f in range(3):
        n0, n1, n2 = nodes[0, f], nodes[1, f], nodes[2, f]
        start = jnp.where(first, init[f], prev[f])
        g = (DT / 24.0) * (12.0 * start - 7.0 * n0 + 8.0 * n1 - n2)
        k = (DT / 4.0) * (n0 - 2.0 * n1 + n2)
        g_out[f] = g
        k_out[f] = k
        edge_out[0, 3 * f : 3 * f + 3, :] = g[:3]
        edge_out[1, 3 * f : 3 * f + 3, :] = g[rows - 3 :]
        edge_out[0, 9 + 2 * f : 11 + 2 * f, :] = k[:2]
        edge_out[1, 9 + 2 * f : 11 + 2 * f, :] = k[rows - 2 :]


def fine_body(width, reach, g_ref, k_ref, below, above, depth_ref, msg_out, b_out, v_out):
    rows, cols = g_ref.shape[1:]
    depth = depth_ref[...]

    def with_halo(ref, f, base, deep):
        gap = jnp.zeros((TILE - 2 * deep, cols), jnp.float32)
        lo = base + deep * f
        return jnp.concatenate([ref[f], below[lo : lo + deep, :], gap, above[lo : lo + deep, :]], axis=0)

    g = tuple(with_halo(g_ref, f, 0, 3) for f in range(3))
    k = tuple(with_halo(k_ref, f, 9, 2) for f in range(3))
    fg = tendency(g, depth)
    u = tendency(fg, depth)
    v = tendency(tuple(a + HALF * b for a, b in zip(k, fg)), depth)
    fv = tendency(v, depth)
    span = msg_out.shape[2]
    lane = lax.broadcasted_iota(jnp.int32, (rows, LANES), 1)
    for f in range(3):
        b = DT * (u[f][:rows] + (1.0 / 6.0) * fv[f][:rows])
        v_out[f] = v[f][:rows]
        b_out[f] = b
        for j in range(msg_out.shape[0]):
            at = j * width
            if width % LANES == 0:
                parts = [b[:, (at + t) % cols : (at + t) % cols + LANES] for t in range(0, span, LANES)]
                tail = b[:, (at - LANES) % cols : (at - LANES) % cols + LANES]
            else:
                turned = rolled(b, -at, 1)
                parts = [turned[:, t : t + LANES] for t in range(0, span, LANES)]
                tail = turned[:, cols - LANES :]
            parts[-1] = jnp.where(lane < LANES - reach, parts[-1], tail)
            for t, part in enumerate(parts):
                msg_out[j, f * rows : (f + 1) * rows, t * LANES : (t + 1) * LANES] = part


def gathered(recv, slot, spaces, rows):
    return tuple(
        jnp.concatenate([recv[slot * spaces + y, f * rows : (f + 1) * rows, :] for y in range(spaces)], axis=0)
        for f in range(3)
    )


def total_body(spaces, recv, depth_ref, x0, total_out):
    rows = recv.shape[1] // 3
    slots = recv.shape[0] // spaces
    depth = depth_ref[...]
    q = tuple(x0[f] for f in range(3))
    for slot in range(slots):
        b = gathered(recv, slot, spaces, rows)
        q = tuple(x + y for x, y in zip(b, stepped(q, depth)))
    for f in range(3):
        total_out[f] = q[f]


def chain_body(spaces, lower_ref, recv, depth_ref, x0, carry, msg_out):
    rows = recv.shape[1] // 3
    slots = recv.shape[0] // spaces
    width = msg_out.shape[2]
    all_rows = rows * spaces
    depth = depth_ref[...]
    lower = lower_ref[0] == 1
    q = tuple(jnp.where(lower, x0[f], carry[f]) for f in range(3))
    for slot in range(slots):
        for y in range(spaces):
            at = slot * spaces + y
            for f in range(3):
                here = q[f][:, :width]
                lo, hi = y * rows, (y + 1) * rows
                msg_out[at, f * rows : (f + 1) * rows, :] = here[lo:hi]
                before, after = (lo - 1) % all_rows, hi % all_rows
                msg_out[at, 3 * rows + f : 3 * rows + f + 1, :] = here[before : before + 1]
                msg_out[at, 3 * rows + 3 + f : 3 * rows + 4 + f, :] = here[after : after + 1]
            msg_out[at, 3 * rows + 6 :, :] = jnp.zeros((2, width), jnp.float32)
        if slot + 1 < slots:
            b = gathered(recv, slot, spaces, rows)
            q = tuple(x + y for x, y in zip(b, stepped(q, depth)))


def finish_body(recv, b_ref, v_ref, depth_ref, out, state):
    rows = b_ref.shape[1]
    pieces, _, width = recv.shape
    for f in range(3):
        state[f, rows:, :] = jnp.zeros((TILE, state.shape[2]), jnp.float32)
        for j in range(pieces):
            cut = slice(j * width, (j + 1) * width)
            state[f, :rows, cut] = recv[j, f * rows : (f + 1) * rows, :]
            state[f, rows + TILE - 1 : rows + TILE, cut] = recv[j, 3 * rows + f : 3 * rows + f + 1, :]
            state[f, rows : rows + 1, cut] = recv[j, 3 * rows + 3 + f : 3 * rows + 4 + f, :]
    q = tuple(state[f] for f in range(3))
    after = stepped(q, depth_ref[...])
    for f in range(3):
        begin = q[f][:rows]
        end = b_ref[f] + after[f][:rows]
        out[0, f] = begin
        out[1, f] = 0.5 * ((begin + end) - v_ref[f])
        out[2, f] = end


def kernel(body, shapes, name, scalars=0, **more):
    vmem = pl.BlockSpec(memory_space=pltpu.VMEM)
    smem = pl.BlockSpec(memory_space=pltpu.SMEM)

    def call(*args):
        many = isinstance(shapes, list)
        outs = [jax.ShapeDtypeStruct(s, jnp.float32) for s in (shapes if many else [shapes])]
        return pl.pallas_call(
            body,
            out_shape=outs if many else outs[0],
            in_specs=[smem] * scalars + [vmem] * (len(args) - scalars),
            out_specs=[vmem] * len(outs) if many else vmem,
            compiler_params=pltpu.CompilerParams(vmem_limit_bytes=56 * 1024 * 1024),
            name=name,
            **more,
        )(*args)

    return call


def swap_rows(top, bottom):
    count = lax.axis_size("space")
    if count == 2:
        both = lax.ppermute(jnp.stack([top, bottom]), "space", [(0, 1), (1, 0)])
        return both[0], both[1]
    below = lax.ppermute(top, "space", [((i + 1) % count, i) for i in range(count)])
    above = lax.ppermute(bottom, "space", [(i, (i + 1) % count) for i in range(count)])
    return below, above


def per_device(fine_nodes, init_state, mean_depth):
    nodes = fine_nodes[0]
    rows, cols = nodes.shape[-2:]
    outer, inner, spaces = lax.axis_size("outer"), lax.axis_size("inner"), lax.axis_size("space")
    group = ("inner", "space")
    owners = inner * spaces
    width = cols // owners
    reach = outer * inner - 1
    span = -(-(width + 2 * reach) // LANES) * LANES
    at_outer, at_inner = lax.axis_index("outer"), lax.axis_index("inner")
    slice_index = at_outer * inner + at_inner
    first = (slice_index == 0).astype(jnp.int32).reshape(1)
    lower = (at_outer == 0).astype(jnp.int32).reshape(1)

    slices = outer * inner
    prev = lax.ppermute(nodes[2], ("outer", "inner"), [(i, i + 1) for i in range(slices - 1)])

    fixed = jnp.concatenate([mean_depth[None], init_state], axis=0)
    onward = jnp.concatenate([fixed, fixed[..., :span]], axis=-1)
    behind = jnp.concatenate([fixed[..., cols - span :], fixed], axis=-1)
    lane = lax.broadcasted_iota(jnp.int32, (4, rows, span), 2)
    windows = []
    for y in range(spaces):
        start = (at_inner * spaces + y) * width
        ahead = lax.dynamic_slice_in_dim(onward, start, span, axis=2)
        back = lax.dynamic_slice_in_dim(behind, start, span, axis=2)
        windows.append(jnp.where(lane < span - reach, ahead, back))
    windows = lax.all_to_all(jnp.stack(windows), "space", 0, 0, tiled=True)
    windows = windows.transpose(1, 0, 2, 3).reshape(4, spaces * rows, span)
    depth_block, init_block = windows[0], windows[1:]

    low, high = swap_rows(mean_depth[:DEEP], mean_depth[rows - DEEP :])
    gap = jnp.zeros((TILE - 2 * DEEP, cols), jnp.float32)
    depth = jnp.concatenate([mean_depth, low, gap, high], axis=0)

    state = (3, rows, cols)
    g, k, edges = kernel(combine_body, [state, state, (2, 16, cols)], "combine", scalars=1)(
        first, nodes, prev, init_state
    )
    below, above = swap_rows(edges[0], edges[1])
    msgs, drift, vee = kernel(
        functools.partial(fine_body, width, reach), [(owners, 3 * rows, span), state, state], "fine"
    )(g, k, below, above, depth)

    recv = lax.all_to_all(msgs, group, 0, 0, tiled=True)
    block = (3, spaces * rows, span)
    total = kernel(functools.partial(total_body, spaces), block, "total")(recv, depth_block, init_block)
    carry = lax.ppermute(total, "outer", [(i, i + 1) for i in range(outer - 1)])
    back = kernel(functools.partial(chain_body, spaces), (owners, 3 * rows + TILE, width), "chain", scalars=1)(
        lower, recv, depth_block, init_block, carry
    )
    mine = lax.all_to_all(back, group, 0, 0, tiled=True)
    if width % LANES:
        mine = mine.transpose(1, 0, 2).reshape(1, 3 * rows + TILE, cols)
    out = kernel(
        finish_body,
        (3,) + state,
        "finish",
        scratch_shapes=[pltpu.VMEM((3, rows + TILE, cols), jnp.float32)],
    )(mine, drift, vee, depth)
    return out[None]


def solution(mesh):
    slices, spaces = mesh.shape["tm"], mesh.shape["space"]
    split = Mesh(mesh.devices.reshape(2, slices // 2, spaces), ("outer", "inner", "space"))
    nodes = P(("outer", "inner"), None, None, "space", None)
    return jax.shard_map(
        per_device,
        mesh=split,
        in_specs=(nodes, P(None, "space", None), P("space", None)),
        out_specs=nodes,
        check_vma=False,
    )
```

```python
import functools

import jax
import jax.numpy as jnp
from jax import lax
from jax.experimental import pallas as pl
from jax.experimental.pallas import tpu as pltpu
from jax.sharding import Mesh
from jax.sharding import PartitionSpec as P


DT = 0.3
HALF = 0.5 * DT
NU = 1.0 / 3.0
FC = 0.5
DEEP = 3
TILE = 8
LANES = 128
VMEM_BYTES = 20 * 1024 * 1024


def rolled(x, by, axis):
    return pltpu.roll(x, by % x.shape[axis], axis)


def advanced(q, flow, scale, keep):
    height, east, north = q
    soft, slope, turn = scale * NU, scale * 0.5, scale * FC
    stay = keep - 4.0 * soft
    h_soft, e_soft, n_soft = soft * height, soft * east, soft * north
    h_slope = slope * height
    flow_e, flow_n = flow * east, flow * north
    new_h = (
        (rolled(h_soft + flow_e, 1, 1) + rolled(h_soft - flow_e, -1, 1))
        + (rolled(h_soft + flow_n, 1, 0) + rolled(h_soft - flow_n, -1, 0))
        + stay * height
    )
    new_e = (
        (rolled(e_soft + h_slope, 1, 1) + rolled(e_soft - h_slope, -1, 1))
        + (rolled(e_soft, 1, 0) + rolled(e_soft, -1, 0))
        + (stay * east + turn * north)
    )
    new_n = (
        (rolled(n_soft, 1, 1) + rolled(n_soft, -1, 1))
        + (rolled(n_soft + h_slope, 1, 0) + rolled(n_soft - h_slope, -1, 0))
        + (stay * north - turn * east)
    )
    return new_h, new_e, new_n


def tendency(q, half_depth):
    return advanced(q, half_depth, 1.0, 0.0)


def stepped(q, step_depth):
    return advanced(q, step_depth, DT, 1.0)


def last_body(nodes, last_out, edge_out, sem):
    rows = last_out.shape[1]
    copy = pltpu.make_async_copy(nodes.at[2], last_out, sem)
    copy.start()
    copy.wait()
    for f in range(3):
        for r in range(DEEP):
            edge_out[0, DEEP * f + r] = last_out[f, r : r + 1, :]
            edge_out[1, DEEP * f + r] = last_out[f, rows - DEEP + r : rows - DEEP + r + 1, :]


def blend_body(nodes, depth, base_out, bend_out, edge_out):
    rows = depth.shape[0]
    for f in range(3):
        n0, n1, n2 = nodes[0, f], nodes[1, f], nodes[2, f]
        bend = (DT / 4.0) * (n0 - 2.0 * n1 + n2)
        base_out[f] = (DT / 24.0) * (8.0 * n1 - 7.0 * n0 - n2)
        bend_out[f] = bend
        for r in range(2):
            edge_out[0, 2 * f + r] = bend[r : r + 1]
            edge_out[1, 2 * f + r] = bend[rows - 2 + r : rows - 1 + r]
    for r in range(DEEP):
        edge_out[0, 6 + r] = depth[r : r + 1, :]
        edge_out[1, 6 + r] = depth[rows - DEEP + r : rows - DEEP + r + 1, :]


def edge_body(first_ref, base, prev_edge, init, edge_out):
    rows = base.shape[1]
    first = first_ref[0] == 1
    for f in range(3):
        for side, lo in ((0, 0), (1, rows - DEEP)):
            for r in range(DEEP):
                at = slice(lo + r, lo + r + 1)
                start = jnp.where(first, init[f, at, :], prev_edge[side, DEEP * f + r])
                edge_out[side, DEEP * f + r] = HALF * start + base[f, at, :]


def with_halo(own, low, high, first, deep, state):
    rows = own.shape[0]
    state[:rows, :] = own
    state[rows:, :] = jnp.zeros((TILE, own.shape[1]), jnp.float32)
    for r in range(deep):
        state[rows + r : rows + r + 1, :] = low[first + r]
        state[rows + TILE - deep + r : rows + TILE - deep + r + 1, :] = high[first + r]


def fine_body(
    width, reach, first_ref, base, bend, prev, init, depth, low, high, low_early, high_early,
    msg_out, b_out, v_out, depth_out, state,
):
    rows, _ = depth.shape
    first = first_ref[0] == 1
    with_halo(depth[...], low_early, high_early, 6, DEEP, depth_out)
    half_depth = 0.5 * depth_out[...]
    for f in range(3):
        start = jnp.where(first, init[f], prev[f])
        with_halo(HALF * start + base[f], low, high, DEEP * f, DEEP, state.at[f])
        with_halo(bend[f], low_early, high_early, 2 * f, 2, state.at[3 + f])
    g = tuple(state[f] for f in range(3))
    k = tuple(state[3 + f] for f in range(3))
    fg = tendency(g, half_depth)
    u = tendency(fg, half_depth)
    v = tendency(tuple(x + HALF * y for x, y in zip(k, fg)), half_depth)
    fv = tendency(v, half_depth)
    for f in range(3):
        b = DT * (u[f][:rows] + (1.0 / 6.0) * fv[f][:rows])
        v_out[f] = v[f][:rows]
        b_out[f] = b
        pack_blocks(b, f, width, reach, msg_out)


def dense(width, reach, rows):
    return width % LANES == 0 and 2 * reach <= 32 and rows % TILE == 0


def packed_rows(rows, width, reach):
    if not dense(width, reach, rows):
        return None
    tiles = 3 * rows // TILE
    return 3 * rows * (width // LANES) + TILE * -(-tiles // 4)


def pack_blocks(b, f, width, reach, msg_out):
    rows, cols = b.shape
    lane = lax.broadcasted_iota(jnp.int32, (rows, LANES), 1)
    if dense(width, reach, rows):
        small = lax.broadcasted_iota(jnp.int32, (TILE, LANES), 1)
        parts = width // LANES
        for j in range(msg_out.shape[0]):
            for t in range(parts):
                at = j * width + t * LANES
                msg_out[j, (f * parts + t) * rows : (f * parts + t + 1) * rows, :] = b[:, at : at + LANES]
            after = (j + 1) * width % cols
            before = (j * width - LANES) % cols
            halo = jnp.where(lane < LANES // 2, b[:, after : after + LANES], b[:, before : before + LANES])
            put_halo(halo, f * rows // TILE, 3 * parts * rows, small, msg_out.at[j])
        return
    span = msg_out.shape[2]
    for j in range(msg_out.shape[0]):
        turned = rolled(b, -j * width, 1)
        parts = [turned[:, t : t + LANES] for t in range(0, span, LANES)]
        parts[-1] = jnp.where(lane < LANES - reach, parts[-1], turned[:, cols - LANES :])
        for t, part in enumerate(parts):
            msg_out[j, f * rows : (f + 1) * rows, t * LANES : (t + 1) * LANES] = part


def put_halo(halo, tile, base, small, out):
    for i in range(halo.shape[0] // TILE):
        q = (tile + i) % 4
        at = base + (tile + i) // 4 * TILE
        moved = rolled(halo[i * TILE : (i + 1) * TILE], 16 + 32 * q, 1)
        if q:
            moved = jnp.where(small >= 32 * q, moved, out[at : at + TILE, :])
        out[at : at + TILE, :] = moved


def get_halo(source, tile, count, base):
    found = []
    for i in range(tile, tile + count):
        at = base + i // 4 * TILE
        found.append(rolled(source[at : at + TILE, :], -(16 + 32 * (i % 4)), 1))
    return jnp.concatenate(found, axis=0)


def block_of(message, f, rows, width, reach):
    if not dense(width, reach, rows):
        return message[f * rows : (f + 1) * rows, :]
    parts = width // LANES
    main = [message[(f * parts + t) * rows : (f * parts + t + 1) * rows, :] for t in range(parts)]
    return jnp.concatenate(main + [get_halo(message, f * rows // TILE, rows // TILE, 3 * parts * rows)], axis=1)


def gathered(recv, slot, spaces, rows, width, reach):
    return tuple(
        jnp.concatenate(
            [block_of(recv.at[slot * spaces + y], f, rows, width, reach) for y in range(spaces)], axis=0
        )
        for f in range(3)
    )


def total_body(spaces, rows, width, reach, recv, depth_ref, x0, total_out):
    slots = recv.shape[0] // spaces
    step_depth = HALF * depth_ref[...]
    q = tuple(x0[f] for f in range(3))
    for slot in range(slots):
        b = gathered(recv, slot, spaces, rows, width, reach)
        q = tuple(x + y for x, y in zip(b, stepped(q, step_depth)))
    all_rows = rows * spaces
    if not dense(width, reach, rows):
        for f in range(3):
            total_out[f * all_rows : (f + 1) * all_rows, :] = q[f]
        return
    small = lax.broadcasted_iota(jnp.int32, (TILE, LANES), 1)
    parts = width // LANES
    for f in range(3):
        for t in range(parts):
            total_out[(f * parts + t) * all_rows : (f * parts + t + 1) * all_rows, :] = q[f][
                :, t * LANES : (t + 1) * LANES
            ]
        put_halo(q[f][:, width:], f * all_rows // TILE, 3 * parts * all_rows, small, total_out)


def chain_body(spaces, rows, width, reach, lower_ref, recv, depth_ref, x0, carry, msg_out):
    slots = recv.shape[0] // spaces
    all_rows = rows * spaces
    step_depth = HALF * depth_ref[...]
    lower = lower_ref[0] == 1
    q = tuple(jnp.where(lower, x0[f], block_of(carry, f, all_rows, width, reach)) for f in range(3))
    for slot in range(slots):
        for y in range(spaces):
            at = slot * spaces + y
            for f in range(3):
                here = q[f][:, :width]
                lo, hi = y * rows, (y + 1) * rows
                msg_out[at, f * rows : (f + 1) * rows, :] = here[lo:hi]
                before, after = (lo - 1) % all_rows, hi % all_rows
                msg_out[at, 3 * rows + f : 3 * rows + f + 1, :] = here[before : before + 1]
                msg_out[at, 3 * rows + 3 + f : 3 * rows + 4 + f, :] = here[after : after + 1]
            msg_out[at, 3 * rows + 6 :, :] = jnp.zeros((2, width), jnp.float32)
        if slot + 1 < slots:
            b = gathered(recv, slot, spaces, rows, width, reach)
            q = tuple(x + y for x, y in zip(b, stepped(q, step_depth)))


def finish_body(recv, b_ref, v_ref, depth_ref, out, state, made, sems):
    rows = b_ref.shape[1]
    pieces, _, width = recv.shape
    for f in range(3):
        state[f, rows:, :] = jnp.zeros((TILE, state.shape[2]), jnp.float32)
        for j in range(pieces):
            cut = slice(j * width, (j + 1) * width)
            state[f, :rows, cut] = recv[j, f * rows : (f + 1) * rows, :]
            state[f, rows + TILE - 1 : rows + TILE, cut] = recv[j, 3 * rows + f : 3 * rows + f + 1, :]
            state[f, rows : rows + 1, cut] = recv[j, 3 * rows + 3 + f : 3 * rows + 4 + f, :]
    copies = [
        pltpu.make_async_copy(state.at[f, pl.ds(0, rows), :], out.at[0, f], sems.at[f]) for f in range(3)
    ]
    for copy in copies:
        copy.start()
    q = tuple(state[f] for f in range(3))
    after = stepped(q, HALF * depth_ref[...])
    for f in range(3):
        begin = q[f][:rows]
        end = b_ref[f] + after[f][:rows]
        made[0, f] = 0.5 * ((begin + end) - v_ref[f])
        made[1, f] = end
        for part in range(2):
            copy = pltpu.make_async_copy(made.at[part, f], out.at[part + 1, f], sems.at[3 + 2 * f + part])
            copy.start()
            copies.append(copy)
    for copy in copies:
        copy.wait()


def kernel(body, shapes, *args, scalars=0, far_in=(), far_out=False, **more):
    def spec(far):
        return pl.BlockSpec(memory_space=pltpu.HBM if far else pltpu.VMEM)

    smem = pl.BlockSpec(memory_space=pltpu.SMEM)
    many = isinstance(shapes, list)
    outs = [jax.ShapeDtypeStruct(s, jnp.float32) for s in (shapes if many else [shapes])]
    return pl.pallas_call(
        body,
        out_shape=outs if many else outs[0],
        in_specs=[smem if i < scalars else spec(i in far_in) for i in range(len(args))],
        out_specs=[spec(far_out)] * len(outs) if many else spec(far_out),
        compiler_params=pltpu.CompilerParams(vmem_limit_bytes=VMEM_BYTES),
        **more,
    )(*args)


def swap_rows(edges):
    count = lax.axis_size("space")
    if count == 2:
        both = lax.ppermute(edges, "space", [(0, 1), (1, 0)])
        return both[0], both[1]
    below = lax.ppermute(edges[0], "space", [((i + 1) % count, i) for i in range(count)])
    above = lax.ppermute(edges[1], "space", [(i, (i + 1) % count) for i in range(count)])
    return below, above


def per_device(fine_nodes, init_state, mean_depth):
    nodes = fine_nodes[0]
    rows, cols = nodes.shape[-2:]
    outer, inner, spaces = lax.axis_size("outer"), lax.axis_size("inner"), lax.axis_size("space")
    group = ("inner", "space")
    owners = inner * spaces
    width = cols // owners
    slices = outer * inner
    reach = slices - 1
    span = -(-(width + 2 * reach) // LANES) * LANES
    at_outer, at_inner = lax.axis_index("outer"), lax.axis_index("inner")
    first = (at_outer * inner + at_inner == 0).astype(jnp.int32).reshape(1)
    lower = (at_outer == 0).astype(jnp.int32).reshape(1)
    onward_pairs = [(i, i + 1) for i in range(slices - 1)]
    state = (3, rows, cols)

    last, last_edge = kernel(
        last_body, [state, (2, 3 * DEEP, 1, cols)], nodes, far_in=(0,),
        scratch_shapes=[pltpu.SemaphoreType.DMA],
    )
    prev_edge = lax.ppermute(last_edge, ("outer", "inner"), onward_pairs)
    prev = lax.ppermute(last, ("outer", "inner"), onward_pairs)

    base, bend, early = kernel(blend_body, [state, state, (2, 9, 1, cols)], nodes, mean_depth)
    low_early, high_early = swap_rows(early)

    edges = kernel(edge_body, (2, 3 * DEEP, 1, cols), first, base, prev_edge, init_state, scalars=1)
    low, high = swap_rows(edges)

    fixed = jnp.concatenate([mean_depth[None], init_state], axis=0)
    onward = jnp.concatenate([fixed, fixed[..., :span]], axis=-1)
    behind = jnp.concatenate([fixed[..., cols - span :], fixed], axis=-1)
    lane = lax.broadcasted_iota(jnp.int32, (4, rows, span), 2)
    windows = []
    for y in range(spaces):
        start = (at_inner * spaces + y) * width
        ahead = lax.dynamic_slice_in_dim(onward, start, span, axis=2)
        back = lax.dynamic_slice_in_dim(behind, start, span, axis=2)
        windows.append(jnp.where(lane < span - reach, ahead, back))
    windows = lax.all_to_all(jnp.stack(windows), "space", 0, 0, tiled=True)
    windows = windows.transpose(1, 0, 2, 3).reshape(4, spaces * rows, span)
    depth_block, init_block = windows[0], windows[1:]

    tight = packed_rows(rows, width, reach)
    msg_shape = (owners, tight, LANES) if tight else (owners, 3 * rows, span)
    tight = packed_rows(spaces * rows, width, reach)
    total_shape = (tight, LANES) if tight else (3 * spaces * rows, span)
    msgs, drift, vee, depth = kernel(
        functools.partial(fine_body, width, reach),
        [msg_shape, state, state, (rows + TILE, cols)],
        first, base, bend, prev, init_state, mean_depth, low, high, low_early, high_early,
        scalars=1,
        scratch_shapes=[pltpu.VMEM((6, rows + TILE, cols), jnp.float32)],
    )
    recv = lax.all_to_all(msgs, group, 0, 0, tiled=True)
    plan = (spaces, rows, width, reach)
    total = kernel(functools.partial(total_body, *plan), total_shape, recv, depth_block, init_block)
    carry = lax.ppermute(total, "outer", [(i, i + 1) for i in range(outer - 1)])
    back = kernel(
        functools.partial(chain_body, *plan), (owners, 3 * rows + TILE, width),
        lower, recv, depth_block, init_block, carry, scalars=1,
    )
    mine = lax.all_to_all(back, group, 0, 0, tiled=True)
    if width % LANES:
        mine = mine.transpose(1, 0, 2).reshape(1, 3 * rows + TILE, cols)
    out = kernel(
        finish_body, (3,) + state, mine, drift, vee, depth, far_out=True,
        scratch_shapes=[
            pltpu.VMEM((3, rows + TILE, cols), jnp.float32),
            pltpu.VMEM((2,) + state, jnp.float32),
            pltpu.SemaphoreType.DMA((9,)),
        ],
    )
    return out[None]


def solution(mesh):
    slices, spaces = mesh.shape["tm"], mesh.shape["space"]
    split = Mesh(mesh.devices.reshape(2, slices // 2, spaces), ("outer", "inner", "space"))
    nodes = P(("outer", "inner"), None, None, "space", None)
    return jax.shard_map(
        per_device,
        mesh=split,
        in_specs=(nodes, P(None, "space", None), P("space", None)),
        out_specs=nodes,
        check_vma=False,
    )
```

```python
import functools

import jax
import jax.numpy as jnp
from jax import lax
from jax.experimental import pallas as pl
from jax.experimental.pallas import tpu as pltpu
from jax.sharding import Mesh
from jax.sharding import PartitionSpec as P


DT = 0.3
HALF = 0.5 * DT
NU = 1.0 / 3.0
FC = 0.5
DEEP = 3
TILE = 8
LANES = 128
VMEM_BYTES = 20 * 1024 * 1024


def rolled(x, by, axis):
    return pltpu.roll(x, by % x.shape[axis], axis)


def advanced(q, flow, scale, keep):
    height, east, north = q
    soft, slope, turn = scale * NU, scale * 0.5, scale * FC
    stay = keep - 4.0 * soft
    h_soft, e_soft, n_soft = soft * height, soft * east, soft * north
    h_slope = slope * height
    flow_e, flow_n = flow * east, flow * north
    new_h = (
        (rolled(h_soft + flow_e, 1, 1) + rolled(h_soft - flow_e, -1, 1))
        + (rolled(h_soft + flow_n, 1, 0) + rolled(h_soft - flow_n, -1, 0))
        + stay * height
    )
    new_e = (
        (rolled(e_soft + h_slope, 1, 1) + rolled(e_soft - h_slope, -1, 1))
        + (rolled(e_soft, 1, 0) + rolled(e_soft, -1, 0))
        + (stay * east + turn * north)
    )
    new_n = (
        (rolled(n_soft, 1, 1) + rolled(n_soft, -1, 1))
        + (rolled(n_soft + h_slope, 1, 0) + rolled(n_soft - h_slope, -1, 0))
        + (stay * north - turn * east)
    )
    return new_h, new_e, new_n


def tendency(q, half_depth):
    return advanced(q, half_depth, 1.0, 0.0)


def stepped(q, step_depth):
    return advanced(q, step_depth, DT, 1.0)


def dense(width, reach, rows):
    return width % LANES == 0 and 2 * reach <= 32 and rows % TILE == 0


def packed_rows(rows, width, reach):
    if not dense(width, reach, rows):
        return None
    tiles = 3 * rows // TILE
    return 3 * rows * (width // LANES) + TILE * -(-tiles // 4)


def cut(ref, lead, at, size=LANES):
    return ref[lead + (slice(None), pl.ds(pl.multiple_of(at, LANES), size))]


def prepare_body(spaces, width, reach, place, depth, init, edge_out, win_out):
    rows, cols = depth.shape
    for r in range(DEEP):
        edge_out[0, r] = depth[r : r + 1, :]
        edge_out[1, r] = depth[rows - DEEP + r : rows - DEEP + r + 1, :]
    lane = lax.broadcasted_iota(jnp.int32, (rows, LANES), 1)
    for y in range(spaces):
        start = place[2] * (cols // 2) + (place[3] * spaces + y) * width
        after = lax.rem(start + width, cols)
        before = lax.rem(start - LANES + cols, cols)
        for i in range(4):
            ref, lead = (depth, ()) if i == 0 else (init, (i - 1,))
            at = slice(i * rows, (i + 1) * rows)
            win_out[y, at, :width] = cut(ref, lead, start, width)
            win_out[y, at, width:] = jnp.where(
                lane < LANES - reach, cut(ref, lead, after), cut(ref, lead, before)
            )


def blend_body(nodes, depth, low, high, base_out, fk_out, ffk_out, depth_out, state):
    rows, cols = depth.shape
    none = jnp.zeros((TILE, cols), jnp.float32)
    depth_out[:rows, :] = 0.5 * depth[...]
    depth_out[rows:, :] = none
    for r in range(DEEP):
        depth_out[rows + r : rows + r + 1, :] = 0.5 * low[r]
        depth_out[rows + TILE - DEEP + r : rows + TILE - DEEP + r + 1, :] = 0.5 * high[r]
    for f in range(3):
        n0, n1, n2 = nodes[0, f], nodes[1, f], nodes[2, f]
        base_out[f] = (DT / 24.0) * (8.0 * n1 - 7.0 * n0 - n2)
        state[f, :rows, :] = (DT / 4.0) * (n0 - 2.0 * n1 + n2)
        state[f, rows:, :] = none
    half_depth = depth_out[...]
    fk = tendency(tuple(state[f] for f in range(3)), half_depth)
    ffk = tendency(fk, half_depth)
    for f in range(3):
        fk_out[f] = fk[f]
        ffk_out[f] = ffk[f]


def fine_body(place, base, prev, init, fk, ffk, depth_ref, b_out, v_out, give_out, spill_out, state):
    rows, cols = base.shape[1:]
    first = place[0] == 1
    half_depth = depth_ref[...]
    for f in range(3):
        state[f, :rows, :] = HALF * jnp.where(first, init[f], prev[f]) + base[f]
        state[f, rows:, :] = jnp.zeros((TILE, cols), jnp.float32)
    fg = tendency(tuple(state[f] for f in range(3)), half_depth)
    u = tendency(fg, half_depth)
    fu = tendency(u, half_depth)
    wide = rows + TILE
    for f in range(3):
        v_out[f] = fk[f] + HALF * u[f]
        b_out[f] = DT * (u[f] + (1.0 / 6.0) * (HALF * fu[f] + ffk[f]))
    theirs = (1 - place[2]) * (cols // 2) + (cols - LANES)
    for f in range(3):
        for t in range(give_out.shape[1] // LANES):
            at = lax.rem(theirs + t * LANES, cols)
            give_out[f * wide : (f + 1) * wide, t * LANES : (t + 1) * LANES] = cut(b_out, (f,), at)
    for f in range(3):
        for side, spread, edge in ((0, wide - DEEP, 0), (1, rows, rows - 1)):
            for r in range(DEEP):
                spill_out[side, DEEP * f + r] = b_out[f, spread + r : spread + r + 1, :]
            spill_out[side, 9 + f] = b_out[f, edge : edge + 1, :]
            spread = wide - 2 if side == 0 else rows
            for r in range(2):
                spill_out[side, 12 + 2 * f + r] = v_out[f, spread + r : spread + r + 1, :]


def mend_body(b_raw, v_raw, low, high, b_out, v_out):
    rows = v_out.shape[1]
    wide = rows + TILE
    for f in range(3):
        b_out[f] = b_raw[f]
        v_out[f] = v_raw[f, :rows, :]
        for r in range(DEEP):
            for at, more in ((r, high), (rows - DEEP + r, low)):
                b_out[f, at : at + 1, :] = b_raw[f, at : at + 1, :] + more[DEEP * f + r]
        for r in range(2):
            for at, more in ((r, high), (rows - 2 + r, low)):
                v_out[f, at : at + 1, :] = v_raw[f, at : at + 1, :] + more[12 + 2 * f + r]
        for at, more in ((rows, low), (wide - 1, high)):
            b_out[f, at : at + 1, :] = b_raw[f, at : at + 1, :] + more[9 + f]


def pair_body(width, reach, place, b_own, got, depth_ref, msg_out):
    wide, cols = b_own.shape[1:]
    tiles = got.shape[1] // LANES
    mine = place[2] * (cols // 2) + (cols - LANES)
    even = place[2] == 0

    def window(ref, lead):
        parts = [cut(ref, lead, lax.rem(mine + t * LANES, cols)) for t in range(tiles)]
        return jnp.concatenate(parts, axis=1)

    step_depth = DT * window(depth_ref, ())
    own = tuple(window(b_own, (f,)) for f in range(3))
    other = tuple(got[f * wide : (f + 1) * wide, :] for f in range(3))
    first = tuple(jnp.where(even, x, y) for x, y in zip(own, other))
    second = tuple(jnp.where(even, y, x) for x, y in zip(own, other))
    moved = stepped(first, step_depth)
    for f in range(3):
        pack_blocks(second[f] + moved[f], f, width, reach, msg_out)


def pack_blocks(b, f, width, reach, msg_out):
    rows, cols = b.shape
    lane = lax.broadcasted_iota(jnp.int32, (rows, LANES), 1)
    if dense(width, reach, rows):
        small = lax.broadcasted_iota(jnp.int32, (TILE, LANES), 1)
        parts = width // LANES
        for j in range(msg_out.shape[0]):
            for t in range(parts):
                at = LANES + j * width + t * LANES
                msg_out[j, (f * parts + t) * rows : (f * parts + t + 1) * rows, :] = b[:, at : at + LANES]
            after = LANES + (j + 1) * width
            before = j * width
            halo = jnp.where(lane < LANES // 2, b[:, after : after + LANES], b[:, before : before + LANES])
            put_halo(halo, f * rows // TILE, 3 * parts * rows, small, msg_out.at[j])
        return
    span = msg_out.shape[2]
    for j in range(msg_out.shape[0]):
        turned = rolled(b, -(LANES + j * width), 1)
        parts = [turned[:, t : t + LANES] for t in range(0, span, LANES)]
        parts[-1] = jnp.where(lane < LANES - reach, parts[-1], turned[:, cols - LANES :])
        for t, part in enumerate(parts):
            msg_out[j, f * rows : (f + 1) * rows, t * LANES : (t + 1) * LANES] = part


def put_halo(halo, tile, base, small, out):
    for i in range(halo.shape[0] // TILE):
        q = (tile + i) % 4
        at = base + (tile + i) // 4 * TILE
        moved = rolled(halo[i * TILE : (i + 1) * TILE], 16 + 32 * q, 1)
        if q:
            moved = jnp.where(small >= 32 * q, moved, out[at : at + TILE, :])
        out[at : at + TILE, :] = moved


def get_halo(source, tile, count, base):
    found = []
    for i in range(tile, tile + count):
        at = base + i // 4 * TILE
        found.append(rolled(source[at : at + TILE, :], -(16 + 32 * (i % 4)), 1))
    return jnp.concatenate(found, axis=0)


def block_of(message, f, rows, width, reach):
    if not dense(width, reach, rows):
        return message[f * rows : (f + 1) * rows, :]
    parts = width // LANES
    main = [message[(f * parts + t) * rows : (f * parts + t + 1) * rows, :] for t in range(parts)]
    return jnp.concatenate(main + [get_halo(message, f * rows // TILE, rows // TILE, 3 * parts * rows)], axis=1)


def joined(recv, slot, spaces, rows, width, reach):
    wide = rows + TILE
    fields = []
    for f in range(3):
        blocks = [block_of(recv.at[slot * spaces + y], f, wide, width, reach) for y in range(spaces)]
        row = lax.broadcasted_iota(jnp.int32, (TILE, blocks[0].shape[1]), 0)
        tiles = []
        for y in range(spaces):
            here = [blocks[y][t : t + TILE] for t in range(0, rows, TILE)]
            here[0] = here[0] + jnp.where(row < TILE // 2, blocks[(y - 1) % spaces][rows:], 0.0)
            here[-1] = here[-1] + jnp.where(row < TILE // 2, 0.0, blocks[(y + 1) % spaces][rows:])
            tiles += here
        fields.append(jnp.concatenate(tiles, axis=0))
    return tuple(fields)


def window_field(win, i, rows):
    return jnp.concatenate([win[y, i * rows : (i + 1) * rows, :] for y in range(win.shape[0])], axis=0)


def two_steps(q, step_depth):
    return stepped(stepped(q, step_depth), step_depth)


def total_body(spaces, rows, width, reach, recv, win, total_out):
    slots = recv.shape[0] // spaces
    step_depth = HALF * window_field(win, 0, rows)
    q = tuple(window_field(win, 1 + f, rows) for f in range(3))
    for slot in range(slots):
        b = joined(recv, slot, spaces, rows, width, reach)
        q = tuple(x + y for x, y in zip(b, two_steps(q, step_depth)))
    all_rows = rows * spaces
    if not dense(width, reach, rows):
        for f in range(3):
            total_out[f * all_rows : (f + 1) * all_rows, :] = q[f]
        return
    small = lax.broadcasted_iota(jnp.int32, (TILE, LANES), 1)
    parts = width // LANES
    for f in range(3):
        for t in range(parts):
            total_out[(f * parts + t) * all_rows : (f * parts + t + 1) * all_rows, :] = q[f][
                :, t * LANES : (t + 1) * LANES
            ]
        put_halo(q[f][:, width:], f * all_rows // TILE, 3 * parts * all_rows, small, total_out)


def chain_body(spaces, rows, width, reach, place, recv, win, carry, msg_out):
    slots = recv.shape[0] // spaces
    all_rows = rows * spaces
    step_depth = HALF * window_field(win, 0, rows)
    lower = place[1] == 1
    q = tuple(
        jnp.where(lower, window_field(win, 1 + f, rows), block_of(carry, f, all_rows, width, reach))
        for f in range(3)
    )
    for slot in range(slots):
        for y in range(spaces):
            at = slot * spaces + y
            for f in range(3):
                here = q[f][:, :width]
                lo, hi = y * rows, (y + 1) * rows
                msg_out[at, f * rows : (f + 1) * rows, :] = here[lo:hi]
                for r, source in enumerate((hi, hi + 1, lo - 2, lo - 1)):
                    source %= all_rows
                    to = 3 * rows + 4 * f + r
                    msg_out[at, to : to + 1, :] = here[source : source + 1]
            msg_out[at, 3 * rows + 12 :, :] = jnp.zeros((4, width), jnp.float32)
        if slot + 1 < slots:
            b = joined(recv, slot, spaces, rows, width, reach)
            q = tuple(x + y for x, y in zip(b, two_steps(q, step_depth)))


def finish_body(place, mine, other, b_own, b_lent, v_ref, depth_ref, out, state, made, sems):
    rows, cols = v_ref.shape[1:]
    wide = rows + TILE
    pieces, _, width = mine.shape
    even = place[2] == 0
    for f in range(3):
        state[f, rows:, :] = jnp.zeros((TILE, cols), jnp.float32)
        for source, half in ((mine, place[2]), (other, 1 - place[2])):
            for j in range(pieces):
                to = pl.ds(pl.multiple_of(half * (cols // 2) + j * width, LANES), width)
                state[f, :rows, to] = source[j, f * rows : (f + 1) * rows, :]
                for r, row in enumerate((rows, rows + 1, wide - 2, wide - 1)):
                    at = 3 * rows + 4 * f + r
                    state[f, row : row + 1, to] = source[j, at : at + 1, :]
    step_depth = DT * depth_ref[...]
    carried = tuple(state[f] for f in range(3))
    after = tuple(
        jnp.where(even, b_own[f], b_lent[f]) + x for f, x in enumerate(stepped(carried, step_depth))
    )
    last = stepped(after, step_depth)
    copies = []
    for f in range(3):
        begin = jnp.where(even, carried[f][:rows], after[f][:rows])
        end = jnp.where(even, after[f][:rows], b_own[f, :rows, :] + last[f][:rows])
        made[0, f] = begin
        made[1, f] = 0.5 * ((begin + end) - v_ref[f])
        made[2, f] = end
        for part in range(3):
            copy = pltpu.make_async_copy(made.at[part, f], out.at[part, f], sems.at[3 * f + part])
            copy.start()
            copies.append(copy)
    for copy in copies:
        copy.wait()


def kernel(body, shapes, *args, scalars=0, far_in=(), far_out=False, **more):
    def spec(far):
        return pl.BlockSpec(memory_space=pltpu.HBM if far else pltpu.VMEM)

    smem = pl.BlockSpec(memory_space=pltpu.SMEM)
    many = isinstance(shapes, list)
    outs = [jax.ShapeDtypeStruct(s, jnp.float32) for s in (shapes if many else [shapes])]
    return pl.pallas_call(
        body,
        out_shape=outs if many else outs[0],
        in_specs=[smem if i < scalars else spec(i in far_in) for i in range(len(args))],
        out_specs=[spec(far_out)] * len(outs) if many else spec(far_out),
        compiler_params=pltpu.CompilerParams(vmem_limit_bytes=VMEM_BYTES),
        **more,
    )(*args)


def swap_rows(edges):
    count = lax.axis_size("space")
    if count == 2:
        both = lax.ppermute(edges, "space", [(0, 1), (1, 0)])
        return both[0], both[1]
    below = lax.ppermute(edges[0], "space", [((i + 1) % count, i) for i in range(count)])
    above = lax.ppermute(edges[1], "space", [(i, (i + 1) % count) for i in range(count)])
    return below, above


def per_device(fine_nodes, init_state, mean_depth):
    nodes = fine_nodes[0]
    rows, cols = nodes.shape[-2:]
    outer, inner, spaces = lax.axis_size("outer"), lax.axis_size("inner"), lax.axis_size("space")
    group = ("inner", "space")
    owners = inner * spaces
    half = cols // 2
    width = half // owners
    slices = outer * inner * 2
    reach = slices - 2
    span = -(-(width + 2 * reach) // LANES) * LANES
    wide = rows + TILE
    at_outer, at_inner, at_core = (lax.axis_index(name) for name in ("outer", "inner", "core"))
    first = at_outer + at_inner + at_core == 0
    place = jnp.stack([first.astype(jnp.int32), (at_outer == 0).astype(jnp.int32), at_core, at_inner])
    state, spread = (3, rows, cols), (3, wide, cols)
    swapped = [(0, 1), (1, 0)]
    plan = (spaces, rows, width, reach)

    prev = lax.ppermute(nodes[2], ("outer", "inner", "core"), [(i, i + 1) for i in range(slices - 1)])

    edges, windows = kernel(
        functools.partial(prepare_body, spaces, width, reach) if dense(width, reach, rows) else edge_body,
        [(2, DEEP, 1, cols), (spaces, 4 * rows, span)],
        place, mean_depth, init_state, scalars=1,
    )
    if not dense(width, reach, rows):
        windows = sparse_windows(mean_depth, init_state, at_core * half, at_inner, spaces, width, reach, span)
    low, high = swap_rows(edges)
    windows = lax.all_to_all(windows, "space", 0, 0, tiled=True)

    base, fk, ffk, depth = kernel(
        blend_body, [state, spread, spread, (wide, cols)], nodes, mean_depth, low, high,
        scratch_shapes=[pltpu.VMEM(spread, jnp.float32)],
    )
    b_raw, v_raw, give, spill = kernel(
        fine_body, [spread, spread, (3 * wide, half + 2 * LANES), (2, 18, 1, cols)],
        place, base, prev, init_state, fk, ffk, depth, scalars=1,
        scratch_shapes=[pltpu.VMEM(spread, jnp.float32)],
    )
    got = lax.ppermute(give, "core", swapped)
    tight = packed_rows(wide, width, reach)
    msg_shape = (owners, tight, LANES) if tight else (owners, 3 * wide, span)
    msgs = kernel(functools.partial(pair_body, width, reach), msg_shape, place, b_raw, got, depth, scalars=1)
    recv = lax.all_to_all(msgs, group, 0, 0, tiled=True)
    low, high = swap_rows(spill)
    b_own, vee = kernel(mend_body, [spread, state], b_raw, v_raw, low, high)
    b_lent = lax.ppermute(b_own, "core", [(0, 1)])

    tight = packed_rows(spaces * rows, width, reach)
    total_shape = (tight, LANES) if tight else (3 * spaces * rows, span)
    total = kernel(functools.partial(total_body, *plan), total_shape, recv, windows)
    carry = lax.ppermute(total, "outer", [(i, i + 1) for i in range(outer - 1)])
    back = kernel(
        functools.partial(chain_body, *plan), (owners, 3 * rows + 2 * TILE, width),
        place, recv, windows, carry, scalars=1,
    )
    mine = lax.all_to_all(back, group, 0, 0, tiled=True)
    if width % LANES:
        mine = mine.transpose(1, 0, 2).reshape(1, 3 * rows + 2 * TILE, half)
    other = lax.ppermute(mine, "core", swapped)
    out = kernel(
        finish_body, (3,) + state, place, mine, other, b_own, b_lent, vee, depth,
        scalars=1, far_out=True,
        scratch_shapes=[
            pltpu.VMEM(spread, jnp.float32),
            pltpu.VMEM((3,) + state, jnp.float32),
            pltpu.SemaphoreType.DMA((9,)),
        ],
    )
    return out[None]


def edge_body(place, depth, init, edge_out, win_out):
    rows = depth.shape[0]
    win_out[...] = jnp.zeros(win_out.shape, jnp.float32)
    for r in range(DEEP):
        edge_out[0, r] = depth[r : r + 1, :]
        edge_out[1, r] = depth[rows - DEEP + r : rows - DEEP + r + 1, :]


def sparse_windows(depth, init, offset, at_inner, spaces, width, reach, span):
    fixed = jnp.concatenate([depth[None], init], axis=0)
    _, rows, cols = fixed.shape
    onward = jnp.concatenate([fixed, fixed[..., :span]], axis=-1)
    behind = jnp.concatenate([fixed[..., cols - span :], fixed], axis=-1)
    lane = lax.broadcasted_iota(jnp.int32, (4, rows, span), 2)
    windows = []
    for y in range(spaces):
        start = offset + (at_inner * spaces + y) * width
        ahead = lax.dynamic_slice_in_dim(onward, start, span, axis=2)
        back = lax.dynamic_slice_in_dim(behind, start, span, axis=2)
        windows.append(jnp.where(lane < span - reach, ahead, back).reshape(4 * rows, span))
    return jnp.stack(windows)


def solution(mesh):
    slices, spaces = mesh.shape["tm"], mesh.shape["space"]
    split = Mesh(mesh.devices.reshape(2, slices // 4, 2, spaces), ("outer", "inner", "core", "space"))
    nodes = P(("outer", "inner", "core"), None, None, "space", None)
    return jax.shard_map(
        per_device,
        mesh=split,
        in_specs=(nodes, P(None, "space", None), P("space", None)),
        out_specs=nodes,
        check_vma=False,
    )
```

```python
import functools

import jax
import jax.numpy as jnp
from jax import lax
from jax.experimental import pallas as pl
from jax.experimental.pallas import tpu as pltpu
from jax.sharding import Mesh
from jax.sharding import PartitionSpec as P


DT = 0.3
HALF = 0.5 * DT
NU = 1.0 / 3.0
FC = 0.5
DEEP = 3
TILE = 8
LANES = 128
VMEM_BYTES = 20 * 1024 * 1024


def rolled(x, by, axis):
    return pltpu.roll(x, by % x.shape[axis], axis)


def advanced(q, flow, scale, keep):
    height, east, north = q
    soft, slope, turn = scale * NU, scale * 0.5, scale * FC
    stay = keep - 4.0 * soft
    h_soft, e_soft, n_soft = soft * height, soft * east, soft * north
    h_slope = slope * height
    flow_e, flow_n = flow * east, flow * north
    new_h = (
        (rolled(h_soft + flow_e, 1, 1) + rolled(h_soft - flow_e, -1, 1))
        + (rolled(h_soft + flow_n, 1, 0) + rolled(h_soft - flow_n, -1, 0))
        + stay * height
    )
    new_e = (
        (rolled(e_soft + h_slope, 1, 1) + rolled(e_soft - h_slope, -1, 1))
        + (rolled(e_soft, 1, 0) + rolled(e_soft, -1, 0))
        + (stay * east + turn * north)
    )
    new_n = (
        (rolled(n_soft, 1, 1) + rolled(n_soft, -1, 1))
        + (rolled(n_soft + h_slope, 1, 0) + rolled(n_soft - h_slope, -1, 0))
        + (stay * north - turn * east)
    )
    return new_h, new_e, new_n


def tendency(q, half_depth):
    return advanced(q, half_depth, 1.0, 0.0)


def stepped(q, step_depth):
    return advanced(q, step_depth, DT, 1.0)


def dense(width, reach, rows):
    return width % LANES == 0 and 2 * reach <= 32 and rows % TILE == 0


def packed_rows(rows, width, reach):
    if not dense(width, reach, rows):
        return None
    tiles = 3 * rows // TILE
    return 3 * rows * (width // LANES) + TILE * -(-tiles // 4)


def cut(ref, lead, at, size=LANES):
    return ref[lead + (slice(None), pl.ds(pl.multiple_of(at, LANES), size))]


def prepare_body(width, reach, place, depth, init, own_out, edge_out):
    rows, cols = depth.shape
    lane = lax.broadcasted_iota(jnp.int32, (rows, LANES), 1)
    for out, y in ((own_out, place[4]), (edge_out, 1 - place[4])):
        start = place[2] * (cols // 2) + (place[3] * 2 + y) * width
        after = lax.rem(start + width, cols)
        before = lax.rem(start - LANES + cols, cols)
        for i in range(4):
            ref, lead = (depth, ()) if i == 0 else (init, (i - 1,))
            parts = [cut(ref, lead, start + t * LANES) for t in range(width // LANES)]
            parts.append(jnp.where(lane < LANES - reach, cut(ref, lead, after), cut(ref, lead, before)))
            for t, part in enumerate(parts):
                at = (4 * t + i) * rows
                out[at : at + rows, :] = part
    at = own_out.shape[0]
    for r in (*range(DEEP), *range(rows - DEEP, rows)):
        for t in range(cols // LANES):
            edge_out[at : at + 1, :] = depth[r : r + 1, t * LANES : (t + 1) * LANES]
            at += 1


def blend_body(nodes, depth, base_out, fk_out, state, near, sems):
    rows, cols = depth.shape
    copies = [pltpu.make_async_copy(nodes.at[:, f], near.at[f], sems.at[f]) for f in range(3)]
    for copy in copies:
        copy.start()
    none = jnp.zeros((TILE, cols), jnp.float32)
    for f in range(3):
        copies[f].wait()
        n0, n1, n2 = near[f, 0], near[f, 1], near[f, 2]
        base_out[f] = (DT / 24.0) * (8.0 * n1 - 7.0 * n0 - n2)
        state[f, :rows, :] = (DT / 4.0) * (n0 - 2.0 * n1 + n2)
        state[f, rows:, :] = none
    half_depth = jnp.concatenate([0.5 * depth[...], none], axis=0)
    fk = tendency(tuple(state[f] for f in range(3)), half_depth)
    for f in range(3):
        fk_out[f] = fk[f]


def second_body(fk, depth, *rest):
    *edges, ffk_out, depth_out = rest
    rows, cols = depth.shape
    depth_out[:rows, :] = 0.5 * depth[...]
    depth_out[rows:, :] = jnp.zeros((TILE, cols), jnp.float32)
    for r in range(DEEP):
        below, above = rows + r, rows + TILE - DEEP + r
        if len(edges) == 2:
            depth_out[below : below + 1, :] = 0.5 * edges[0][r]
            depth_out[above : above + 1, :] = 0.5 * edges[1][r]
            continue
        tiles = cols // LANES
        base = edges[0].shape[0] - 2 * DEEP * tiles
        for t in range(tiles):
            for to, at in ((below, base + r * tiles + t), (above, base + (DEEP + r) * tiles + t)):
                depth_out[to : to + 1, t * LANES : (t + 1) * LANES] = 0.5 * edges[0][at : at + 1, :]
    ffk = tendency(tuple(fk[f] for f in range(3)), depth_out[...])
    for f in range(3):
        ffk_out[f] = ffk[f]


def window(ref, lead, half):
    cols = ref.shape[-1]
    start = half * (cols // 2) + (cols - LANES)
    parts = [cut(ref, lead, lax.rem(start + t * LANES, cols)) for t in range(cols // 2 // LANES + 2)]
    return jnp.concatenate(parts, axis=1)


def fine_body(own_half, place, base, prev, init, fk, ffk, depth_ref, b_out, v_out):
    half = place[2] if own_half else 1 - place[2]
    first = place[0] == 1
    wide = fk.shape[1]
    half_depth = window(depth_ref, (), half)
    none = jnp.zeros((TILE, half_depth.shape[1]), jnp.float32)
    g = []
    for f in range(3):
        start = jnp.where(first, window(init, (f,), half), window(prev, (f,), half))
        g.append(jnp.concatenate([HALF * start + window(base, (f,), half), none], axis=0))
    u = tendency(tendency(tuple(g), half_depth), half_depth)
    fu = tendency(u, half_depth)
    for f in range(3):
        at = slice(f * wide, (f + 1) * wide)
        v = window(fk, (f,), half) + HALF * u[f]
        v_out[at, :] = v[:, LANES : v.shape[1] - LANES]
        b_out[at, :] = DT * (u[f] + (1.0 / 6.0) * (HALF * fu[f] + window(ffk, (f,), half)))


def spill_body(b_keep, b_give, v_keep, v_give, spill_out):
    wide = b_keep.shape[0] // 3
    rows = wide - TILE
    for h, (b, v) in enumerate(((b_keep, v_keep), (b_give, v_give))):
        inside = slice(LANES, b.shape[1] - LANES)
        for f in range(3):
            top = f * wide
            for side, spread, edge in ((0, wide - DEEP, 0), (1, rows, rows - 1)):
                for r in range(DEEP):
                    spill_out[side, h, DEEP * f + r] = b[top + spread + r : top + spread + r + 1, inside]
                spill_out[side, h, 9 + f] = b[top + edge : top + edge + 1, inside]
                spread = wide - 2 if side == 0 else rows
                for r in range(2):
                    spill_out[side, h, 12 + 2 * f + r] = v[top + spread + r : top + spread + r + 1, :]


def mend_body(place, b_keep, b_give, v_keep, v_give, low, high, b_out, v_far, v_out, sem):
    rows = v_out.shape[1]
    wide = rows + TILE
    size = v_keep.shape[1]
    halves = ((place[2], b_keep, v_keep), (1 - place[2], b_give, v_give))
    for h, (half, _, v) in enumerate(halves):
        to = pl.ds(pl.multiple_of(half * size, LANES), size)
        for f in range(3):
            v_out[f, :, to] = v[f * wide : f * wide + rows, :]
            for r in range(2):
                for at, more in ((r, high), (rows - 2 + r, low)):
                    old = v[f * wide + at : f * wide + at + 1, :]
                    v_out[f, at : at + 1, to] = old + more[h, 12 + 2 * f + r]
    copy = pltpu.make_async_copy(v_out, v_far, sem)
    copy.start()
    for h, (half, b, _) in enumerate(halves):
        to = pl.ds(pl.multiple_of(half * size, LANES), size)
        inside = slice(LANES, LANES + size)
        for f in range(3):
            top = f * wide
            b_out[f, :, to] = b[top : top + wide, inside]
            adds = [(rows, 9 + f, low), (wide - 1, 9 + f, high)]
            for r in range(DEEP):
                adds += [(r, DEEP * f + r, high), (rows - DEEP + r, DEEP * f + r, low)]
            for at, i, more in adds:
                b_out[f, at : at + 1, to] = b[top + at : top + at + 1, inside] + more[h, i]
    copy.wait()


def pair_body(width, reach, count, place, depth_ref, got, *rest):
    near, far = rest[:count], rest[count + 1 : 2 * count + 1]
    msg_far, msg_out, sems = rest[count], rest[-2], rest[-1]
    owners = msg_out.shape[0]
    copies = [pltpu.make_async_copy(a, b, sems.at[owners + i]) for i, (a, b) in enumerate(zip(near, far))]
    for copy in copies:
        copy.start()
    keep = near[0]
    wide = keep.shape[0] // 3
    even = place[2] == 0
    step_depth = DT * window(depth_ref, (), place[2])
    own = tuple(keep[f * wide : (f + 1) * wide, :] for f in range(3))
    other = tuple(got[f * wide : (f + 1) * wide, :] for f in range(3))
    first = tuple(jnp.where(even, x, y) for x, y in zip(own, other))
    second = tuple(jnp.where(even, y, x) for x, y in zip(own, other))
    both = tuple(x + y for x, y in zip(second, stepped(first, step_depth)))
    for j in range(owners):
        for f in range(3):
            pack_block(both[f], f, j, width, reach, msg_out.at[j])
    copies.append(pltpu.make_async_copy(msg_out, msg_far, sems.at[0]))
    copies[-1].start()
    for copy in copies:
        copy.wait()


def pack_block(b, f, j, width, reach, out):
    rows, cols = b.shape
    at = LANES + j * width
    lane = lax.broadcasted_iota(jnp.int32, (rows, LANES), 1)
    if dense(width, reach, rows):
        small = lax.broadcasted_iota(jnp.int32, (TILE, LANES), 1)
        parts = width // LANES
        for t in range(parts):
            out[(f * parts + t) * rows : (f * parts + t + 1) * rows, :] = b[:, at + t * LANES : at + (t + 1) * LANES]
        after, before = at + width, at - LANES
        halo = jnp.where(lane < LANES // 2, b[:, after : after + LANES], b[:, before : before + LANES])
        put_halo(halo, f * rows // TILE, 3 * parts * rows, small, out)
        return
    span = out.shape[1]
    turned = rolled(b, -at, 1)
    parts = [turned[:, t : t + LANES] for t in range(0, span, LANES)]
    parts[-1] = jnp.where(lane < LANES - reach, parts[-1], turned[:, cols - LANES :])
    for t, part in enumerate(parts):
        out[f * rows : (f + 1) * rows, t * LANES : (t + 1) * LANES] = part


def put_halo(halo, tile, base, small, out):
    for i in range(halo.shape[0] // TILE):
        q = (tile + i) % 4
        at = base + (tile + i) // 4 * TILE
        moved = rolled(halo[i * TILE : (i + 1) * TILE], 16 + 32 * q, 1)
        if q:
            moved = jnp.where(small >= 32 * q, moved, out[at : at + TILE, :])
        out[at : at + TILE, :] = moved


def get_halo(source, tile, count, base):
    found = []
    for i in range(tile, tile + count):
        at = base + i // 4 * TILE
        found.append(rolled(source[at : at + TILE, :], -(16 + 32 * (i % 4)), 1))
    return jnp.concatenate(found, axis=0)


def block_of(message, f, rows, width, reach):
    if not dense(width, reach, rows):
        return message[f * rows : (f + 1) * rows, :]
    parts = width // LANES
    main = [message[(f * parts + t) * rows : (f * parts + t + 1) * rows, :] for t in range(parts)]
    return jnp.concatenate(main + [get_halo(message, f * rows // TILE, rows // TILE, 3 * parts * rows)], axis=1)


def joined(recv, slot, spaces, rows, width, reach):
    wide = rows + TILE
    fields = []
    for f in range(3):
        blocks = [block_of(recv.at[slot * spaces + y], f, wide, width, reach) for y in range(spaces)]
        row = lax.broadcasted_iota(jnp.int32, (TILE, blocks[0].shape[1]), 0)
        tiles = []
        for y in range(spaces):
            here = [blocks[y][t : t + TILE] for t in range(0, rows, TILE)]
            here[0] = here[0] + jnp.where(row < TILE // 2, blocks[(y - 1) % spaces][rows:], 0.0)
            here[-1] = here[-1] + jnp.where(row < TILE // 2, 0.0, blocks[(y + 1) % spaces][rows:])
            tiles += here
        fields.append(jnp.concatenate(tiles, axis=0))
    return tuple(fields)


def window_field(win, i, rows, place):
    if len(win) == 1:
        return jnp.concatenate([win[0][y, i * rows : (i + 1) * rows, :] for y in range(win[0].shape[0])], axis=0)
    own, theirs = (
        jnp.concatenate([part[at : at + rows, :] for at in range(i * rows, part.shape[0], 4 * rows)], axis=1)
        for part in (win[0], win[1].at[: win[0].shape[0]])
    )
    above = place[4] == 0
    return jnp.concatenate([jnp.where(above, own, theirs), jnp.where(above, theirs, own)], axis=0)


def two_steps(q, step_depth):
    return stepped(stepped(q, step_depth), step_depth)


def total_body(spaces, rows, width, reach, place, recv, *rest):
    *win, total_out = rest
    slots = recv.shape[0] // spaces
    step_depth = HALF * window_field(win, 0, rows, place)
    q = tuple(window_field(win, 1 + f, rows, place) for f in range(3))
    for slot in range(slots):
        b = joined(recv, slot, spaces, rows, width, reach)
        q = tuple(x + y for x, y in zip(b, two_steps(q, step_depth)))
    all_rows = rows * spaces
    if not dense(width, reach, rows):
        for f in range(3):
            total_out[f * all_rows : (f + 1) * all_rows, :] = q[f]
        return
    small = lax.broadcasted_iota(jnp.int32, (TILE, LANES), 1)
    parts = width // LANES
    for f in range(3):
        for t in range(parts):
            total_out[(f * parts + t) * all_rows : (f * parts + t + 1) * all_rows, :] = q[f][
                :, t * LANES : (t + 1) * LANES
            ]
        put_halo(q[f][:, width:], f * all_rows // TILE, 3 * parts * all_rows, small, total_out)


def chain_body(spaces, rows, width, reach, place, recv, carry, *rest):
    *win, msg_far, msg_out, sems = rest
    slots = recv.shape[0] // spaces
    all_rows = rows * spaces
    copies = []
    step_depth = HALF * window_field(win, 0, rows, place)
    lower = place[1] == 1
    q = tuple(
        jnp.where(lower, window_field(win, 1 + f, rows, place), block_of(carry, f, all_rows, width, reach))
        for f in range(3)
    )
    for slot in range(slots):
        for y in range(spaces):
            at = slot * spaces + y
            for f in range(3):
                here = q[f][:, :width]
                lo, hi = y * rows, (y + 1) * rows
                msg_out[at, f * rows : (f + 1) * rows, :] = here[lo:hi]
                for r, source in enumerate((hi, hi + 1, lo - 2, lo - 1)):
                    source %= all_rows
                    to = 3 * rows + 4 * f + r
                    msg_out[at, to : to + 1, :] = here[source : source + 1]
            msg_out[at, 3 * rows + 12 :, :] = jnp.zeros((4, width), jnp.float32)
            copies.append(pltpu.make_async_copy(msg_out.at[at], msg_far.at[at], sems.at[at]))
            copies[-1].start()
        if slot + 1 < slots:
            b = joined(recv, slot, spaces, rows, width, reach)
            q = tuple(x + y for x, y in zip(b, two_steps(q, step_depth)))
    for copy in copies:
        copy.wait()


def finish_body(place, mine, other, b_far, b_lent, v_far, depth_ref, out, state, made, v_ref, b_own, sems):
    rows, cols = v_ref.shape[1:]
    fetches = [pltpu.make_async_copy(b_far, b_own, sems.at[9]), pltpu.make_async_copy(v_far, v_ref, sems.at[10])]
    for fetch in fetches:
        fetch.start()
    wide = rows + TILE
    pieces, _, width = mine.shape
    even = place[2] == 0
    for f in range(3):
        state[f, rows:, :] = jnp.zeros((TILE, cols), jnp.float32)
        for source, half in ((mine, place[2]), (other, 1 - place[2])):
            for j in range(pieces):
                to = pl.ds(pl.multiple_of(half * (cols // 2) + j * width, LANES), width)
                state[f, :rows, to] = source[j, f * rows : (f + 1) * rows, :]
                for r, row in enumerate((rows, rows + 1, wide - 2, wide - 1)):
                    at = 3 * rows + 4 * f + r
                    state[f, row : row + 1, to] = source[j, at : at + 1, :]
    step_depth = DT * depth_ref[...]
    carried = tuple(state[f] for f in range(3))
    for fetch in fetches:
        fetch.wait()
    after = tuple(
        jnp.where(even, b_own[f], b_lent[f]) + x for f, x in enumerate(stepped(carried, step_depth))
    )
    last = stepped(after, step_depth)
    copies = []
    for f in range(3):
        begin = jnp.where(even, carried[f][:rows], after[f][:rows])
        end = jnp.where(even, after[f][:rows], b_own[f, :rows, :] + last[f][:rows])
        made[0, f] = begin
        made[1, f] = 0.5 * ((begin + end) - v_ref[f])
        made[2, f] = end
        for part in range(3):
            copy = pltpu.make_async_copy(made.at[part, f], out.at[part, f], sems.at[3 * f + part])
            copy.start()
            copies.append(copy)
    for copy in copies:
        copy.wait()


def kernel(body, shapes, *args, scalars=0, far=(), far_out=(), **more):
    vmem = pl.BlockSpec(memory_space=pltpu.VMEM)
    hbm = pl.BlockSpec(memory_space=pltpu.HBM)
    smem = pl.BlockSpec(memory_space=pltpu.SMEM)
    many = isinstance(shapes, list)
    outs = [
        pltpu.HBM(shape, jnp.float32) if i in far_out else jax.ShapeDtypeStruct(shape, jnp.float32)
        for i, shape in enumerate(shapes if many else [shapes])
    ]
    specs = [hbm if i in far_out else vmem for i in range(len(outs))]
    return pl.pallas_call(
        body,
        out_shape=outs if many else outs[0],
        in_specs=[smem if i < scalars else hbm if i in far else vmem for i in range(len(args))],
        out_specs=specs if many else specs[0],
        compiler_params=pltpu.CompilerParams(vmem_limit_bytes=VMEM_BYTES),
        **more,
    )(*[pltpu.with_memory_space_constraint(x, pltpu.HBM) if i in far else x for i, x in enumerate(args)])


def swap_rows(edges):
    count = lax.axis_size("space")
    if count == 2:
        both = lax.ppermute(edges, "space", [(0, 1), (1, 0)])
        return both[0], both[1]
    below = lax.ppermute(edges[0], "space", [((i + 1) % count, i) for i in range(count)])
    above = lax.ppermute(edges[1], "space", [(i, (i + 1) % count) for i in range(count)])
    return below, above


def per_device(fine_nodes, init_state, mean_depth):
    nodes = fine_nodes[0]
    rows, cols = nodes.shape[-2:]
    outer, inner, spaces = lax.axis_size("outer"), lax.axis_size("inner"), lax.axis_size("space")
    group = ("inner", "space")
    owners = inner * spaces
    half = cols // 2
    width = half // owners
    slices = outer * inner * 2
    reach = slices - 2
    span = -(-(width + 2 * reach) // LANES) * LANES
    wide = rows + TILE
    at_outer, at_inner, at_core, at_space = (
        lax.axis_index(name) for name in ("outer", "inner", "core", "space")
    )
    first = at_outer + at_inner + at_core == 0
    place = jnp.stack([first.astype(jnp.int32), (at_outer == 0).astype(jnp.int32), at_core, at_inner, at_space])
    state, spread = (3, rows, cols), (3, wide, cols)
    swapped = [(0, 1), (1, 0)]
    plan = (spaces, rows, width, reach)

    prev = lax.ppermute(nodes[2], ("outer", "inner", "core"), [(i, i + 1) for i in range(slices - 1)])

    if spaces == 2 and dense(width, reach, rows):
        own_rows = 4 * rows * span // LANES
        own, edges = kernel(
            functools.partial(prepare_body, width, reach),
            [(own_rows, LANES), (own_rows + 2 * DEEP * cols // LANES, LANES)],
            place, mean_depth, init_state, scalars=1,
        )
        edges = lax.ppermute(edges, "space", swapped)
        windows, edges = (own, edges), (edges,)
    else:
        windows = all_windows(mean_depth, init_state, at_core * half, at_inner, spaces, width, reach, span)
        windows = (lax.all_to_all(windows, "space", 0, 0, tiled=True),)
        edges = jnp.stack([mean_depth[:DEEP, None], mean_depth[rows - DEEP :, None]])
        edges = swap_rows(edges)

    base, fk = kernel(
        blend_body, [state, spread], nodes, mean_depth, far=(0,),
        scratch_shapes=[
            pltpu.VMEM(spread, jnp.float32),
            pltpu.VMEM((3,) + state, jnp.float32),
            pltpu.SemaphoreType.DMA((3,)),
        ],
    )
    ffk, depth = kernel(second_body, [spread, (wide, cols)], fk, mean_depth, *edges)
    fine_shapes = [(3 * wide, half + 2 * LANES), (3 * wide, half)]
    fine_args = (place, base, prev, init_state, fk, ffk, depth)
    give, v_give = kernel(functools.partial(fine_body, False), fine_shapes, *fine_args, scalars=1)
    got = lax.ppermute(give, "core", swapped)
    keep, v_keep = kernel(functools.partial(fine_body, True), fine_shapes, *fine_args, scalars=1)
    tight = packed_rows(wide, width, reach)
    msg_shape = (owners, tight, LANES) if tight else (owners, 3 * wide, span)
    parts = (keep, give, v_keep, v_give)
    msgs, *parts = kernel(
        functools.partial(pair_body, width, reach, len(parts)), [msg_shape] + [x.shape for x in parts],
        place, depth, got, *parts, scalars=1, far_out=range(1 + len(parts)),
        scratch_shapes=[pltpu.VMEM(msg_shape, jnp.float32), pltpu.SemaphoreType.DMA((owners + len(parts),))],
    )
    recv = lax.all_to_all(msgs, group, 0, 0, tiled=True)
    spill = kernel(spill_body, (2, 2, 18, 1, half), *parts)
    low, high = swap_rows(spill)
    b_own, vee = kernel(
        mend_body, [spread, state], place, *parts, low, high, scalars=1, far_out=(1,),
        scratch_shapes=[pltpu.VMEM(state, jnp.float32), pltpu.SemaphoreType.DMA],
    )
    b_lent = lax.ppermute(b_own, "core", [(0, 1)])

    tight = packed_rows(spaces * rows, width, reach)
    total_shape = (tight, LANES) if tight else (3 * spaces * rows, span)
    total = kernel(functools.partial(total_body, *plan), total_shape, place, recv, *windows, scalars=1)
    carry = lax.ppermute(total, "outer", [(i, i + 1) for i in range(outer - 1)])
    back = kernel(
        functools.partial(chain_body, *plan), (owners, 3 * rows + 2 * TILE, width),
        place, recv, carry, *windows, scalars=1, far_out=(0,),
        scratch_shapes=[
            pltpu.VMEM((owners, 3 * rows + 2 * TILE, width), jnp.float32),
            pltpu.SemaphoreType.DMA((owners,)),
        ],
    )
    mine = lax.all_to_all(back, group, 0, 0, tiled=True)
    if width % LANES:
        mine = mine.transpose(1, 0, 2).reshape(1, 3 * rows + 2 * TILE, half)
    other = lax.ppermute(mine, "core", swapped)
    out = kernel(
        finish_body, (3,) + state, place, mine, other, b_own, b_lent, vee, depth,
        scalars=1, far=(3, 5), far_out=(0,),
        scratch_shapes=[
            pltpu.VMEM(spread, jnp.float32),
            pltpu.VMEM((3,) + state, jnp.float32),
            pltpu.VMEM(state, jnp.float32),
            pltpu.VMEM(spread, jnp.float32),
            pltpu.SemaphoreType.DMA((11,)),
        ],
    )
    return out[None]


def all_windows(depth, init, offset, at_inner, spaces, width, reach, span):
    fixed = jnp.concatenate([depth[None], init], axis=0)
    _, rows, cols = fixed.shape
    onward = jnp.concatenate([fixed, fixed[..., :span]], axis=-1)
    behind = jnp.concatenate([fixed[..., cols - span :], fixed], axis=-1)
    lane = lax.broadcasted_iota(jnp.int32, (4, rows, span), 2)
    windows = []
    for y in range(spaces):
        start = offset + (at_inner * spaces + y) * width
        ahead = lax.dynamic_slice_in_dim(onward, start, span, axis=2)
        back = lax.dynamic_slice_in_dim(behind, start, span, axis=2)
        windows.append(jnp.where(lane < span - reach, ahead, back).reshape(4 * rows, span))
    return jnp.stack(windows)


def solution(mesh):
    slices, spaces = mesh.shape["tm"], mesh.shape["space"]
    split = Mesh(mesh.devices.reshape(2, slices // 4, 2, spaces), ("outer", "inner", "core", "space"))
    nodes = P(("outer", "inner", "core"), None, None, "space", None)
    return jax.shard_map(
        per_device,
        mesh=split,
        in_specs=(nodes, P(None, "space", None), P("space", None)),
        out_specs=nodes,
        check_vma=False,
    )
```

```python
import functools

import jax
import jax.numpy as jnp
from jax import lax
from jax.experimental import pallas as pl
from jax.experimental.pallas import tpu as pltpu
from jax.sharding import Mesh
from jax.sharding import PartitionSpec as P


DT = 0.3
HALF = 0.5 * DT
NU = 1.0 / 3.0
FC = 0.5
DEEP = 3
TILE = 8
LANES = 128
VMEM_BYTES = 20 * 1024 * 1024


def rolled(x, by, axis):
    return pltpu.roll(x, by % x.shape[axis], axis)


def advanced(q, flow, scale, keep):
    height, east, north = q
    soft, slope, turn = scale * NU, scale * 0.5, scale * FC
    stay = keep - 4.0 * soft
    h_soft, e_soft, n_soft = soft * height, soft * east, soft * north
    h_slope = slope * height
    flow_e, flow_n = flow * east, flow * north
    new_h = (
        (rolled(h_soft + flow_e, 1, 1) + rolled(h_soft - flow_e, -1, 1))
        + (rolled(h_soft + flow_n, 1, 0) + rolled(h_soft - flow_n, -1, 0))
        + stay * height
    )
    new_e = (
        (rolled(e_soft + h_slope, 1, 1) + rolled(e_soft - h_slope, -1, 1))
        + (rolled(e_soft, 1, 0) + rolled(e_soft, -1, 0))
        + (stay * east + turn * north)
    )
    new_n = (
        (rolled(n_soft, 1, 1) + rolled(n_soft, -1, 1))
        + (rolled(n_soft + h_slope, 1, 0) + rolled(n_soft - h_slope, -1, 0))
        + (stay * north - turn * east)
    )
    return new_h, new_e, new_n


def tendency(q, half_depth):
    return advanced(q, half_depth, 1.0, 0.0)


def stepped(q, step_depth):
    return advanced(q, step_depth, DT, 1.0)


def dense(width, reach, rows):
    return width % LANES == 0 and 2 * reach <= 32 and rows % TILE == 0


def packed_rows(rows, width, reach):
    if not dense(width, reach, rows):
        return None
    tiles = 3 * rows // TILE
    return 3 * rows * (width // LANES) + TILE * -(-tiles // 4)


def cut(ref, lead, at, size=LANES):
    return ref[lead + (slice(None), pl.ds(pl.multiple_of(at, LANES), size))]


def last_body(nodes, out, sem):
    copy = pltpu.make_async_copy(nodes.at[2], out, sem)
    copy.start()
    copy.wait()


def prepare_body(width, reach, place, depth_far, init, own_out, edge_out, depth, held, sems):
    rows, cols = depth.shape
    lane = lax.broadcasted_iota(jnp.int32, (rows, LANES), 1)
    copies = [pltpu.make_async_copy(depth_far, depth, sems.at[0])]
    for h, y in enumerate((place[4], 1 - place[4])):
        start = place[2] * (cols // 2) + (place[3] * 2 + y) * width
        after = lax.rem(start + width, cols)
        before = lax.rem(start - LANES + cols, cols)
        for i in range(4):
            ref = depth_far if i == 0 else init.at[i - 1]
            for k, (at, to, size) in enumerate(
                ((start, 0, width), (after, width, LANES), (before, width + LANES, LANES))
            ):
                copies.append(
                    pltpu.make_async_copy(
                        ref.at[:, pl.ds(pl.multiple_of(at, LANES), size)],
                        held.at[h, i, :, to : to + size],
                        sems.at[1 + (h * 4 + i) * 3 + k],
                    )
                )
    for copy in copies:
        copy.start()
    for copy in copies:
        copy.wait()
    for h, out in enumerate((own_out, edge_out)):
        for i in range(4):
            parts = [held[h, i, :, t * LANES : (t + 1) * LANES] for t in range(width // LANES)]
            after, before = held[h, i, :, width : width + LANES], held[h, i, :, width + LANES :]
            parts.append(jnp.where(lane < LANES - reach, after, before))
            for t, part in enumerate(parts):
                at = (4 * t + i) * rows
                out[at : at + rows, :] = part
    at = own_out.shape[0]
    for r in (*range(DEEP), *range(rows - DEEP, rows)):
        for t in range(cols // LANES):
            edge_out[at : at + 1, :] = depth[r : r + 1, t * LANES : (t + 1) * LANES]
            at += 1


def blend_body(nodes, depth_far, base_out, fk_out, depth_out, state, near, depth, sems):
    rows, cols = depth.shape
    copies = [pltpu.make_async_copy(nodes.at[:, f], near.at[f], sems.at[f]) for f in range(3)]
    copies.append(pltpu.make_async_copy(depth_far, depth, sems.at[3]))
    for copy in copies:
        copy.start()
    none = jnp.zeros((TILE, cols), jnp.float32)
    for f in range(3):
        copies[f].wait()
        n0, n1, n2 = near[f, 0], near[f, 1], near[f, 2]
        base_out[f] = (DT / 24.0) * (8.0 * n1 - 7.0 * n0 - n2)
        state[f, :rows, :] = (DT / 4.0) * (n0 - 2.0 * n1 + n2)
        state[f, rows:, :] = none
    copies[3].wait()
    half_depth = jnp.concatenate([0.5 * depth[...], none], axis=0)
    depth_out[...] = half_depth
    fk = tendency(tuple(state[f] for f in range(3)), half_depth)
    for f in range(3):
        fk_out[f] = fk[f]


def second_body(fk, bare, *rest):
    *edges, ffk_out, depth_out = rest
    rows, cols = bare.shape[0] - TILE, bare.shape[1]
    depth_out[...] = bare[...]
    for r in range(DEEP):
        below, above = rows + r, rows + TILE - DEEP + r
        if len(edges) == 2 or len(edges[0].shape) > 2:
            low, high = edges if len(edges) == 2 else (edges[0].at[0], edges[0].at[1])
            depth_out[below : below + 1, :] = 0.5 * low[r]
            depth_out[above : above + 1, :] = 0.5 * high[r]
            continue
        tiles = cols // LANES
        base = edges[0].shape[0] - 2 * DEEP * tiles
        for t in range(tiles):
            for to, at in ((below, base + r * tiles + t), (above, base + (DEEP + r) * tiles + t)):
                depth_out[to : to + 1, t * LANES : (t + 1) * LANES] = 0.5 * edges[0][at : at + 1, :]
    ffk = tendency(tuple(fk[f] for f in range(3)), depth_out[...])
    for f in range(3):
        ffk_out[f] = ffk[f]


def window(ref, lead, half):
    cols = ref.shape[-1]
    start = half * (cols // 2) + (cols - LANES)
    parts = [cut(ref, lead, lax.rem(start + t * LANES, cols)) for t in range(cols // 2 // LANES + 2)]
    return jnp.concatenate(parts, axis=1)


def fine_body(own_half, place, base, prev, init, fk, ffk, depth_ref, b_out, v_out):
    half = place[2] if own_half else 1 - place[2]
    first = place[0] == 1
    wide = fk.shape[1]
    half_depth = window(depth_ref, (), half)
    none = jnp.zeros((TILE, half_depth.shape[1]), jnp.float32)
    g = []
    for f in range(3):
        start = jnp.where(first, window(init, (f,), half), window(prev, (f,), half))
        g.append(jnp.concatenate([HALF * start + window(base, (f,), half), none], axis=0))
    u = tendency(tendency(tuple(g), half_depth), half_depth)
    fu = tendency(u, half_depth)
    for f in range(3):
        at = slice(f * wide, (f + 1) * wide)
        v = window(fk, (f,), half) + HALF * u[f]
        v_out[at, :] = v[:, LANES : v.shape[1] - LANES]
        b_out[at, :] = DT * (u[f] + (1.0 / 6.0) * (HALF * fu[f] + window(ffk, (f,), half)))


def spill_body(b_keep, b_give, v_keep, v_give, spill_out, v_spread, sems):
    wide = b_keep.shape[0] // 3
    rows = wide - TILE
    copies = [
        pltpu.make_async_copy(v.at[pl.ds(f * wide + rows, TILE), :], v_spread.at[h, f], sems.at[3 * h + f])
        for h, v in enumerate((v_keep, v_give))
        for f in range(3)
    ]
    for copy in copies:
        copy.start()
    for h, b in enumerate((b_keep, b_give)):
        inside = slice(LANES, b.shape[1] - LANES)
        for f in range(3):
            top = f * wide
            for side, spread, edge in ((0, wide - DEEP, 0), (1, rows, rows - 1)):
                for r in range(DEEP):
                    spill_out[side, h, DEEP * f + r] = b[top + spread + r : top + spread + r + 1, inside]
                spill_out[side, h, 9 + f] = b[top + edge : top + edge + 1, inside]
    for copy in copies:
        copy.wait()
    for h in range(2):
        for f in range(3):
            for side, spread in ((0, TILE - 2), (1, 0)):
                for r in range(2):
                    spill_out[side, h, 12 + 2 * f + r] = v_spread[h, f, spread + r : spread + r + 1, :]


def mend_body(place, *refs):
    far, edges, (b_out, v_far, v_out, *near, sems) = refs[:4], refs[4:-8], refs[-8:]
    low, high = (edges[0].at[0], edges[0].at[1]) if len(edges) == 1 else edges
    copies = [pltpu.make_async_copy(x, y, sems.at[i]) for i, (x, y) in enumerate(zip(far, near))]
    for i in (2, 3, 0, 1):
        copies[i].start()
    b_keep, b_give, v_keep, v_give = near
    copies[2].wait()
    copies[3].wait()
    rows = v_out.shape[1]
    wide = rows + TILE
    size = v_keep.shape[1]
    halves = ((place[2], b_keep, v_keep), (1 - place[2], b_give, v_give))
    for h, (half, _, v) in enumerate(halves):
        to = pl.ds(pl.multiple_of(half * size, LANES), size)
        for f in range(3):
            v_out[f, :, to] = v[f * wide : f * wide + rows, :]
            for r in range(2):
                for at, more in ((r, high), (rows - 2 + r, low)):
                    old = v[f * wide + at : f * wide + at + 1, :]
                    v_out[f, at : at + 1, to] = old + more[h, 12 + 2 * f + r]
    copy = pltpu.make_async_copy(v_out, v_far, sems.at[4])
    copy.start()
    copies[0].wait()
    copies[1].wait()
    for h, (half, b, _) in enumerate(halves):
        to = pl.ds(pl.multiple_of(half * size, LANES), size)
        inside = slice(LANES, LANES + size)
        for f in range(3):
            top = f * wide
            b_out[f, :, to] = b[top : top + wide, inside]
            adds = [(rows, 9 + f, low), (wide - 1, 9 + f, high)]
            for r in range(DEEP):
                adds += [(r, DEEP * f + r, high), (rows - DEEP + r, DEEP * f + r, low)]
            for at, i, more in adds:
                b_out[f, at : at + 1, to] = b[top + at : top + at + 1, inside] + more[h, i]
    copy.wait()


def pair_body(width, reach, count, place, depth_ref, got, *rest):
    near, far = rest[:count], rest[count + 1 : 2 * count + 1]
    msg_far, msg_out, sems = rest[count], rest[-2], rest[-1]
    owners = msg_out.shape[0]
    copies = [pltpu.make_async_copy(a, b, sems.at[owners + i]) for i, (a, b) in enumerate(zip(near, far))]
    for copy in copies:
        copy.start()
    keep = near[0]
    wide = keep.shape[0] // 3
    even = place[2] == 0
    step_depth = DT * window(depth_ref, (), place[2])
    own = tuple(keep[f * wide : (f + 1) * wide, :] for f in range(3))
    other = tuple(got[f * wide : (f + 1) * wide, :] for f in range(3))
    first = tuple(jnp.where(even, x, y) for x, y in zip(own, other))
    second = tuple(jnp.where(even, y, x) for x, y in zip(own, other))
    both = tuple(x + y for x, y in zip(second, stepped(first, step_depth)))
    for j in range(owners):
        for f in range(3):
            pack_block(both[f], f, j, width, reach, msg_out.at[j])
    copies.append(pltpu.make_async_copy(msg_out, msg_far, sems.at[0]))
    copies[-1].start()
    for copy in copies:
        copy.wait()


def pack_block(b, f, j, width, reach, out):
    rows, cols = b.shape
    at = LANES + j * width
    lane = lax.broadcasted_iota(jnp.int32, (rows, LANES), 1)
    if dense(width, reach, rows):
        small = lax.broadcasted_iota(jnp.int32, (TILE, LANES), 1)
        parts = width // LANES
        for t in range(parts):
            out[(f * parts + t) * rows : (f * parts + t + 1) * rows, :] = b[:, at + t * LANES : at + (t + 1) * LANES]
        after, before = at + width, at - LANES
        halo = jnp.where(lane < LANES // 2, b[:, after : after + LANES], b[:, before : before + LANES])
        put_halo(halo, f * rows // TILE, 3 * parts * rows, small, out)
        return
    span = out.shape[1]
    turned = rolled(b, -at, 1)
    parts = [turned[:, t : t + LANES] for t in range(0, span, LANES)]
    parts[-1] = jnp.where(lane < LANES - reach, parts[-1], turned[:, cols - LANES :])
    for t, part in enumerate(parts):
        out[f * rows : (f + 1) * rows, t * LANES : (t + 1) * LANES] = part


def put_halo(halo, tile, base, small, out):
    for i in range(halo.shape[0] // TILE):
        q = (tile + i) % 4
        at = base + (tile + i) // 4 * TILE
        moved = rolled(halo[i * TILE : (i + 1) * TILE], 16 + 32 * q, 1)
        if q:
            moved = jnp.where(small >= 32 * q, moved, out[at : at + TILE, :])
        out[at : at + TILE, :] = moved


def get_halo(source, tile, count, base):
    found = []
    for i in range(tile, tile + count):
        at = base + i // 4 * TILE
        found.append(rolled(source[at : at + TILE, :], -(16 + 32 * (i % 4)), 1))
    return jnp.concatenate(found, axis=0)


def block_of(message, f, rows, width, reach):
    if not dense(width, reach, rows):
        return message[f * rows : (f + 1) * rows, :]
    parts = width // LANES
    main = [message[(f * parts + t) * rows : (f * parts + t + 1) * rows, :] for t in range(parts)]
    return jnp.concatenate(main + [get_halo(message, f * rows // TILE, rows // TILE, 3 * parts * rows)], axis=1)


def joined(recv, slot, spaces, rows, width, reach):
    wide = rows + TILE
    fields = []
    for f in range(3):
        blocks = [block_of(recv.at[slot * spaces + y], f, wide, width, reach) for y in range(spaces)]
        row = lax.broadcasted_iota(jnp.int32, (TILE, blocks[0].shape[1]), 0)
        tiles = []
        for y in range(spaces):
            here = [blocks[y][t : t + TILE] for t in range(0, rows, TILE)]
            here[0] = here[0] + jnp.where(row < TILE // 2, blocks[(y - 1) % spaces][rows:], 0.0)
            here[-1] = here[-1] + jnp.where(row < TILE // 2, 0.0, blocks[(y + 1) % spaces][rows:])
            tiles += here
        fields.append(jnp.concatenate(tiles, axis=0))
    return tuple(fields)


def window_field(win, i, rows, place):
    if len(win) == 1:
        return jnp.concatenate([win[0][y, i * rows : (i + 1) * rows, :] for y in range(win[0].shape[0])], axis=0)
    own, theirs = (
        jnp.concatenate([part[at : at + rows, :] for at in range(i * rows, part.shape[0], 4 * rows)], axis=1)
        for part in (win[0], win[1].at[: win[0].shape[0]])
    )
    above = place[4] == 0
    return jnp.concatenate([jnp.where(above, own, theirs), jnp.where(above, theirs, own)], axis=0)


def two_steps(q, step_depth):
    return stepped(stepped(q, step_depth), step_depth)


def ahead_body(slots, rows, place, *rest):
    *win, out = rest
    step_depth = HALF * window_field(win, 0, rows, place)
    q = tuple(window_field(win, 1 + f, rows, place) for f in range(3))
    for _ in range(slots):
        q = two_steps(q, step_depth)
    for f in range(3):
        out[f] = q[f]


def total_body(spaces, rows, width, reach, place, recv, ahead, *rest):
    *win, total_out = rest
    slots = recv.shape[0] // spaces
    step_depth = HALF * window_field(win, 0, rows, place)
    q = joined(recv, 0, spaces, rows, width, reach)
    for slot in range(1, slots):
        b = joined(recv, slot, spaces, rows, width, reach)
        q = tuple(x + y for x, y in zip(b, two_steps(q, step_depth)))
    q = tuple(x + ahead[f] for f, x in enumerate(q))
    all_rows = rows * spaces
    if not dense(width, reach, rows):
        for f in range(3):
            total_out[f * all_rows : (f + 1) * all_rows, :] = q[f]
        return
    small = lax.broadcasted_iota(jnp.int32, (TILE, LANES), 1)
    parts = width // LANES
    for f in range(3):
        for t in range(parts):
            total_out[(f * parts + t) * all_rows : (f * parts + t + 1) * all_rows, :] = q[f][
                :, t * LANES : (t + 1) * LANES
            ]
        put_halo(q[f][:, width:], f * all_rows // TILE, 3 * parts * all_rows, small, total_out)


def chain_body(spaces, rows, width, reach, place, recv, carry, *rest):
    *win, msg_far, msg_out, sems = rest
    slots = recv.shape[0] // spaces
    all_rows = rows * spaces
    copies = []
    step_depth = HALF * window_field(win, 0, rows, place)
    lower = place[1] == 1
    q = tuple(
        jnp.where(lower, window_field(win, 1 + f, rows, place), block_of(carry, f, all_rows, width, reach))
        for f in range(3)
    )
    for slot in range(slots):
        for y in range(spaces):
            at = slot * spaces + y
            for f in range(3):
                here = q[f][:, :width]
                lo, hi = y * rows, (y + 1) * rows
                msg_out[at, f * rows : (f + 1) * rows, :] = here[lo:hi]
                for r, source in enumerate((hi, hi + 1, lo - 2, lo - 1)):
                    source %= all_rows
                    to = 3 * rows + 4 * f + r
                    msg_out[at, to : to + 1, :] = here[source : source + 1]
            msg_out[at, 3 * rows + 12 :, :] = jnp.zeros((4, width), jnp.float32)
            copies.append(pltpu.make_async_copy(msg_out.at[at], msg_far.at[at], sems.at[at]))
            copies[-1].start()
        if slot + 1 < slots:
            b = joined(recv, slot, spaces, rows, width, reach)
            q = tuple(x + y for x, y in zip(b, two_steps(q, step_depth)))
    for copy in copies:
        copy.wait()


def finish_body(near, place, *refs):
    if near:
        mine, b_far, b_lent, v_far, depth_ref, out, state, b_own, v_ref, made, sems = refs
        other = None
    else:
        mine, other, b_far, b_lent, v_far, depth_ref, _, out, state, b_own, v_ref, made, sems = refs
    rows = v_ref.shape[1]
    wide = rows + TILE
    half = depth_ref.shape[1] // 2
    ours, theirs = place[2] * half, (1 - place[2]) * half
    side = 2 * LANES
    if near:
        parts = [(ours, half, mine, 0)]
        pieces = [(LANES, half - 2 * LANES, ours + LANES)]
    else:
        parts = [(ours + half - side, side, mine, half - side), (theirs, half, other, 0), (ours, side, mine, 0)]
        pieces = [(LANES, LANES, ours + half - LANES), (side, half, theirs), (side + half, LANES, ours)]

    def at(start, size):
        return pl.ds(pl.multiple_of(start, LANES), size)

    fetches, local = [], 0
    for i, (start, size, source, first) in enumerate(parts):
        width = source.shape[2]
        here = slice(local, local + size)
        for k, (far, held) in enumerate(((b_far, b_own), (v_far, v_ref))):
            copy = pltpu.make_async_copy(far.at[:, :, at(start, size)], held.at[:, :, here], sems.at[2 * i + k])
            copy.start()
            fetches.append(copy)
        step = min(width, size)
        for c in range(0, size, step):
            j, off = (first + c) // width, (first + c) % width
            to = slice(local + c, local + c + step)
            for f in range(3):
                state[f, :rows, to] = source[j, f * rows : (f + 1) * rows, off : off + step]
                for r, row in enumerate((rows, rows + 1, wide - 2, wide - 1)):
                    line = 3 * rows + 4 * f + r
                    state[f, row : row + 1, to] = source[j, line : line + 1, off : off + step]
        local += size
    for f in range(3):
        state[f, rows + 2 : wide - 2, :] = jnp.zeros((TILE - 4, local), jnp.float32)

    def taken(ref, lead):
        return jnp.concatenate([cut(ref, lead, start, size) for start, size, _, _ in parts], axis=1)

    even = place[2] == 0
    step_depth = DT * taken(depth_ref, ())
    carried = tuple(state[f] for f in range(3))
    moved = stepped(carried, step_depth)
    for fetch in fetches:
        fetch.wait()
    after = tuple(jnp.where(even, b_own[f], taken(b_lent, (f,))) + x for f, x in enumerate(moved))
    last = stepped(after, step_depth)
    copies = []
    for f in range(3):
        begin = jnp.where(even, carried[f][:rows], after[f][:rows])
        end = jnp.where(even, after[f][:rows], b_own[f, :rows, :] + last[f][:rows])
        made[0, f] = begin
        made[1, f] = 0.5 * ((begin + end) - v_ref[f])
        made[2, f] = end
        for part in range(3):
            for i, (lo, size, to) in enumerate(pieces):
                copy = pltpu.make_async_copy(
                    made.at[part, f, :, lo : lo + size],
                    out.at[part, f, :, at(to, size)],
                    sems.at[6 + (3 * f + part) * 3 + i],
                )
                copy.start()
                copies.append(copy)
    for copy in copies:
        copy.wait()


def kernel(body, shapes, *args, scalars=0, far=(), far_out=(), near=(), near_out=(), **more):
    vmem = pl.BlockSpec(memory_space=pltpu.VMEM)
    hbm = pl.BlockSpec(memory_space=pltpu.HBM)
    smem = pl.BlockSpec(memory_space=pltpu.SMEM)
    many = isinstance(shapes, list)
    outs = []
    for i, shape in enumerate(shapes if many else [shapes]):
        make = pltpu.HBM if i in far_out else pltpu.VMEM if i in near_out else jax.ShapeDtypeStruct
        outs.append(make(shape, jnp.float32))
    placed = list(args)
    for held, space in ((far, pltpu.HBM), (near, pltpu.VMEM)):
        for i in held:
            placed[i] = pltpu.with_memory_space_constraint(args[i], space)
    specs = [hbm if i in far_out else vmem for i in range(len(outs))]
    return pl.pallas_call(
        body,
        out_shape=outs if many else outs[0],
        in_specs=[smem if i < scalars else hbm if i in far else vmem for i in range(len(args))],
        out_specs=specs if many else specs[0],
        compiler_params=pltpu.CompilerParams(vmem_limit_bytes=VMEM_BYTES),
        **more,
    )(*placed)


def swap_rows(edges):
    count = lax.axis_size("space")
    if count == 2:
        return (lax.ppermute(edges, "space", [(0, 1), (1, 0)]),)
    below = lax.ppermute(edges[0], "space", [((i + 1) % count, i) for i in range(count)])
    above = lax.ppermute(edges[1], "space", [(i, (i + 1) % count) for i in range(count)])
    return below, above


def per_device(fine_nodes, init_state, mean_depth):
    nodes = fine_nodes[0]
    rows, cols = nodes.shape[-2:]
    outer, inner, spaces = lax.axis_size("outer"), lax.axis_size("inner"), lax.axis_size("space")
    group = ("inner", "space")
    owners = inner * spaces
    half = cols // 2
    width = half // owners
    slices = outer * inner * 2
    reach = slices - 2
    span = -(-(width + 2 * reach) // LANES) * LANES
    wide = rows + TILE
    at_outer, at_inner, at_core, at_space = (
        lax.axis_index(name) for name in ("outer", "inner", "core", "space")
    )
    first = at_outer + at_inner + at_core == 0
    place = jnp.stack([first.astype(jnp.int32), (at_outer == 0).astype(jnp.int32), at_core, at_inner, at_space])
    state, spread = (3, rows, cols), (3, wide, cols)
    swapped = [(0, 1), (1, 0)]
    plan = (spaces, rows, width, reach)

    last = kernel(last_body, state, nodes, far=(0,), scratch_shapes=[pltpu.SemaphoreType.DMA])
    prev = lax.ppermute(last, ("outer", "inner", "core"), [(i, i + 1) for i in range(slices - 1)])

    if spaces == 2 and dense(width, reach, rows):
        own_rows = 4 * rows * span // LANES
        own, edges = kernel(
            functools.partial(prepare_body, width, reach),
            [(own_rows, LANES), (own_rows + 2 * DEEP * cols // LANES, LANES)],
            place, mean_depth, init_state, scalars=1, far=(1, 2),
            scratch_shapes=[
                pltpu.VMEM((rows, cols), jnp.float32),
                pltpu.VMEM((2, 4, rows, width + 2 * LANES), jnp.float32),
                pltpu.SemaphoreType.DMA((25,)),
            ],
        )
        edges = lax.ppermute(edges, "space", swapped)
        windows, edges = (own, edges), (edges,)
    else:
        windows = all_windows(mean_depth, init_state, at_core * half, at_inner, spaces, width, reach, span)
        windows = (lax.all_to_all(windows, "space", 0, 0, tiled=True),)
        edges = jnp.stack([mean_depth[:DEEP, None], mean_depth[rows - DEEP :, None]])
        edges = swap_rows(edges)

    base, fk, bare = kernel(
        blend_body, [state, spread, (wide, cols)], nodes, mean_depth, far=(0, 1),
        scratch_shapes=[
            pltpu.VMEM(spread, jnp.float32),
            pltpu.VMEM((3,) + state, jnp.float32),
            pltpu.VMEM((rows, cols), jnp.float32),
            pltpu.SemaphoreType.DMA((4,)),
        ],
    )
    ffk, depth = kernel(second_body, [spread, (wide, cols)], fk, bare, *edges)
    fine_shapes = [(3 * wide, half + 2 * LANES), (3 * wide, half)]
    fine_args = (place, base, prev, init_state, fk, ffk, depth)
    give, v_give = kernel(functools.partial(fine_body, False), fine_shapes, *fine_args, scalars=1)
    got = lax.ppermute(give, "core", swapped)
    keep, v_keep = kernel(functools.partial(fine_body, True), fine_shapes, *fine_args, scalars=1)
    tight = packed_rows(wide, width, reach)
    msg_shape = (owners, tight, LANES) if tight else (owners, 3 * wide, span)
    parts = (keep, give, v_keep, v_give)
    msgs, *far_parts = kernel(
        functools.partial(pair_body, width, reach, len(parts)), [msg_shape] + [x.shape for x in parts],
        place, depth, got, *parts, scalars=1, far_out=range(1 + len(parts)),
        scratch_shapes=[pltpu.VMEM(msg_shape, jnp.float32), pltpu.SemaphoreType.DMA((owners + len(parts),))],
    )
    recv = lax.all_to_all(msgs, group, 0, 0, tiled=True)
    spill = kernel(
        spill_body, (2, 2, 18, 1, half), keep, give, *far_parts[2:], far=(2, 3),
        scratch_shapes=[pltpu.VMEM((2, 3, TILE, half), jnp.float32), pltpu.SemaphoreType.DMA((6,))],
    )
    ahead = kernel(
        functools.partial(ahead_body, inner, rows), (3, spaces * rows, span),
        place, *windows, scalars=1,
    )
    spill = swap_rows(spill)
    b_own, vee = kernel(
        mend_body, [spread, state], place, *far_parts, *spill, scalars=1,
        far=range(1, 5), far_out=(1,),
        scratch_shapes=[pltpu.VMEM(state, jnp.float32)]
        + [pltpu.VMEM(x.shape, jnp.float32) for x in far_parts]
        + [pltpu.SemaphoreType.DMA((5,))],
    )
    b_lent = lax.ppermute(b_own, "core", [(0, 1)])

    tight = packed_rows(spaces * rows, width, reach)
    total_shape = (tight, LANES) if tight else (3 * spaces * rows, span)
    total = kernel(functools.partial(total_body, *plan), total_shape, place, recv, ahead, *windows, scalars=1)
    carry = lax.ppermute(total, "outer", [(i, i + 1) for i in range(outer - 1)])
    back = kernel(
        functools.partial(chain_body, *plan), (owners, 3 * rows + 2 * TILE, width),
        place, recv, carry, *windows, scalars=1, far_out=(0,),
        scratch_shapes=[
            pltpu.VMEM((owners, 3 * rows + 2 * TILE, width), jnp.float32),
            pltpu.SemaphoreType.DMA((owners,)),
        ],
    )
    mine = lax.all_to_all(back, group, 0, 0, tiled=True)
    if width % LANES:
        mine = mine.transpose(1, 0, 2).reshape(1, 3 * rows + 2 * TILE, half)
    other = lax.ppermute(mine, "core", swapped)

    def finish(near, cols_held, *args, **more):
        held = (3, wide, cols_held)
        return kernel(
            functools.partial(finish_body, near), (3,) + state,
            place, *args, scalars=1, far_out=(0,),
            scratch_shapes=[
                pltpu.VMEM(held, jnp.float32),
                pltpu.VMEM(held, jnp.float32),
                pltpu.VMEM((3, rows, cols_held), jnp.float32),
                pltpu.VMEM((3, 3, rows, cols_held), jnp.float32),
                pltpu.SemaphoreType.DMA((33,)),
            ],
            **more,
        )

    out = finish(True, half, mine, b_own, b_lent, vee, depth, far=(2, 4))
    out = finish(
        False, half + 4 * LANES, mine, other, b_own, b_lent, vee, depth, out,
        far=(3, 5, 7), input_output_aliases={7: 0},
    )
    return out[None]


def all_windows(depth, init, offset, at_inner, spaces, width, reach, span):
    fixed = jnp.concatenate([depth[None], init], axis=0)
    _, rows, cols = fixed.shape
    onward = jnp.concatenate([fixed, fixed[..., :span]], axis=-1)
    behind = jnp.concatenate([fixed[..., cols - span :], fixed], axis=-1)
    lane = lax.broadcasted_iota(jnp.int32, (4, rows, span), 2)
    windows = []
    for y in range(spaces):
        start = offset + (at_inner * spaces + y) * width
        ahead = lax.dynamic_slice_in_dim(onward, start, span, axis=2)
        back = lax.dynamic_slice_in_dim(behind, start, span, axis=2)
        windows.append(jnp.where(lane < span - reach, ahead, back).reshape(4 * rows, span))
    return jnp.stack(windows)


def solution(mesh):
    slices, spaces = mesh.shape["tm"], mesh.shape["space"]
    split = Mesh(mesh.devices.reshape(2, slices // 4, 2, spaces), ("outer", "inner", "core", "space"))
    nodes = P(("outer", "inner", "core"), None, None, "space", None)
    return jax.shard_map(
        per_device,
        mesh=split,
        in_specs=(nodes, P(None, "space", None), P("space", None)),
        out_specs=nodes,
        check_vma=False,
    )
```

```python
import functools

import jax
import jax.numpy as jnp
from jax import lax
from jax.experimental import pallas as pl
from jax.experimental.pallas import tpu as pltpu
from jax.sharding import Mesh
from jax.sharding import PartitionSpec as P


DT = 0.3
HALF = 0.5 * DT
NU = 1.0 / 3.0
FC = 0.5
DEEP = 3
TILE = 8
LANES = 128
VMEM_BYTES = 20 * 1024 * 1024


def rolled(x, by, axis):
    return pltpu.roll(x, by % x.shape[axis], axis)


def advanced(q, flow, scale, keep):
    height, east, north = q
    soft, slope, turn = scale * NU, scale * 0.5, scale * FC
    stay = keep - 4.0 * soft
    h_soft, e_soft, n_soft = soft * height, soft * east, soft * north
    h_slope = slope * height
    flow_e, flow_n = flow * east, flow * north
    new_h = (
        (rolled(h_soft + flow_e, 1, 1) + rolled(h_soft - flow_e, -1, 1))
        + (rolled(h_soft + flow_n, 1, 0) + rolled(h_soft - flow_n, -1, 0))
        + stay * height
    )
    new_e = (
        (rolled(e_soft + h_slope, 1, 1) + rolled(e_soft - h_slope, -1, 1))
        + (rolled(e_soft, 1, 0) + rolled(e_soft, -1, 0))
        + (stay * east + turn * north)
    )
    new_n = (
        (rolled(n_soft, 1, 1) + rolled(n_soft, -1, 1))
        + (rolled(n_soft + h_slope, 1, 0) + rolled(n_soft - h_slope, -1, 0))
        + (stay * north - turn * east)
    )
    return new_h, new_e, new_n


def tendency(q, half_depth):
    return advanced(q, half_depth, 1.0, 0.0)


def stepped(q, step_depth):
    return advanced(q, step_depth, DT, 1.0)


def dense(width, reach, rows):
    return width % LANES == 0 and 2 * reach <= 32 and rows % TILE == 0


def packed_rows(rows, width, reach):
    if not dense(width, reach, rows):
        return None
    tiles = 3 * rows // TILE
    return 3 * rows * (width // LANES) + TILE * -(-tiles // 4)


def cut(ref, lead, at, size=LANES):
    return ref[lead + (slice(None), pl.ds(pl.multiple_of(at, LANES), size))]


def last_body(place, nodes, soon_out, late_out, sems):
    cols = nodes.shape[-1]
    half = cols // 2
    start = place[2] * half
    before, after = lax.rem(start + (cols - LANES), cols), lax.rem(start + half, cols)
    cuts = (
        (before, LANES, soon_out, 0),
        (start, half, soon_out, LANES),
        (after, LANES, soon_out, LANES + half),
        (after, half, late_out, 0),
    )
    copies = []
    for i, (at, size, out, to) in enumerate(cuts):
        source = nodes.at[2, :, :, pl.ds(pl.multiple_of(at, LANES), size)]
        copies.append(pltpu.make_async_copy(source, out.at[:, :, to : to + size], sems.at[i]))
        copies[-1].start()
    for copy in copies:
        copy.wait()


def prepare_body(width, reach, place, depth_far, init, own_out, edge_out, depth, held, sems):
    rows, cols = depth.shape
    lane = lax.broadcasted_iota(jnp.int32, (rows, LANES), 1)
    copies = [pltpu.make_async_copy(depth_far, depth, sems.at[0])]
    for h, y in enumerate((place[4], 1 - place[4])):
        start = place[2] * (cols // 2) + (place[3] * 2 + y) * width
        after = lax.rem(start + width, cols)
        before = lax.rem(start - LANES + cols, cols)
        for i in range(4):
            ref = depth_far if i == 0 else init.at[i - 1]
            for k, (at, to, size) in enumerate(
                ((start, 0, width), (after, width, LANES), (before, width + LANES, LANES))
            ):
                copies.append(
                    pltpu.make_async_copy(
                        ref.at[:, pl.ds(pl.multiple_of(at, LANES), size)],
                        held.at[h, i, :, to : to + size],
                        sems.at[1 + (h * 4 + i) * 3 + k],
                    )
                )
    for copy in copies:
        copy.start()
    for copy in copies:
        copy.wait()
    for h, out in enumerate((own_out, edge_out)):
        for i in range(4):
            parts = [held[h, i, :, t * LANES : (t + 1) * LANES] for t in range(width // LANES)]
            after, before = held[h, i, :, width : width + LANES], held[h, i, :, width + LANES :]
            parts.append(jnp.where(lane < LANES - reach, after, before))
            for t, part in enumerate(parts):
                at = (4 * t + i) * rows
                out[at : at + rows, :] = part
    at = own_out.shape[0]
    for r in (*range(DEEP), *range(rows - DEEP, rows)):
        for t in range(cols // LANES):
            edge_out[at : at + 1, :] = depth[r : r + 1, t * LANES : (t + 1) * LANES]
            at += 1


def blend_body(nodes, depth_far, base_out, fk_out, depth_out, state, near, depth, sems):
    rows, cols = depth.shape
    copies = [pltpu.make_async_copy(nodes.at[:, f], near.at[f], sems.at[f]) for f in range(3)]
    copies.append(pltpu.make_async_copy(depth_far, depth, sems.at[3]))
    for copy in copies:
        copy.start()
    none = jnp.zeros((TILE, cols), jnp.float32)
    for f in range(3):
        copies[f].wait()
        n0, n1, n2 = near[f, 0], near[f, 1], near[f, 2]
        base_out[f] = (DT / 24.0) * (8.0 * n1 - 7.0 * n0 - n2)
        state[f, :rows, :] = (DT / 4.0) * (n0 - 2.0 * n1 + n2)
        state[f, rows:, :] = none
    copies[3].wait()
    half_depth = jnp.concatenate([0.5 * depth[...], none], axis=0)
    depth_out[...] = half_depth
    fk = tendency(tuple(state[f] for f in range(3)), half_depth)
    for f in range(3):
        fk_out[f] = fk[f]


def second_body(fk, bare, *rest):
    *edges, ffk_out, depth_out = rest
    rows, cols = bare.shape[0] - TILE, bare.shape[1]
    depth_out[...] = bare[...]
    for r in range(DEEP):
        below, above = rows + r, rows + TILE - DEEP + r
        if len(edges) == 2 or len(edges[0].shape) > 2:
            low, high = edges if len(edges) == 2 else (edges[0].at[0], edges[0].at[1])
            depth_out[below : below + 1, :] = 0.5 * low[r]
            depth_out[above : above + 1, :] = 0.5 * high[r]
            continue
        tiles = cols // LANES
        base = edges[0].shape[0] - 2 * DEEP * tiles
        for t in range(tiles):
            for to, at in ((below, base + r * tiles + t), (above, base + (DEEP + r) * tiles + t)):
                depth_out[to : to + 1, t * LANES : (t + 1) * LANES] = 0.5 * edges[0][at : at + 1, :]
    ffk = tendency(tuple(fk[f] for f in range(3)), depth_out[...])
    for f in range(3):
        ffk_out[f] = ffk[f]


def window(ref, lead, half):
    cols = ref.shape[-1]
    start = half * (cols // 2) + (cols - LANES)
    parts = [cut(ref, lead, lax.rem(start + t * LANES, cols)) for t in range(cols // 2 // LANES + 2)]
    return jnp.concatenate(parts, axis=1)


def fine_body(own_half, place, base, init, fk, ffk, depth_ref, prev, *rest):
    *late, b_out, v_out = rest
    half = place[2] if own_half else 1 - place[2]
    first = place[0] == 1
    wide = fk.shape[1]
    half_depth = window(depth_ref, (), half)
    none = jnp.zeros((TILE, half_depth.shape[1]), jnp.float32)
    g = []
    for f in range(3):
        before = prev[f]
        if own_half:
            size = late[0].shape[2]
            before = jnp.concatenate([before[:, size : size + LANES], late[0][f], before[:, LANES : 2 * LANES]], axis=1)
        start = jnp.where(first, window(init, (f,), half), before)
        g.append(jnp.concatenate([HALF * start + window(base, (f,), half), none], axis=0))
    u = tendency(tendency(tuple(g), half_depth), half_depth)
    fu = tendency(u, half_depth)
    for f in range(3):
        at = slice(f * wide, (f + 1) * wide)
        v = window(fk, (f,), half) + HALF * u[f]
        v_out[at, :] = v[:, LANES : v.shape[1] - LANES]
        b_out[at, :] = DT * (u[f] + (1.0 / 6.0) * (HALF * fu[f] + window(ffk, (f,), half)))


def spill_body(b_keep, b_give, v_keep, v_give, spill_out, v_spread, sems):
    wide = b_keep.shape[0] // 3
    rows = wide - TILE
    copies = [
        pltpu.make_async_copy(v.at[pl.ds(f * wide + rows, TILE), :], v_spread.at[h, f], sems.at[3 * h + f])
        for h, v in enumerate((v_keep, v_give))
        for f in range(3)
    ]
    for copy in copies:
        copy.start()
    for h, b in enumerate((b_keep, b_give)):
        inside = slice(LANES, b.shape[1] - LANES)
        for f in range(3):
            top = f * wide
            for side, spread, edge in ((0, wide - DEEP, 0), (1, rows, rows - 1)):
                for r in range(DEEP):
                    spill_out[side, h, DEEP * f + r] = b[top + spread + r : top + spread + r + 1, inside]
                spill_out[side, h, 9 + f] = b[top + edge : top + edge + 1, inside]
    for copy in copies:
        copy.wait()
    for h in range(2):
        for f in range(3):
            for side, spread in ((0, TILE - 2), (1, 0)):
                for r in range(2):
                    spill_out[side, h, 12 + 2 * f + r] = v_spread[h, f, spread + r : spread + r + 1, :]


def mend_body(place, *refs):
    far, edges, (b_out, v_far, v_out, *near, sems) = refs[:4], refs[4:-8], refs[-8:]
    low, high = (edges[0].at[0], edges[0].at[1]) if len(edges) == 1 else edges
    copies = [pltpu.make_async_copy(x, y, sems.at[i]) for i, (x, y) in enumerate(zip(far, near))]
    for i in (2, 3, 0, 1):
        copies[i].start()
    b_keep, b_give, v_keep, v_give = near
    copies[2].wait()
    copies[3].wait()
    rows = v_out.shape[1]
    wide = rows + TILE
    size = v_keep.shape[1]
    halves = ((place[2], b_keep, v_keep), (1 - place[2], b_give, v_give))
    for h, (half, _, v) in enumerate(halves):
        to = pl.ds(pl.multiple_of(half * size, LANES), size)
        for f in range(3):
            v_out[f, :, to] = v[f * wide : f * wide + rows, :]
            for r in range(2):
                for at, more in ((r, high), (rows - 2 + r, low)):
                    old = v[f * wide + at : f * wide + at + 1, :]
                    v_out[f, at : at + 1, to] = old + more[h, 12 + 2 * f + r]
    copy = pltpu.make_async_copy(v_out, v_far, sems.at[4])
    copy.start()
    copies[0].wait()
    copies[1].wait()
    for h, (half, b, _) in enumerate(halves):
        to = pl.ds(pl.multiple_of(half * size, LANES), size)
        inside = slice(LANES, LANES + size)
        for f in range(3):
            top = f * wide
            b_out[f, :, to] = b[top : top + wide, inside]
            adds = [(rows, 9 + f, low), (wide - 1, 9 + f, high)]
            for r in range(DEEP):
                adds += [(r, DEEP * f + r, high), (rows - DEEP + r, DEEP * f + r, low)]
            for at, i, more in adds:
                b_out[f, at : at + 1, to] = b[top + at : top + at + 1, inside] + more[h, i]
    copy.wait()


def pair_body(width, reach, count, place, depth_ref, got, *rest):
    near, far = rest[:count], rest[count + 1 : 2 * count + 1]
    msg_far, msg_out, sems = rest[count], rest[-2], rest[-1]
    owners = msg_out.shape[0]
    copies = [pltpu.make_async_copy(a, b, sems.at[owners + i]) for i, (a, b) in enumerate(zip(near, far))]
    for copy in copies:
        copy.start()
    keep = near[0]
    wide = keep.shape[0] // 3
    even = place[2] == 0
    step_depth = DT * window(depth_ref, (), place[2])
    own = tuple(keep[f * wide : (f + 1) * wide, :] for f in range(3))
    other = tuple(got[f * wide : (f + 1) * wide, :] for f in range(3))
    first = tuple(jnp.where(even, x, y) for x, y in zip(own, other))
    second = tuple(jnp.where(even, y, x) for x, y in zip(own, other))
    both = tuple(x + y for x, y in zip(second, stepped(first, step_depth)))
    for j in range(owners):
        for f in range(3):
            pack_block(both[f], f, j, width, reach, msg_out.at[j])
    copies.append(pltpu.make_async_copy(msg_out, msg_far, sems.at[0]))
    copies[-1].start()
    for copy in copies:
        copy.wait()


def pack_block(b, f, j, width, reach, out):
    rows, cols = b.shape
    at = LANES + j * width
    lane = lax.broadcasted_iota(jnp.int32, (rows, LANES), 1)
    if dense(width, reach, rows):
        small = lax.broadcasted_iota(jnp.int32, (TILE, LANES), 1)
        parts = width // LANES
        for t in range(parts):
            out[(f * parts + t) * rows : (f * parts + t + 1) * rows, :] = b[:, at + t * LANES : at + (t + 1) * LANES]
        after, before = at + width, at - LANES
        halo = jnp.where(lane < LANES // 2, b[:, after : after + LANES], b[:, before : before + LANES])
        put_halo(halo, f * rows // TILE, 3 * parts * rows, small, out)
        return
    span = out.shape[1]
    turned = rolled(b, -at, 1)
    parts = [turned[:, t : t + LANES] for t in range(0, span, LANES)]
    parts[-1] = jnp.where(lane < LANES - reach, parts[-1], turned[:, cols - LANES :])
    for t, part in enumerate(parts):
        out[f * rows : (f + 1) * rows, t * LANES : (t + 1) * LANES] = part


def put_halo(halo, tile, base, small, out):
    for i in range(halo.shape[0] // TILE):
        q = (tile + i) % 4
        at = base + (tile + i) // 4 * TILE
        moved = rolled(halo[i * TILE : (i + 1) * TILE], 16 + 32 * q, 1)
        if q:
            moved = jnp.where(small >= 32 * q, moved, out[at : at + TILE, :])
        out[at : at + TILE, :] = moved


def get_halo(source, tile, count, base):
    found = []
    for i in range(tile, tile + count):
        at = base + i // 4 * TILE
        found.append(rolled(source[at : at + TILE, :], -(16 + 32 * (i % 4)), 1))
    return jnp.concatenate(found, axis=0)


def block_of(message, f, rows, width, reach):
    if not dense(width, reach, rows):
        return message[f * rows : (f + 1) * rows, :]
    parts = width // LANES
    main = [message[(f * parts + t) * rows : (f * parts + t + 1) * rows, :] for t in range(parts)]
    return jnp.concatenate(main + [get_halo(message, f * rows // TILE, rows // TILE, 3 * parts * rows)], axis=1)


def joined(recv, slot, spaces, rows, width, reach):
    wide = rows + TILE
    fields = []
    for f in range(3):
        blocks = [block_of(recv.at[slot * spaces + y], f, wide, width, reach) for y in range(spaces)]
        row = lax.broadcasted_iota(jnp.int32, (TILE, blocks[0].shape[1]), 0)
        tiles = []
        for y in range(spaces):
            here = [blocks[y][t : t + TILE] for t in range(0, rows, TILE)]
            here[0] = here[0] + jnp.where(row < TILE // 2, blocks[(y - 1) % spaces][rows:], 0.0)
            here[-1] = here[-1] + jnp.where(row < TILE // 2, 0.0, blocks[(y + 1) % spaces][rows:])
            tiles += here
        fields.append(jnp.concatenate(tiles, axis=0))
    return tuple(fields)


def window_field(win, i, rows, place):
    if len(win) == 1:
        return jnp.concatenate([win[0][y, i * rows : (i + 1) * rows, :] for y in range(win[0].shape[0])], axis=0)
    own, theirs = (
        jnp.concatenate([part[at : at + rows, :] for at in range(i * rows, part.shape[0], 4 * rows)], axis=1)
        for part in (win[0], win[1].at[: win[0].shape[0]])
    )
    above = place[4] == 0
    return jnp.concatenate([jnp.where(above, own, theirs), jnp.where(above, theirs, own)], axis=0)


def two_steps(q, step_depth):
    return stepped(stepped(q, step_depth), step_depth)


def ahead_body(slots, rows, place, *rest):
    *win, out = rest
    step_depth = HALF * window_field(win, 0, rows, place)
    q = tuple(window_field(win, 1 + f, rows, place) for f in range(3))
    for _ in range(slots):
        q = two_steps(q, step_depth)
    for f in range(3):
        out[f] = q[f]


def total_body(spaces, rows, width, reach, place, recv, ahead, *rest):
    *win, total_out = rest
    slots = recv.shape[0] // spaces
    step_depth = HALF * window_field(win, 0, rows, place)
    q = joined(recv, 0, spaces, rows, width, reach)
    for slot in range(1, slots):
        b = joined(recv, slot, spaces, rows, width, reach)
        q = tuple(x + y for x, y in zip(b, two_steps(q, step_depth)))
    q = tuple(x + ahead[f] for f, x in enumerate(q))
    all_rows = rows * spaces
    if not dense(width, reach, rows):
        for f in range(3):
            total_out[f * all_rows : (f + 1) * all_rows, :] = q[f]
        return
    small = lax.broadcasted_iota(jnp.int32, (TILE, LANES), 1)
    parts = width // LANES
    for f in range(3):
        for t in range(parts):
            total_out[(f * parts + t) * all_rows : (f * parts + t + 1) * all_rows, :] = q[f][
                :, t * LANES : (t + 1) * LANES
            ]
        put_halo(q[f][:, width:], f * all_rows // TILE, 3 * parts * all_rows, small, total_out)


def chain_body(spaces, rows, width, reach, place, recv, carry, *rest):
    *win, msg_far, msg_out, sems = rest
    slots = recv.shape[0] // spaces
    all_rows = rows * spaces
    copies = []
    step_depth = HALF * window_field(win, 0, rows, place)
    lower = place[1] == 1
    q = tuple(
        jnp.where(lower, window_field(win, 1 + f, rows, place), block_of(carry, f, all_rows, width, reach))
        for f in range(3)
    )
    for slot in range(slots):
        for y in range(spaces):
            at = slot * spaces + y
            for f in range(3):
                here = q[f][:, :width]
                lo, hi = y * rows, (y + 1) * rows
                msg_out[at, f * rows : (f + 1) * rows, :] = here[lo:hi]
                for r, source in enumerate((hi, hi + 1, lo - 2, lo - 1)):
                    source %= all_rows
                    to = 3 * rows + 4 * f + r
                    msg_out[at, to : to + 1, :] = here[source : source + 1]
            msg_out[at, 3 * rows + 12 :, :] = jnp.zeros((4, width), jnp.float32)
            copies.append(pltpu.make_async_copy(msg_out.at[at], msg_far.at[at], sems.at[at]))
            copies[-1].start()
        if slot + 1 < slots:
            b = joined(recv, slot, spaces, rows, width, reach)
            q = tuple(x + y for x, y in zip(b, two_steps(q, step_depth)))
    for copy in copies:
        copy.wait()


def finish_body(near, place, *refs):
    if near:
        mine, b_far, b_lent, v_far, depth_ref, out, state, b_own, v_ref, made, sems = refs
        other = None
    else:
        mine, other, b_far, b_lent, v_far, depth_ref, _, out, state, b_own, v_ref, made, sems = refs
    rows = v_ref.shape[1]
    wide = rows + TILE
    half = depth_ref.shape[1] // 2
    ours, theirs = place[2] * half, (1 - place[2]) * half
    side = 2 * LANES
    if near:
        parts = [(ours, half, mine, 0)]
        pieces = [(LANES, half - 2 * LANES, ours + LANES)]
    else:
        parts = [(ours + half - side, side, mine, half - side), (theirs, half, other, 0), (ours, side, mine, 0)]
        pieces = [(LANES, LANES, ours + half - LANES), (side, half, theirs), (side + half, LANES, ours)]

    def at(start, size):
        return pl.ds(pl.multiple_of(start, LANES), size)

    fetches, local = [], 0
    for i, (start, size, source, first) in enumerate(parts):
        width = source.shape[2]
        here = slice(local, local + size)
        for k, (far, held) in enumerate(((b_far, b_own), (v_far, v_ref))):
            copy = pltpu.make_async_copy(far.at[:, :, at(start, size)], held.at[:, :, here], sems.at[2 * i + k])
            copy.start()
            fetches.append(copy)
        step = min(width, size)
        for c in range(0, size, step):
            j, off = (first + c) // width, (first + c) % width
            to = slice(local + c, local + c + step)
            for f in range(3):
                state[f, :rows, to] = source[j, f * rows : (f + 1) * rows, off : off + step]
                for r, row in enumerate((rows, rows + 1, wide - 2, wide - 1)):
                    line = 3 * rows + 4 * f + r
                    state[f, row : row + 1, to] = source[j, line : line + 1, off : off + step]
        local += size
    for f in range(3):
        state[f, rows + 2 : wide - 2, :] = jnp.zeros((TILE - 4, local), jnp.float32)

    def taken(ref, lead):
        return jnp.concatenate([cut(ref, lead, start, size) for start, size, _, _ in parts], axis=1)

    even = place[2] == 0
    step_depth = DT * taken(depth_ref, ())
    carried = tuple(state[f] for f in range(3))
    moved = stepped(carried, step_depth)
    for fetch in fetches:
        fetch.wait()
    after = tuple(jnp.where(even, b_own[f], taken(b_lent, (f,))) + x for f, x in enumerate(moved))
    last = stepped(after, step_depth)
    copies = []
    for f in range(3):
        begin = jnp.where(even, carried[f][:rows], after[f][:rows])
        end = jnp.where(even, after[f][:rows], b_own[f, :rows, :] + last[f][:rows])
        made[0, f] = begin
        made[1, f] = 0.5 * ((begin + end) - v_ref[f])
        made[2, f] = end
        for part in range(3):
            for i, (lo, size, to) in enumerate(pieces):
                copy = pltpu.make_async_copy(
                    made.at[part, f, :, lo : lo + size],
                    out.at[part, f, :, at(to, size)],
                    sems.at[6 + (3 * f + part) * 3 + i],
                )
                copy.start()
                copies.append(copy)
    for copy in copies:
        copy.wait()


def kernel(body, shapes, *args, scalars=0, far=(), far_out=(), near=(), near_out=(), **more):
    vmem = pl.BlockSpec(memory_space=pltpu.VMEM)
    hbm = pl.BlockSpec(memory_space=pltpu.HBM)
    smem = pl.BlockSpec(memory_space=pltpu.SMEM)
    many = isinstance(shapes, list)
    outs = []
    for i, shape in enumerate(shapes if many else [shapes]):
        make = pltpu.HBM if i in far_out else pltpu.VMEM if i in near_out else jax.ShapeDtypeStruct
        outs.append(make(shape, jnp.float32))
    placed = list(args)
    for held, space in ((far, pltpu.HBM), (near, pltpu.VMEM)):
        for i in held:
            placed[i] = pltpu.with_memory_space_constraint(args[i], space)
    specs = [hbm if i in far_out else vmem for i in range(len(outs))]
    return pl.pallas_call(
        body,
        out_shape=outs if many else outs[0],
        in_specs=[smem if i < scalars else hbm if i in far else vmem for i in range(len(args))],
        out_specs=specs if many else specs[0],
        compiler_params=pltpu.CompilerParams(vmem_limit_bytes=VMEM_BYTES),
        **more,
    )(*placed)


def swap_rows(edges):
    count = lax.axis_size("space")
    if count == 2:
        return (lax.ppermute(edges, "space", [(0, 1), (1, 0)]),)
    below = lax.ppermute(edges[0], "space", [((i + 1) % count, i) for i in range(count)])
    above = lax.ppermute(edges[1], "space", [(i, (i + 1) % count) for i in range(count)])
    return below, above


def per_device(fine_nodes, init_state, mean_depth):
    nodes = fine_nodes[0]
    rows, cols = nodes.shape[-2:]
    outer, inner, spaces = lax.axis_size("outer"), lax.axis_size("inner"), lax.axis_size("space")
    group = ("inner", "space")
    owners = inner * spaces
    half = cols // 2
    width = half // owners
    slices = outer * inner * 2
    reach = slices - 2
    span = -(-(width + 2 * reach) // LANES) * LANES
    wide = rows + TILE
    at_outer, at_inner, at_core, at_space = (
        lax.axis_index(name) for name in ("outer", "inner", "core", "space")
    )
    first = at_outer + at_inner + at_core == 0
    place = jnp.stack([first.astype(jnp.int32), (at_outer == 0).astype(jnp.int32), at_core, at_inner, at_space])
    state, spread = (3, rows, cols), (3, wide, cols)
    swapped = [(0, 1), (1, 0)]
    plan = (spaces, rows, width, reach)

    soon, late = kernel(
        last_body, [(3, rows, half + 2 * LANES), (3, rows, half)], place, nodes, scalars=1, far=(1,),
        scratch_shapes=[pltpu.SemaphoreType.DMA((4,))],
    )
    onward = [(i, i + 1) for i in range(slices - 1)]
    prev = lax.ppermute(soon, ("outer", "inner", "core"), onward)
    prev_late = lax.ppermute(late, ("outer", "inner", "core"), onward)

    if spaces == 2 and dense(width, reach, rows):
        own_rows = 4 * rows * span // LANES
        own, edges = kernel(
            functools.partial(prepare_body, width, reach),
            [(own_rows, LANES), (own_rows + 2 * DEEP * cols // LANES, LANES)],
            place, mean_depth, init_state, scalars=1, far=(1, 2),
            scratch_shapes=[
                pltpu.VMEM((rows, cols), jnp.float32),
                pltpu.VMEM((2, 4, rows, width + 2 * LANES), jnp.float32),
                pltpu.SemaphoreType.DMA((25,)),
            ],
        )
        edges = lax.ppermute(edges, "space", swapped)
        windows, edges = (own, edges), (edges,)
    else:
        windows = all_windows(mean_depth, init_state, at_core * half, at_inner, spaces, width, reach, span)
        windows = (lax.all_to_all(windows, "space", 0, 0, tiled=True),)
        edges = jnp.stack([mean_depth[:DEEP, None], mean_depth[rows - DEEP :, None]])
        edges = swap_rows(edges)

    base, fk, bare = kernel(
        blend_body, [state, spread, (wide, cols)], nodes, mean_depth, far=(0, 1),
        scratch_shapes=[
            pltpu.VMEM(spread, jnp.float32),
            pltpu.VMEM((3,) + state, jnp.float32),
            pltpu.VMEM((rows, cols), jnp.float32),
            pltpu.SemaphoreType.DMA((4,)),
        ],
    )
    ffk, depth = kernel(second_body, [spread, (wide, cols)], fk, bare, *edges)
    fine_shapes = [(3 * wide, half + 2 * LANES), (3 * wide, half)]
    fine_args = (place, base, init_state, fk, ffk, depth, prev)
    give, v_give = kernel(functools.partial(fine_body, False), fine_shapes, *fine_args, scalars=1)
    got = lax.ppermute(give, "core", swapped)
    keep, v_keep = kernel(functools.partial(fine_body, True), fine_shapes, *fine_args, prev_late, scalars=1)
    tight = packed_rows(wide, width, reach)
    msg_shape = (owners, tight, LANES) if tight else (owners, 3 * wide, span)
    parts = (keep, give, v_keep, v_give)
    msgs, *far_parts = kernel(
        functools.partial(pair_body, width, reach, len(parts)), [msg_shape] + [x.shape for x in parts],
        place, depth, got, *parts, scalars=1, far_out=range(1 + len(parts)),
        scratch_shapes=[pltpu.VMEM(msg_shape, jnp.float32), pltpu.SemaphoreType.DMA((owners + len(parts),))],
    )
    recv = lax.all_to_all(msgs, group, 0, 0, tiled=True)
    spill = kernel(
        spill_body, (2, 2, 18, 1, half), keep, give, *far_parts[2:], far=(2, 3),
        scratch_shapes=[pltpu.VMEM((2, 3, TILE, half), jnp.float32), pltpu.SemaphoreType.DMA((6,))],
    )
    ahead = kernel(
        functools.partial(ahead_body, inner, rows), (3, spaces * rows, span),
        place, *windows, scalars=1,
    )
    spill = swap_rows(spill)
    b_own, vee = kernel(
        mend_body, [spread, state], place, *far_parts, *spill, scalars=1,
        far=range(1, 5), far_out=(1,),
        scratch_shapes=[pltpu.VMEM(state, jnp.float32)]
        + [pltpu.VMEM(x.shape, jnp.float32) for x in far_parts]
        + [pltpu.SemaphoreType.DMA((5,))],
    )
    b_lent = lax.ppermute(b_own, "core", [(0, 1)])

    tight = packed_rows(spaces * rows, width, reach)
    total_shape = (tight, LANES) if tight else (3 * spaces * rows, span)
    total = kernel(functools.partial(total_body, *plan), total_shape, place, recv, ahead, *windows, scalars=1)
    carry = lax.ppermute(total, "outer", [(i, i + 1) for i in range(outer - 1)])
    back = kernel(
        functools.partial(chain_body, *plan), (owners, 3 * rows + 2 * TILE, width),
        place, recv, carry, *windows, scalars=1, far_out=(0,),
        scratch_shapes=[
            pltpu.VMEM((owners, 3 * rows + 2 * TILE, width), jnp.float32),
            pltpu.SemaphoreType.DMA((owners,)),
        ],
    )
    mine = lax.all_to_all(back, group, 0, 0, tiled=True)
    if width % LANES:
        mine = mine.transpose(1, 0, 2).reshape(1, 3 * rows + 2 * TILE, half)
    other = lax.ppermute(mine, "core", swapped)

    def finish(near, cols_held, *args, **more):
        held = (3, wide, cols_held)
        return kernel(
            functools.partial(finish_body, near), (3,) + state,
            place, *args, scalars=1, far_out=(0,),
            scratch_shapes=[
                pltpu.VMEM(held, jnp.float32),
                pltpu.VMEM(held, jnp.float32),
                pltpu.VMEM((3, rows, cols_held), jnp.float32),
                pltpu.VMEM((3, 3, rows, cols_held), jnp.float32),
                pltpu.SemaphoreType.DMA((33,)),
            ],
            **more,
        )

    out = finish(True, half, mine, b_own, b_lent, vee, depth, far=(2, 4))
    out = finish(
        False, half + 4 * LANES, mine, other, b_own, b_lent, vee, depth, out,
        far=(3, 5, 7), input_output_aliases={7: 0},
    )
    return out[None]


def all_windows(depth, init, offset, at_inner, spaces, width, reach, span):
    fixed = jnp.concatenate([depth[None], init], axis=0)
    _, rows, cols = fixed.shape
    onward = jnp.concatenate([fixed, fixed[..., :span]], axis=-1)
    behind = jnp.concatenate([fixed[..., cols - span :], fixed], axis=-1)
    lane = lax.broadcasted_iota(jnp.int32, (4, rows, span), 2)
    windows = []
    for y in range(spaces):
        start = offset + (at_inner * spaces + y) * width
        ahead = lax.dynamic_slice_in_dim(onward, start, span, axis=2)
        back = lax.dynamic_slice_in_dim(behind, start, span, axis=2)
        windows.append(jnp.where(lane < span - reach, ahead, back).reshape(4 * rows, span))
    return jnp.stack(windows)


def solution(mesh):
    slices, spaces = mesh.shape["tm"], mesh.shape["space"]
    split = Mesh(mesh.devices.reshape(2, slices // 4, 2, spaces), ("outer", "inner", "core", "space"))
    nodes = P(("outer", "inner", "core"), None, None, "space", None)
    return jax.shard_map(
        per_device,
        mesh=split,
        in_specs=(nodes, P(None, "space", None), P("space", None)),
        out_specs=nodes,
        check_vma=False,
    )
```

```python
import functools

import jax
import jax.numpy as jnp
from jax import lax
from jax.experimental import pallas as pl
from jax.experimental.pallas import tpu as pltpu
from jax.sharding import Mesh
from jax.sharding import PartitionSpec as P


DT = 0.3
HALF = 0.5 * DT
NU = 1.0 / 3.0
FC = 0.5
DEEP = 3
TILE = 8
LANES = 128
VMEM_BYTES = 20 * 1024 * 1024


def rolled(x, by, axis):
    return pltpu.roll(x, by % x.shape[axis], axis)


def advanced(q, flow, scale, keep):
    height, east, north = q
    soft, slope, turn = scale * NU, scale * 0.5, scale * FC
    stay = keep - 4.0 * soft
    h_soft, e_soft, n_soft = soft * height, soft * east, soft * north
    h_slope = slope * height
    flow_e, flow_n = flow * east, flow * north
    new_h = (
        (rolled(h_soft + flow_e, 1, 1) + rolled(h_soft - flow_e, -1, 1))
        + (rolled(h_soft + flow_n, 1, 0) + rolled(h_soft - flow_n, -1, 0))
        + stay * height
    )
    new_e = (
        (rolled(e_soft + h_slope, 1, 1) + rolled(e_soft - h_slope, -1, 1))
        + (rolled(e_soft, 1, 0) + rolled(e_soft, -1, 0))
        + (stay * east + turn * north)
    )
    new_n = (
        (rolled(n_soft, 1, 1) + rolled(n_soft, -1, 1))
        + (rolled(n_soft + h_slope, 1, 0) + rolled(n_soft - h_slope, -1, 0))
        + (stay * north - turn * east)
    )
    return new_h, new_e, new_n


def tendency(q, half_depth):
    return advanced(q, half_depth, 1.0, 0.0)


def stepped(q, step_depth):
    return advanced(q, step_depth, DT, 1.0)


def dense(width, reach, rows):
    return width % LANES == 0 and 2 * reach <= 32 and rows % TILE == 0


def packed_rows(rows, width, reach):
    if not dense(width, reach, rows):
        return None
    tiles = 3 * rows // TILE
    return 3 * rows * (width // LANES) + TILE * -(-tiles // 4)


def cut(ref, lead, at, size=LANES):
    return ref[lead + (slice(None), pl.ds(pl.multiple_of(at, LANES), size))]


def last_copies(place, nodes, soon_out, late_out, sems):
    cols = nodes.shape[-1]
    half = cols // 2
    start = place[2] * half
    before, after = lax.rem(start + (cols - LANES), cols), lax.rem(start + half, cols)
    cuts = (
        (before, LANES, soon_out, 0),
        (start, half, soon_out, LANES),
        (after, LANES, soon_out, LANES + half),
        (after, half, late_out, 0),
    )
    copies = []
    for i, (at, size, out, to) in enumerate(cuts):
        source = nodes.at[2, :, :, pl.ds(pl.multiple_of(at, LANES), size)]
        copies.append(pltpu.make_async_copy(source, out.at[:, :, to : to + size], sems.at[i]))
        copies[-1].start()
    return copies


def last_body(place, nodes, soon_out, late_out, sems):
    for copy in last_copies(place, nodes, soon_out, late_out, sems):
        copy.wait()


def begin_body(width, reach, place, nodes, depth_far, init, soon_out, late_out, own_out, edge_out, depth, held, sems, more):
    copies = last_copies(place, nodes, soon_out, late_out, more)
    prepare_body(width, reach, place, depth_far, init, own_out, edge_out, depth, held, sems)
    for copy in copies:
        copy.wait()


def prepare_body(width, reach, place, depth_far, init, own_out, edge_out, depth, held, sems):
    rows, cols = depth.shape
    lane = lax.broadcasted_iota(jnp.int32, (rows, LANES), 1)
    copies = [pltpu.make_async_copy(depth_far, depth, sems.at[0])]
    for h, y in enumerate((place[4], 1 - place[4])):
        start = place[2] * (cols // 2) + (place[3] * 2 + y) * width
        after = lax.rem(start + width, cols)
        before = lax.rem(start - LANES + cols, cols)
        for i in range(4):
            ref = depth_far if i == 0 else init.at[i - 1]
            for k, (at, to, size) in enumerate(
                ((start, 0, width), (after, width, LANES), (before, width + LANES, LANES))
            ):
                copies.append(
                    pltpu.make_async_copy(
                        ref.at[:, pl.ds(pl.multiple_of(at, LANES), size)],
                        held.at[h, i, :, to : to + size],
                        sems.at[1 + (h * 4 + i) * 3 + k],
                    )
                )
    for copy in copies:
        copy.start()
    for copy in copies:
        copy.wait()
    for h, out in enumerate((own_out, edge_out)):
        for i in range(4):
            parts = [held[h, i, :, t * LANES : (t + 1) * LANES] for t in range(width // LANES)]
            after, before = held[h, i, :, width : width + LANES], held[h, i, :, width + LANES :]
            parts.append(jnp.where(lane < LANES - reach, after, before))
            for t, part in enumerate(parts):
                at = (4 * t + i) * rows
                out[at : at + rows, :] = part
    at = own_out.shape[0]
    for r in (*range(DEEP), *range(rows - DEEP, rows)):
        for t in range(cols // LANES):
            edge_out[at : at + 1, :] = depth[r : r + 1, t * LANES : (t + 1) * LANES]
            at += 1


def blend_body(nodes, depth_far, base_out, fk_out, depth_out, state, near, depth, sems):
    rows, cols = depth.shape
    copies = [pltpu.make_async_copy(nodes.at[:, f], near.at[f], sems.at[f]) for f in range(3)]
    copies.append(pltpu.make_async_copy(depth_far, depth, sems.at[3]))
    for copy in copies:
        copy.start()
    none = jnp.zeros((TILE, cols), jnp.float32)
    for f in range(3):
        copies[f].wait()
        n0, n1, n2 = near[f, 0], near[f, 1], near[f, 2]
        base_out[f] = (DT / 24.0) * (8.0 * n1 - 7.0 * n0 - n2)
        state[f, :rows, :] = (DT / 4.0) * (n0 - 2.0 * n1 + n2)
        state[f, rows:, :] = none
    copies[3].wait()
    half_depth = jnp.concatenate([0.5 * depth[...], none], axis=0)
    depth_out[...] = half_depth
    fk = tendency(tuple(state[f] for f in range(3)), half_depth)
    for f in range(3):
        fk_out[f] = fk[f]


def second_body(fk, bare, *rest):
    *edges, ffk_out, depth_out = rest
    rows, cols = bare.shape[0] - TILE, bare.shape[1]
    depth_out[...] = bare[...]
    for r in range(DEEP):
        below, above = rows + r, rows + TILE - DEEP + r
        if len(edges) == 2 or len(edges[0].shape) > 2:
            low, high = edges if len(edges) == 2 else (edges[0].at[0], edges[0].at[1])
            depth_out[below : below + 1, :] = 0.5 * low[r]
            depth_out[above : above + 1, :] = 0.5 * high[r]
            continue
        tiles = cols // LANES
        base = edges[0].shape[0] - 2 * DEEP * tiles
        for t in range(tiles):
            for to, at in ((below, base + r * tiles + t), (above, base + (DEEP + r) * tiles + t)):
                depth_out[to : to + 1, t * LANES : (t + 1) * LANES] = 0.5 * edges[0][at : at + 1, :]
    ffk = tendency(tuple(fk[f] for f in range(3)), depth_out[...])
    for f in range(3):
        ffk_out[f] = ffk[f]


def window(ref, lead, half):
    cols = ref.shape[-1]
    start = half * (cols // 2) + (cols - LANES)
    parts = [cut(ref, lead, lax.rem(start + t * LANES, cols)) for t in range(cols // 2 // LANES + 2)]
    return jnp.concatenate(parts, axis=1)


def fine_body(own_half, place, base, init, fk, ffk, depth_ref, prev, *rest):
    *late, b_out, v_out = rest
    half = place[2] if own_half else 1 - place[2]
    first = place[0] == 1
    wide = fk.shape[1]
    half_depth = window(depth_ref, (), half)
    none = jnp.zeros((TILE, half_depth.shape[1]), jnp.float32)
    g = []
    for f in range(3):
        before = prev[f]
        if own_half:
            size = late[0].shape[2]
            before = jnp.concatenate([before[:, size : size + LANES], late[0][f], before[:, LANES : 2 * LANES]], axis=1)
        start = jnp.where(first, window(init, (f,), half), before)
        g.append(jnp.concatenate([HALF * start + window(base, (f,), half), none], axis=0))
    u = tendency(tendency(tuple(g), half_depth), half_depth)
    fu = tendency(u, half_depth)
    for f in range(3):
        at = slice(f * wide, (f + 1) * wide)
        v = window(fk, (f,), half) + HALF * u[f]
        v_out[at, :] = v[:, LANES : v.shape[1] - LANES]
        b_out[at, :] = DT * (u[f] + (1.0 / 6.0) * (HALF * fu[f] + window(ffk, (f,), half)))


def spill_body(b_keep, b_give, v_keep, v_give, spill_out, v_spread, sems):
    wide = b_keep.shape[0] // 3
    rows = wide - TILE
    copies = [
        pltpu.make_async_copy(v.at[pl.ds(f * wide + rows, TILE), :], v_spread.at[h, f], sems.at[3 * h + f])
        for h, v in enumerate((v_keep, v_give))
        for f in range(3)
    ]
    for copy in copies:
        copy.start()
    for h, b in enumerate((b_keep, b_give)):
        inside = slice(LANES, b.shape[1] - LANES)
        for f in range(3):
            top = f * wide
            for side, spread, edge in ((0, wide - DEEP, 0), (1, rows, rows - 1)):
                for r in range(DEEP):
                    spill_out[side, h, DEEP * f + r] = b[top + spread + r : top + spread + r + 1, inside]
                spill_out[side, h, 9 + f] = b[top + edge : top + edge + 1, inside]
    for copy in copies:
        copy.wait()
    for h in range(2):
        for f in range(3):
            for side, spread in ((0, TILE - 2), (1, 0)):
                for r in range(2):
                    spill_out[side, h, 12 + 2 * f + r] = v_spread[h, f, spread + r : spread + r + 1, :]


def mend_body(place, *refs):
    far, edges, (b_out, v_far, v_out, *near, sems) = refs[:4], refs[4:-8], refs[-8:]
    low, high = (edges[0].at[0], edges[0].at[1]) if len(edges) == 1 else edges
    copies = [pltpu.make_async_copy(x, y, sems.at[i]) for i, (x, y) in enumerate(zip(far, near))]
    for i in (2, 3, 0, 1):
        copies[i].start()
    b_keep, b_give, v_keep, v_give = near
    copies[2].wait()
    copies[3].wait()
    rows = v_out.shape[1]
    wide = rows + TILE
    size = v_keep.shape[1]
    halves = ((place[2], b_keep, v_keep), (1 - place[2], b_give, v_give))
    for h, (half, _, v) in enumerate(halves):
        to = pl.ds(pl.multiple_of(half * size, LANES), size)
        for f in range(3):
            v_out[f, :, to] = v[f * wide : f * wide + rows, :]
            for r in range(2):
                for at, more in ((r, high), (rows - 2 + r, low)):
                    old = v[f * wide + at : f * wide + at + 1, :]
                    v_out[f, at : at + 1, to] = old + more[h, 12 + 2 * f + r]
    copy = pltpu.make_async_copy(v_out, v_far, sems.at[4])
    copy.start()
    copies[0].wait()
    copies[1].wait()
    for h, (half, b, _) in enumerate(halves):
        to = pl.ds(pl.multiple_of(half * size, LANES), size)
        inside = slice(LANES, LANES + size)
        for f in range(3):
            top = f * wide
            b_out[f, :, to] = b[top : top + wide, inside]
            adds = [(rows, 9 + f, low), (wide - 1, 9 + f, high)]
            for r in range(DEEP):
                adds += [(r, DEEP * f + r, high), (rows - DEEP + r, DEEP * f + r, low)]
            for at, i, more in adds:
                b_out[f, at : at + 1, to] = b[top + at : top + at + 1, inside] + more[h, i]
    copy.wait()


def pair_body(width, reach, count, place, depth_ref, got, *rest):
    near, far = rest[:count], rest[count + 1 : 2 * count + 1]
    msg_far, msg_out, sems = rest[count], rest[-2], rest[-1]
    owners = msg_out.shape[0]
    copies = [pltpu.make_async_copy(a, b, sems.at[owners + i]) for i, (a, b) in enumerate(zip(near, far))]
    for copy in copies:
        copy.start()
    keep = near[0]
    wide = keep.shape[0] // 3
    even = place[2] == 0
    step_depth = DT * window(depth_ref, (), place[2])
    own = tuple(keep[f * wide : (f + 1) * wide, :] for f in range(3))
    other = tuple(got[f * wide : (f + 1) * wide, :] for f in range(3))
    first = tuple(jnp.where(even, x, y) for x, y in zip(own, other))
    second = tuple(jnp.where(even, y, x) for x, y in zip(own, other))
    both = tuple(x + y for x, y in zip(second, stepped(first, step_depth)))
    for j in range(owners):
        for f in range(3):
            pack_block(both[f], f, j, width, reach, msg_out.at[j])
    copies.append(pltpu.make_async_copy(msg_out, msg_far, sems.at[0]))
    copies[-1].start()
    for copy in copies:
        copy.wait()


def pack_block(b, f, j, width, reach, out):
    rows, cols = b.shape
    at = LANES + j * width
    lane = lax.broadcasted_iota(jnp.int32, (rows, LANES), 1)
    if dense(width, reach, rows):
        small = lax.broadcasted_iota(jnp.int32, (TILE, LANES), 1)
        parts = width // LANES
        for t in range(parts):
            out[(f * parts + t) * rows : (f * parts + t + 1) * rows, :] = b[:, at + t * LANES : at + (t + 1) * LANES]
        after, before = at + width, at - LANES
        halo = jnp.where(lane < LANES // 2, b[:, after : after + LANES], b[:, before : before + LANES])
        put_halo(halo, f * rows // TILE, 3 * parts * rows, small, out)
        return
    span = out.shape[1]
    turned = rolled(b, -at, 1)
    parts = [turned[:, t : t + LANES] for t in range(0, span, LANES)]
    parts[-1] = jnp.where(lane < LANES - reach, parts[-1], turned[:, cols - LANES :])
    for t, part in enumerate(parts):
        out[f * rows : (f + 1) * rows, t * LANES : (t + 1) * LANES] = part


def put_halo(halo, tile, base, small, out):
    for i in range(halo.shape[0] // TILE):
        q = (tile + i) % 4
        at = base + (tile + i) // 4 * TILE
        moved = rolled(halo[i * TILE : (i + 1) * TILE], 16 + 32 * q, 1)
        if q:
            moved = jnp.where(small >= 32 * q, moved, out[at : at + TILE, :])
        out[at : at + TILE, :] = moved


def get_halo(source, tile, count, base):
    found = []
    for i in range(tile, tile + count):
        at = base + i // 4 * TILE
        found.append(rolled(source[at : at + TILE, :], -(16 + 32 * (i % 4)), 1))
    return jnp.concatenate(found, axis=0)


def block_of(message, f, rows, width, reach):
    if not dense(width, reach, rows):
        return message[f * rows : (f + 1) * rows, :]
    parts = width // LANES
    main = [message[(f * parts + t) * rows : (f * parts + t + 1) * rows, :] for t in range(parts)]
    return jnp.concatenate(main + [get_halo(message, f * rows // TILE, rows // TILE, 3 * parts * rows)], axis=1)


def joined(recv, slot, spaces, rows, width, reach):
    wide = rows + TILE
    fields = []
    for f in range(3):
        blocks = [block_of(recv.at[slot * spaces + y], f, wide, width, reach) for y in range(spaces)]
        row = lax.broadcasted_iota(jnp.int32, (TILE, blocks[0].shape[1]), 0)
        tiles = []
        for y in range(spaces):
            here = [blocks[y][t : t + TILE] for t in range(0, rows, TILE)]
            here[0] = here[0] + jnp.where(row < TILE // 2, blocks[(y - 1) % spaces][rows:], 0.0)
            here[-1] = here[-1] + jnp.where(row < TILE // 2, 0.0, blocks[(y + 1) % spaces][rows:])
            tiles += here
        fields.append(jnp.concatenate(tiles, axis=0))
    return tuple(fields)


def window_field(win, i, rows, place):
    if len(win) == 1:
        return jnp.concatenate([win[0][y, i * rows : (i + 1) * rows, :] for y in range(win[0].shape[0])], axis=0)
    own, theirs = (
        jnp.concatenate([part[at : at + rows, :] for at in range(i * rows, part.shape[0], 4 * rows)], axis=1)
        for part in (win[0], win[1].at[: win[0].shape[0]])
    )
    above = place[4] == 0
    return jnp.concatenate([jnp.where(above, own, theirs), jnp.where(above, theirs, own)], axis=0)


def two_steps(q, step_depth):
    return stepped(stepped(q, step_depth), step_depth)


def ahead_body(slots, rows, place, *rest):
    *win, out = rest
    step_depth = HALF * window_field(win, 0, rows, place)
    q = tuple(window_field(win, 1 + f, rows, place) for f in range(3))
    for _ in range(slots):
        q = two_steps(q, step_depth)
    for f in range(3):
        out[f] = q[f]


def total_body(spaces, rows, width, reach, place, recv, ahead, *rest):
    *win, total_out = rest
    slots = recv.shape[0] // spaces
    step_depth = HALF * window_field(win, 0, rows, place)
    q = joined(recv, 0, spaces, rows, width, reach)
    for slot in range(1, slots):
        b = joined(recv, slot, spaces, rows, width, reach)
        q = tuple(x + y for x, y in zip(b, two_steps(q, step_depth)))
    q = tuple(x + ahead[f] for f, x in enumerate(q))
    all_rows = rows * spaces
    if not dense(width, reach, rows):
        for f in range(3):
            total_out[f * all_rows : (f + 1) * all_rows, :] = q[f]
        return
    small = lax.broadcasted_iota(jnp.int32, (TILE, LANES), 1)
    parts = width // LANES
    for f in range(3):
        for t in range(parts):
            total_out[(f * parts + t) * all_rows : (f * parts + t + 1) * all_rows, :] = q[f][
                :, t * LANES : (t + 1) * LANES
            ]
        put_halo(q[f][:, width:], f * all_rows // TILE, 3 * parts * all_rows, small, total_out)


def chain_body(spaces, rows, width, reach, place, recv, carry, *rest):
    *win, msg_far, msg_out, sems = rest
    slots = recv.shape[0] // spaces
    all_rows = rows * spaces
    copies = []
    step_depth = HALF * window_field(win, 0, rows, place)
    lower = place[1] == 1
    q = tuple(
        jnp.where(lower, window_field(win, 1 + f, rows, place), block_of(carry, f, all_rows, width, reach))
        for f in range(3)
    )
    for slot in range(slots):
        for y in range(spaces):
            at = slot * spaces + y
            for f in range(3):
                here = q[f][:, :width]
                lo, hi = y * rows, (y + 1) * rows
                msg_out[at, f * rows : (f + 1) * rows, :] = here[lo:hi]
                for r, source in enumerate((hi, hi + 1, lo - 2, lo - 1)):
                    source %= all_rows
                    to = 3 * rows + 4 * f + r
                    msg_out[at, to : to + 1, :] = here[source : source + 1]
            msg_out[at, 3 * rows + 12 :, :] = jnp.zeros((4, width), jnp.float32)
            copies.append(pltpu.make_async_copy(msg_out.at[at], msg_far.at[at], sems.at[at]))
            copies[-1].start()
        if slot + 1 < slots:
            b = joined(recv, slot, spaces, rows, width, reach)
            q = tuple(x + y for x, y in zip(b, two_steps(q, step_depth)))
    for copy in copies:
        copy.wait()


def finish_body(near, place, *refs):
    if near:
        mine, b_far, b_lent, v_far, depth_ref, out, state, b_own, v_ref, made, sems = refs
        other = None
    else:
        mine, other, b_far, b_lent, v_far, depth_ref, _, out, state, b_own, v_ref, made, sems = refs
    rows = v_ref.shape[1]
    wide = rows + TILE
    half = depth_ref.shape[1] // 2
    ours, theirs = place[2] * half, (1 - place[2]) * half
    side = 2 * LANES
    if near:
        parts = [(ours, half, mine, 0)]
        pieces = [(LANES, half - 2 * LANES, ours + LANES)]
    else:
        parts = [(ours + half - side, side, mine, half - side), (theirs, half, other, 0), (ours, side, mine, 0)]
        pieces = [(LANES, LANES, ours + half - LANES), (side, half, theirs), (side + half, LANES, ours)]

    def at(start, size):
        return pl.ds(pl.multiple_of(start, LANES), size)

    fetches, local = [], 0
    for i, (start, size, source, first) in enumerate(parts):
        width = source.shape[2]
        here = slice(local, local + size)
        for k, (far, held) in enumerate(((b_far, b_own), (v_far, v_ref))):
            copy = pltpu.make_async_copy(far.at[:, :, at(start, size)], held.at[:, :, here], sems.at[2 * i + k])
            copy.start()
            fetches.append(copy)
        step = min(width, size)
        for c in range(0, size, step):
            j, off = (first + c) // width, (first + c) % width
            to = slice(local + c, local + c + step)
            for f in range(3):
                state[f, :rows, to] = source[j, f * rows : (f + 1) * rows, off : off + step]
                for r, row in enumerate((rows, rows + 1, wide - 2, wide - 1)):
                    line = 3 * rows + 4 * f + r
                    state[f, row : row + 1, to] = source[j, line : line + 1, off : off + step]
        local += size
    for f in range(3):
        state[f, rows + 2 : wide - 2, :] = jnp.zeros((TILE - 4, local), jnp.float32)

    def taken(ref, lead):
        return jnp.concatenate([cut(ref, lead, start, size) for start, size, _, _ in parts], axis=1)

    even = place[2] == 0
    step_depth = DT * taken(depth_ref, ())
    carried = tuple(state[f] for f in range(3))
    moved = stepped(carried, step_depth)
    for fetch in fetches:
        fetch.wait()
    after = tuple(jnp.where(even, b_own[f], taken(b_lent, (f,))) + x for f, x in enumerate(moved))
    last = stepped(after, step_depth)
    copies = []
    for f in range(3):
        begin = jnp.where(even, carried[f][:rows], after[f][:rows])
        end = jnp.where(even, after[f][:rows], b_own[f, :rows, :] + last[f][:rows])
        made[0, f] = begin
        made[1, f] = 0.5 * ((begin + end) - v_ref[f])
        made[2, f] = end
        for part in range(3):
            for i, (lo, size, to) in enumerate(pieces):
                copy = pltpu.make_async_copy(
                    made.at[part, f, :, lo : lo + size],
                    out.at[part, f, :, at(to, size)],
                    sems.at[6 + (3 * f + part) * 3 + i],
                )
                copy.start()
                copies.append(copy)
    for copy in copies:
        copy.wait()


def kernel(body, shapes, *args, scalars=0, far=(), far_out=(), near=(), near_out=(), **more):
    vmem = pl.BlockSpec(memory_space=pltpu.VMEM)
    hbm = pl.BlockSpec(memory_space=pltpu.HBM)
    smem = pl.BlockSpec(memory_space=pltpu.SMEM)
    many = isinstance(shapes, list)
    outs = []
    for i, shape in enumerate(shapes if many else [shapes]):
        make = pltpu.HBM if i in far_out else pltpu.VMEM if i in near_out else jax.ShapeDtypeStruct
        outs.append(make(shape, jnp.float32))
    placed = list(args)
    for held, space in ((far, pltpu.HBM), (near, pltpu.VMEM)):
        for i in held:
            placed[i] = pltpu.with_memory_space_constraint(args[i], space)
    specs = [hbm if i in far_out else vmem for i in range(len(outs))]
    return pl.pallas_call(
        body,
        out_shape=outs if many else outs[0],
        in_specs=[smem if i < scalars else hbm if i in far else vmem for i in range(len(args))],
        out_specs=specs if many else specs[0],
        compiler_params=pltpu.CompilerParams(vmem_limit_bytes=VMEM_BYTES),
        **more,
    )(*placed)


def swap_rows(edges):
    count = lax.axis_size("space")
    if count == 2:
        return (lax.ppermute(edges, "space", [(0, 1), (1, 0)]),)
    below = lax.ppermute(edges[0], "space", [((i + 1) % count, i) for i in range(count)])
    above = lax.ppermute(edges[1], "space", [(i, (i + 1) % count) for i in range(count)])
    return below, above


def per_device(fine_nodes, init_state, mean_depth):
    nodes = fine_nodes[0]
    rows, cols = nodes.shape[-2:]
    outer, inner, spaces = lax.axis_size("outer"), lax.axis_size("inner"), lax.axis_size("space")
    group = ("inner", "space")
    owners = inner * spaces
    half = cols // 2
    width = half // owners
    slices = outer * inner * 2
    reach = slices - 2
    span = -(-(width + 2 * reach) // LANES) * LANES
    wide = rows + TILE
    at_outer, at_inner, at_core, at_space = (
        lax.axis_index(name) for name in ("outer", "inner", "core", "space")
    )
    first = at_outer + at_inner + at_core == 0
    place = jnp.stack([first.astype(jnp.int32), (at_outer == 0).astype(jnp.int32), at_core, at_inner, at_space])
    state, spread = (3, rows, cols), (3, wide, cols)
    swapped = [(0, 1), (1, 0)]
    plan = (spaces, rows, width, reach)

    onward = [(i, i + 1) for i in range(slices - 1)]
    last_shapes = [(3, rows, half + 2 * LANES), (3, rows, half)]
    paired = spaces == 2 and dense(width, reach, rows)
    if paired:
        own_rows = 4 * rows * span // LANES
        soon, late, own, edges = kernel(
            functools.partial(begin_body, width, reach),
            last_shapes + [(own_rows, LANES), (own_rows + 2 * DEEP * cols // LANES, LANES)],
            place, nodes, mean_depth, init_state, scalars=1, far=(1, 2, 3),
            scratch_shapes=[
                pltpu.VMEM((rows, cols), jnp.float32),
                pltpu.VMEM((2, 4, rows, width + 2 * LANES), jnp.float32),
                pltpu.SemaphoreType.DMA((25,)),
                pltpu.SemaphoreType.DMA((4,)),
            ],
        )
    else:
        soon, late = kernel(
            last_body, last_shapes, place, nodes, scalars=1, far=(1,),
            scratch_shapes=[pltpu.SemaphoreType.DMA((4,))],
        )
    prev = lax.ppermute(soon, ("outer", "inner", "core"), onward)
    prev_late = lax.ppermute(late, ("outer", "inner", "core"), onward)
    if paired:
        edges = lax.ppermute(edges, "space", swapped)
        windows, edges = (own, edges), (edges,)
    else:
        windows = all_windows(mean_depth, init_state, at_core * half, at_inner, spaces, width, reach, span)
        windows = (lax.all_to_all(windows, "space", 0, 0, tiled=True),)
        edges = jnp.stack([mean_depth[:DEEP, None], mean_depth[rows - DEEP :, None]])
        edges = swap_rows(edges)

    base, fk, bare = kernel(
        blend_body, [state, spread, (wide, cols)], nodes, mean_depth, far=(0, 1),
        scratch_shapes=[
            pltpu.VMEM(spread, jnp.float32),
            pltpu.VMEM((3,) + state, jnp.float32),
            pltpu.VMEM((rows, cols), jnp.float32),
            pltpu.SemaphoreType.DMA((4,)),
        ],
    )
    ffk, depth = kernel(second_body, [spread, (wide, cols)], fk, bare, *edges)
    fine_shapes = [(3 * wide, half + 2 * LANES), (3 * wide, half)]
    fine_args = (place, base, init_state, fk, ffk, depth, prev)
    give, v_give = kernel(functools.partial(fine_body, False), fine_shapes, *fine_args, scalars=1)
    got = lax.ppermute(give, "core", swapped)
    keep, v_keep = kernel(functools.partial(fine_body, True), fine_shapes, *fine_args, prev_late, scalars=1)
    tight = packed_rows(wide, width, reach)
    msg_shape = (owners, tight, LANES) if tight else (owners, 3 * wide, span)
    parts = (keep, give, v_keep, v_give)
    msgs, *far_parts = kernel(
        functools.partial(pair_body, width, reach, len(parts)), [msg_shape] + [x.shape for x in parts],
        place, depth, got, *parts, scalars=1, far_out=range(1 + len(parts)),
        scratch_shapes=[pltpu.VMEM(msg_shape, jnp.float32), pltpu.SemaphoreType.DMA((owners + len(parts),))],
    )
    recv = lax.all_to_all(msgs, group, 0, 0, tiled=True)
    spill = kernel(
        spill_body, (2, 2, 18, 1, half), keep, give, *far_parts[2:], far=(2, 3),
        scratch_shapes=[pltpu.VMEM((2, 3, TILE, half), jnp.float32), pltpu.SemaphoreType.DMA((6,))],
    )
    ahead = kernel(
        functools.partial(ahead_body, inner, rows), (3, spaces * rows, span),
        place, *windows, scalars=1,
    )
    spill = swap_rows(spill)
    b_own, vee = kernel(
        mend_body, [spread, state], place, *far_parts, *spill, scalars=1,
        far=range(1, 5), far_out=(1,),
        scratch_shapes=[pltpu.VMEM(state, jnp.float32)]
        + [pltpu.VMEM(x.shape, jnp.float32) for x in far_parts]
        + [pltpu.SemaphoreType.DMA((5,))],
    )
    b_lent = lax.ppermute(b_own, "core", [(0, 1)])

    tight = packed_rows(spaces * rows, width, reach)
    total_shape = (tight, LANES) if tight else (3 * spaces * rows, span)
    total = kernel(functools.partial(total_body, *plan), total_shape, place, recv, ahead, *windows, scalars=1)
    carry = lax.ppermute(total, "outer", [(i, i + 1) for i in range(outer - 1)])
    back = kernel(
        functools.partial(chain_body, *plan), (owners, 3 * rows + 2 * TILE, width),
        place, recv, carry, *windows, scalars=1, far_out=(0,),
        scratch_shapes=[
            pltpu.VMEM((owners, 3 * rows + 2 * TILE, width), jnp.float32),
            pltpu.SemaphoreType.DMA((owners,)),
        ],
    )
    mine = lax.all_to_all(back, group, 0, 0, tiled=True)
    if width % LANES:
        mine = mine.transpose(1, 0, 2).reshape(1, 3 * rows + 2 * TILE, half)
    other = lax.ppermute(mine, "core", swapped)

    def finish(near, cols_held, *args, **more):
        held = (3, wide, cols_held)
        return kernel(
            functools.partial(finish_body, near), (3,) + state,
            place, *args, scalars=1, far_out=(0,),
            scratch_shapes=[
                pltpu.VMEM(held, jnp.float32),
                pltpu.VMEM(held, jnp.float32),
                pltpu.VMEM((3, rows, cols_held), jnp.float32),
                pltpu.VMEM((3, 3, rows, cols_held), jnp.float32),
                pltpu.SemaphoreType.DMA((33,)),
            ],
            **more,
        )

    out = finish(True, half, mine, b_own, b_lent, vee, depth, far=(2, 4))
    out = finish(
        False, half + 4 * LANES, mine, other, b_own, b_lent, vee, depth, out,
        far=(3, 5, 7), input_output_aliases={7: 0},
    )
    return out[None]


def all_windows(depth, init, offset, at_inner, spaces, width, reach, span):
    fixed = jnp.concatenate([depth[None], init], axis=0)
    _, rows, cols = fixed.shape
    onward = jnp.concatenate([fixed, fixed[..., :span]], axis=-1)
    behind = jnp.concatenate([fixed[..., cols - span :], fixed], axis=-1)
    lane = lax.broadcasted_iota(jnp.int32, (4, rows, span), 2)
    windows = []
    for y in range(spaces):
        start = offset + (at_inner * spaces + y) * width
        ahead = lax.dynamic_slice_in_dim(onward, start, span, axis=2)
        back = lax.dynamic_slice_in_dim(behind, start, span, axis=2)
        windows.append(jnp.where(lane < span - reach, ahead, back).reshape(4 * rows, span))
    return jnp.stack(windows)


def solution(mesh):
    slices, spaces = mesh.shape["tm"], mesh.shape["space"]
    split = Mesh(mesh.devices.reshape(2, slices // 4, 2, spaces), ("outer", "inner", "core", "space"))
    nodes = P(("outer", "inner", "core"), None, None, "space", None)
    return jax.shard_map(
        per_device,
        mesh=split,
        in_specs=(nodes, P(None, "space", None), P("space", None)),
        out_specs=nodes,
        check_vma=False,
    )
```

```python
import functools

import jax
import jax.numpy as jnp
from jax import lax
from jax.experimental import pallas as pl
from jax.experimental.pallas import tpu as pltpu
from jax.sharding import Mesh
from jax.sharding import PartitionSpec as P


DT = 0.3
HALF = 0.5 * DT
NU = 1.0 / 3.0
FC = 0.5
DEEP = 3
TILE = 8
LANES = 128
VMEM_BYTES = 20 * 1024 * 1024


def rolled(x, by, axis):
    return pltpu.roll(x, by % x.shape[axis], axis)


def advanced(q, flow, scale, keep):
    height, east, north = q
    soft, slope, turn = scale * NU, scale * 0.5, scale * FC
    stay = keep - 4.0 * soft
    h_soft, e_soft, n_soft = soft * height, soft * east, soft * north
    h_slope = slope * height
    flow_e, flow_n = flow * east, flow * north
    new_h = (
        (rolled(h_soft + flow_e, 1, 1) + rolled(h_soft - flow_e, -1, 1))
        + (rolled(h_soft + flow_n, 1, 0) + rolled(h_soft - flow_n, -1, 0))
        + stay * height
    )
    new_e = (
        (rolled(e_soft + h_slope, 1, 1) + rolled(e_soft - h_slope, -1, 1))
        + (rolled(e_soft, 1, 0) + rolled(e_soft, -1, 0))
        + (stay * east + turn * north)
    )
    new_n = (
        (rolled(n_soft, 1, 1) + rolled(n_soft, -1, 1))
        + (rolled(n_soft + h_slope, 1, 0) + rolled(n_soft - h_slope, -1, 0))
        + (stay * north - turn * east)
    )
    return new_h, new_e, new_n


def tendency(q, half_depth):
    return advanced(q, half_depth, 1.0, 0.0)


def stepped(q, step_depth):
    return advanced(q, step_depth, DT, 1.0)


def dense(width, reach, rows):
    return width % LANES == 0 and 2 * reach <= 32 and rows % TILE == 0


def packed_rows(rows, width, reach):
    if not dense(width, reach, rows):
        return None
    tiles = 3 * rows // TILE
    return 3 * rows * (width // LANES) + TILE * -(-tiles // 4)


def cut(ref, lead, at, size=LANES):
    return ref[lead + (slice(None), pl.ds(pl.multiple_of(at, LANES), size))]


def last_copies(place, nodes, soon_out, late_out, sems):
    cols = nodes.shape[-1]
    half = cols // 2
    start = place[2] * half
    before, after = lax.rem(start + (cols - LANES), cols), lax.rem(start + half, cols)
    cuts = (
        (before, LANES, soon_out, 0),
        (start, half, soon_out, LANES),
        (after, LANES, soon_out, LANES + half),
        (after, half, late_out, 0),
    )
    copies = []
    for i, (at, size, out, to) in enumerate(cuts):
        source = nodes.at[2, :, :, pl.ds(pl.multiple_of(at, LANES), size)]
        copies.append(pltpu.make_async_copy(source, out.at[:, :, to : to + size], sems.at[i]))
        copies[-1].start()
    return copies


def last_body(place, nodes, soon_out, late_out, sems):
    for copy in last_copies(place, nodes, soon_out, late_out, sems):
        copy.wait()


def begin_body(width, reach, place, nodes, depth_far, init, soon_out, late_out, own_out, edge_out, depth, held, sems, more):
    copies = last_copies(place, nodes, soon_out, late_out, more)
    prepare_body(width, reach, place, depth_far, init, own_out, edge_out, depth, held, sems)
    for copy in copies:
        copy.wait()


def prepare_body(width, reach, place, depth_far, init, own_out, edge_out, depth, held, sems):
    rows, cols = depth.shape
    lane = lax.broadcasted_iota(jnp.int32, (rows, LANES), 1)
    copies = [pltpu.make_async_copy(depth_far, depth, sems.at[0])]
    for h, y in enumerate((place[4], 1 - place[4])):
        start = place[2] * (cols // 2) + (place[3] * 2 + y) * width
        after = lax.rem(start + width, cols)
        before = lax.rem(start - LANES + cols, cols)
        for i in range(4):
            ref = depth_far if i == 0 else init.at[i - 1]
            for k, (at, to, size) in enumerate(
                ((start, 0, width), (after, width, LANES), (before, width + LANES, LANES))
            ):
                copies.append(
                    pltpu.make_async_copy(
                        ref.at[:, pl.ds(pl.multiple_of(at, LANES), size)],
                        held.at[h, i, :, to : to + size],
                        sems.at[1 + (h * 4 + i) * 3 + k],
                    )
                )
    for copy in copies:
        copy.start()
    for copy in copies:
        copy.wait()
    for h, out in enumerate((own_out, edge_out)):
        for i in range(4):
            parts = [held[h, i, :, t * LANES : (t + 1) * LANES] for t in range(width // LANES)]
            after, before = held[h, i, :, width : width + LANES], held[h, i, :, width + LANES :]
            parts.append(jnp.where(lane < LANES - reach, after, before))
            for t, part in enumerate(parts):
                at = (4 * t + i) * rows
                out[at : at + rows, :] = part
    at = own_out.shape[0]
    for r in (*range(DEEP), *range(rows - DEEP, rows)):
        for t in range(cols // LANES):
            edge_out[at : at + 1, :] = depth[r : r + 1, t * LANES : (t + 1) * LANES]
            at += 1


def blend_body(nodes, depth_far, base_out, fk_out, depth_out, state, near, depth, sems):
    rows, cols = depth.shape
    copies = [pltpu.make_async_copy(nodes.at[:, f], near.at[f], sems.at[f]) for f in range(3)]
    copies.append(pltpu.make_async_copy(depth_far, depth, sems.at[3]))
    for copy in copies:
        copy.start()
    none = jnp.zeros((TILE, cols), jnp.float32)
    for f in range(3):
        copies[f].wait()
        n0, n1, n2 = near[f, 0], near[f, 1], near[f, 2]
        base_out[f] = (DT / 24.0) * (8.0 * n1 - 7.0 * n0 - n2)
        state[f, :rows, :] = (DT / 4.0) * (n0 - 2.0 * n1 + n2)
        state[f, rows:, :] = none
    copies[3].wait()
    half_depth = jnp.concatenate([0.5 * depth[...], none], axis=0)
    depth_out[...] = half_depth
    fk = tendency(tuple(state[f] for f in range(3)), half_depth)
    for f in range(3):
        fk_out[f] = fk[f]


def second_body(fk, bare, *rest):
    *edges, ffk_out, depth_out = rest
    rows, cols = bare.shape[0] - TILE, bare.shape[1]
    depth_out[...] = bare[...]
    for r in range(DEEP):
        below, above = rows + r, rows + TILE - DEEP + r
        if len(edges) == 2 or len(edges[0].shape) > 2:
            low, high = edges if len(edges) == 2 else (edges[0].at[0], edges[0].at[1])
            depth_out[below : below + 1, :] = 0.5 * low[r]
            depth_out[above : above + 1, :] = 0.5 * high[r]
            continue
        tiles = cols // LANES
        base = edges[0].shape[0] - 2 * DEEP * tiles
        for t in range(tiles):
            for to, at in ((below, base + r * tiles + t), (above, base + (DEEP + r) * tiles + t)):
                depth_out[to : to + 1, t * LANES : (t + 1) * LANES] = 0.5 * edges[0][at : at + 1, :]
    ffk = tendency(tuple(fk[f] for f in range(3)), depth_out[...])
    for f in range(3):
        ffk_out[f] = ffk[f]


def window(ref, lead, half):
    cols = ref.shape[-1]
    start = half * (cols // 2) + (cols - LANES)
    parts = [cut(ref, lead, lax.rem(start + t * LANES, cols)) for t in range(cols // 2 // LANES + 2)]
    return jnp.concatenate(parts, axis=1)


def fine_body(own_half, place, base, init, fk, ffk, depth_ref, prev, *rest):
    *late, b_out, v_out = rest
    half = place[2] if own_half else 1 - place[2]
    first = place[0] == 1
    wide = fk.shape[1]
    half_depth = window(depth_ref, (), half)
    none = jnp.zeros((TILE, half_depth.shape[1]), jnp.float32)
    g = []
    for f in range(3):
        before = prev[f]
        if own_half:
            size = late[0].shape[2]
            before = jnp.concatenate([before[:, size : size + LANES], late[0][f], before[:, LANES : 2 * LANES]], axis=1)
        start = jnp.where(first, window(init, (f,), half), before)
        g.append(jnp.concatenate([HALF * start + window(base, (f,), half), none], axis=0))
    u = tendency(tendency(tuple(g), half_depth), half_depth)
    fu = tendency(u, half_depth)
    for f in range(3):
        at = slice(f * wide, (f + 1) * wide)
        v = window(fk, (f,), half) + HALF * u[f]
        v_out[at, :] = v[:, LANES : v.shape[1] - LANES]
        b_out[at, :] = DT * (u[f] + (1.0 / 6.0) * (HALF * fu[f] + window(ffk, (f,), half)))


def spill_body(b_keep, b_give, v_keep, v_give, spill_out, keep_far, give_far, v_spread, sems):
    wide = b_keep.shape[0] // 3
    rows = wide - TILE
    copies = [
        pltpu.make_async_copy(v.at[pl.ds(f * wide + rows, TILE), :], v_spread.at[h, f], sems.at[3 * h + f])
        for h, v in enumerate((v_keep, v_give))
        for f in range(3)
    ]
    copies += [
        pltpu.make_async_copy(b_keep, keep_far, sems.at[6]),
        pltpu.make_async_copy(b_give, give_far, sems.at[7]),
    ]
    for copy in copies:
        copy.start()
    for h, b in enumerate((b_keep, b_give)):
        inside = slice(LANES, b.shape[1] - LANES)
        for f in range(3):
            top = f * wide
            for side, spread, edge in ((0, wide - DEEP, 0), (1, rows, rows - 1)):
                for r in range(DEEP):
                    spill_out[side, h, DEEP * f + r] = b[top + spread + r : top + spread + r + 1, inside]
                spill_out[side, h, 9 + f] = b[top + edge : top + edge + 1, inside]
    for copy in copies[:6]:
        copy.wait()
    for h in range(2):
        for f in range(3):
            for side, spread in ((0, TILE - 2), (1, 0)):
                for r in range(2):
                    spill_out[side, h, 12 + 2 * f + r] = v_spread[h, f, spread + r : spread + r + 1, :]
    for copy in copies[6:]:
        copy.wait()


def mend_body(place, *refs):
    far, edges, (b_out, v_far, v_out, *near, sems) = refs[:4], refs[4:-8], refs[-8:]
    low, high = (edges[0].at[0], edges[0].at[1]) if len(edges) == 1 else edges
    copies = [pltpu.make_async_copy(x, y, sems.at[i]) for i, (x, y) in enumerate(zip(far, near))]
    for i in (2, 3, 0, 1):
        copies[i].start()
    b_keep, b_give, v_keep, v_give = near
    copies[2].wait()
    copies[3].wait()
    rows = v_out.shape[1]
    wide = rows + TILE
    size = v_keep.shape[1]
    halves = ((place[2], b_keep, v_keep), (1 - place[2], b_give, v_give))
    for h, (half, _, v) in enumerate(halves):
        to = pl.ds(pl.multiple_of(half * size, LANES), size)
        for f in range(3):
            v_out[f, :, to] = v[f * wide : f * wide + rows, :]
            for r in range(2):
                for at, more in ((r, high), (rows - 2 + r, low)):
                    old = v[f * wide + at : f * wide + at + 1, :]
                    v_out[f, at : at + 1, to] = old + more[h, 12 + 2 * f + r]
    copy = pltpu.make_async_copy(v_out, v_far, sems.at[4])
    copy.start()
    copies[0].wait()
    copies[1].wait()
    for h, (half, b, _) in enumerate(halves):
        to = pl.ds(pl.multiple_of(half * size, LANES), size)
        inside = slice(LANES, LANES + size)
        for f in range(3):
            top = f * wide
            b_out[f, :, to] = b[top : top + wide, inside]
            adds = [(rows, 9 + f, low), (wide - 1, 9 + f, high)]
            for r in range(DEEP):
                adds += [(r, DEEP * f + r, high), (rows - DEEP + r, DEEP * f + r, low)]
            for at, i, more in adds:
                b_out[f, at : at + 1, to] = b[top + at : top + at + 1, inside] + more[h, i]
    copy.wait()


def pair_body(width, reach, place, depth_ref, got, keep, v_keep, v_give, msg_far, vk_far, vg_far, msg_out, sems):
    copies = [pltpu.make_async_copy(v_keep, vk_far, sems.at[1]), pltpu.make_async_copy(v_give, vg_far, sems.at[2])]
    for copy in copies:
        copy.start()
    wide = keep.shape[0] // 3
    even = place[2] == 0
    step_depth = DT * window(depth_ref, (), place[2])
    own = tuple(keep[f * wide : (f + 1) * wide, :] for f in range(3))
    other = tuple(got[f * wide : (f + 1) * wide, :] for f in range(3))
    first = tuple(jnp.where(even, x, y) for x, y in zip(own, other))
    second = tuple(jnp.where(even, y, x) for x, y in zip(own, other))
    both = tuple(x + y for x, y in zip(second, stepped(first, step_depth)))
    for j in range(msg_out.shape[0]):
        for f in range(3):
            pack_block(both[f], f, j, width, reach, msg_out.at[j])
    copies.append(pltpu.make_async_copy(msg_out, msg_far, sems.at[0]))
    copies[-1].start()
    for copy in copies:
        copy.wait()


def pack_block(b, f, j, width, reach, out):
    rows, cols = b.shape
    at = LANES + j * width
    lane = lax.broadcasted_iota(jnp.int32, (rows, LANES), 1)
    if dense(width, reach, rows):
        small = lax.broadcasted_iota(jnp.int32, (TILE, LANES), 1)
        parts = width // LANES
        for t in range(parts):
            out[(f * parts + t) * rows : (f * parts + t + 1) * rows, :] = b[:, at + t * LANES : at + (t + 1) * LANES]
        after, before = at + width, at - LANES
        halo = jnp.where(lane < LANES // 2, b[:, after : after + LANES], b[:, before : before + LANES])
        put_halo(halo, f * rows // TILE, 3 * parts * rows, small, out)
        return
    span = out.shape[1]
    turned = rolled(b, -at, 1)
    parts = [turned[:, t : t + LANES] for t in range(0, span, LANES)]
    parts[-1] = jnp.where(lane < LANES - reach, parts[-1], turned[:, cols - LANES :])
    for t, part in enumerate(parts):
        out[f * rows : (f + 1) * rows, t * LANES : (t + 1) * LANES] = part


def put_halo(halo, tile, base, small, out):
    for i in range(halo.shape[0] // TILE):
        q = (tile + i) % 4
        at = base + (tile + i) // 4 * TILE
        moved = rolled(halo[i * TILE : (i + 1) * TILE], 16 + 32 * q, 1)
        if q:
            moved = jnp.where(small >= 32 * q, moved, out[at : at + TILE, :])
        out[at : at + TILE, :] = moved


def get_halo(source, tile, count, base):
    found = []
    for i in range(tile, tile + count):
        at = base + i // 4 * TILE
        found.append(rolled(source[at : at + TILE, :], -(16 + 32 * (i % 4)), 1))
    return jnp.concatenate(found, axis=0)


def block_of(message, f, rows, width, reach):
    if not dense(width, reach, rows):
        return message[f * rows : (f + 1) * rows, :]
    parts = width // LANES
    main = [message[(f * parts + t) * rows : (f * parts + t + 1) * rows, :] for t in range(parts)]
    return jnp.concatenate(main + [get_halo(message, f * rows // TILE, rows // TILE, 3 * parts * rows)], axis=1)


def joined(recv, slot, spaces, rows, width, reach):
    wide = rows + TILE
    fields = []
    for f in range(3):
        blocks = [block_of(recv.at[slot * spaces + y], f, wide, width, reach) for y in range(spaces)]
        row = lax.broadcasted_iota(jnp.int32, (TILE, blocks[0].shape[1]), 0)
        tiles = []
        for y in range(spaces):
            here = [blocks[y][t : t + TILE] for t in range(0, rows, TILE)]
            here[0] = here[0] + jnp.where(row < TILE // 2, blocks[(y - 1) % spaces][rows:], 0.0)
            here[-1] = here[-1] + jnp.where(row < TILE // 2, 0.0, blocks[(y + 1) % spaces][rows:])
            tiles += here
        fields.append(jnp.concatenate(tiles, axis=0))
    return tuple(fields)


def window_field(win, i, rows, place):
    if len(win) == 1:
        return jnp.concatenate([win[0][y, i * rows : (i + 1) * rows, :] for y in range(win[0].shape[0])], axis=0)
    own, theirs = (
        jnp.concatenate([part[at : at + rows, :] for at in range(i * rows, part.shape[0], 4 * rows)], axis=1)
        for part in (win[0], win[1].at[: win[0].shape[0]])
    )
    above = place[4] == 0
    return jnp.concatenate([jnp.where(above, own, theirs), jnp.where(above, theirs, own)], axis=0)


def two_steps(q, step_depth):
    return stepped(stepped(q, step_depth), step_depth)


def ahead_body(slots, rows, place, *rest):
    *win, out = rest
    step_depth = HALF * window_field(win, 0, rows, place)
    q = tuple(window_field(win, 1 + f, rows, place) for f in range(3))
    for _ in range(slots):
        q = two_steps(q, step_depth)
    for f in range(3):
        out[f] = q[f]


def total_body(spaces, rows, width, reach, place, recv, ahead, *rest):
    *win, total_out = rest
    slots = recv.shape[0] // spaces
    step_depth = HALF * window_field(win, 0, rows, place)
    q = joined(recv, 0, spaces, rows, width, reach)
    for slot in range(1, slots):
        b = joined(recv, slot, spaces, rows, width, reach)
        q = tuple(x + y for x, y in zip(b, two_steps(q, step_depth)))
    q = tuple(x + ahead[f] for f, x in enumerate(q))
    all_rows = rows * spaces
    if not dense(width, reach, rows):
        for f in range(3):
            total_out[f * all_rows : (f + 1) * all_rows, :] = q[f]
        return
    small = lax.broadcasted_iota(jnp.int32, (TILE, LANES), 1)
    parts = width // LANES
    for f in range(3):
        for t in range(parts):
            total_out[(f * parts + t) * all_rows : (f * parts + t + 1) * all_rows, :] = q[f][
                :, t * LANES : (t + 1) * LANES
            ]
        put_halo(q[f][:, width:], f * all_rows // TILE, 3 * parts * all_rows, small, total_out)


def chain_body(spaces, rows, width, reach, place, recv, carry, *rest):
    *win, msg_far, msg_out, sems = rest
    slots = recv.shape[0] // spaces
    all_rows = rows * spaces
    copies = []
    step_depth = HALF * window_field(win, 0, rows, place)
    lower = place[1] == 1
    q = tuple(
        jnp.where(lower, window_field(win, 1 + f, rows, place), block_of(carry, f, all_rows, width, reach))
        for f in range(3)
    )
    for slot in range(slots):
        for y in range(spaces):
            at = slot * spaces + y
            for f in range(3):
                here = q[f][:, :width]
                lo, hi = y * rows, (y + 1) * rows
                msg_out[at, f * rows : (f + 1) * rows, :] = here[lo:hi]
                for r, source in enumerate((hi, hi + 1, lo - 2, lo - 1)):
                    source %= all_rows
                    to = 3 * rows + 4 * f + r
                    msg_out[at, to : to + 1, :] = here[source : source + 1]
            msg_out[at, 3 * rows + 12 :, :] = jnp.zeros((4, width), jnp.float32)
            copies.append(pltpu.make_async_copy(msg_out.at[at], msg_far.at[at], sems.at[at]))
            copies[-1].start()
        if slot + 1 < slots:
            b = joined(recv, slot, spaces, rows, width, reach)
            q = tuple(x + y for x, y in zip(b, two_steps(q, step_depth)))
    for copy in copies:
        copy.wait()


def finish_body(near, place, *refs):
    if near:
        mine, b_far, b_lent, v_far, depth_ref, out, state, b_own, v_ref, made, sems = refs
        other = None
    else:
        mine, other, b_far, b_lent, v_far, depth_ref, _, out, state, b_own, v_ref, made, sems = refs
    rows = v_ref.shape[1]
    wide = rows + TILE
    half = depth_ref.shape[1] // 2
    ours, theirs = place[2] * half, (1 - place[2]) * half
    side = 2 * LANES
    if near:
        parts = [(ours, half, mine, 0)]
        pieces = [(LANES, half - 2 * LANES, ours + LANES)]
    else:
        parts = [(ours + half - side, side, mine, half - side), (theirs, half, other, 0), (ours, side, mine, 0)]
        pieces = [(LANES, LANES, ours + half - LANES), (side, half, theirs), (side + half, LANES, ours)]

    def at(start, size):
        return pl.ds(pl.multiple_of(start, LANES), size)

    fetches, local = [], 0
    for i, (start, size, source, first) in enumerate(parts):
        width = source.shape[2]
        here = slice(local, local + size)
        for k, (far, held) in enumerate(((b_far, b_own), (v_far, v_ref))):
            copy = pltpu.make_async_copy(far.at[:, :, at(start, size)], held.at[:, :, here], sems.at[2 * i + k])
            copy.start()
            fetches.append(copy)
        step = min(width, size)
        for c in range(0, size, step):
            j, off = (first + c) // width, (first + c) % width
            to = slice(local + c, local + c + step)
            for f in range(3):
                state[f, :rows, to] = source[j, f * rows : (f + 1) * rows, off : off + step]
                for r, row in enumerate((rows, rows + 1, wide - 2, wide - 1)):
                    line = 3 * rows + 4 * f + r
                    state[f, row : row + 1, to] = source[j, line : line + 1, off : off + step]
        local += size
    for f in range(3):
        state[f, rows + 2 : wide - 2, :] = jnp.zeros((TILE - 4, local), jnp.float32)

    def taken(ref, lead):
        return jnp.concatenate([cut(ref, lead, start, size) for start, size, _, _ in parts], axis=1)

    even = place[2] == 0
    step_depth = DT * taken(depth_ref, ())
    carried = tuple(state[f] for f in range(3))
    moved = stepped(carried, step_depth)
    for fetch in fetches:
        fetch.wait()
    after = tuple(jnp.where(even, b_own[f], taken(b_lent, (f,))) + x for f, x in enumerate(moved))
    last = stepped(after, step_depth)
    copies = []
    for f in range(3):
        begin = jnp.where(even, carried[f][:rows], after[f][:rows])
        end = jnp.where(even, after[f][:rows], b_own[f, :rows, :] + last[f][:rows])
        made[0, f] = begin
        made[1, f] = 0.5 * ((begin + end) - v_ref[f])
        made[2, f] = end
        for part in range(3):
            for i, (lo, size, to) in enumerate(pieces):
                copy = pltpu.make_async_copy(
                    made.at[part, f, :, lo : lo + size],
                    out.at[part, f, :, at(to, size)],
                    sems.at[6 + (3 * f + part) * 3 + i],
                )
                copy.start()
                copies.append(copy)
    for copy in copies:
        copy.wait()


def kernel(body, shapes, *args, scalars=0, far=(), far_out=(), near=(), near_out=(), **more):
    vmem = pl.BlockSpec(memory_space=pltpu.VMEM)
    hbm = pl.BlockSpec(memory_space=pltpu.HBM)
    smem = pl.BlockSpec(memory_space=pltpu.SMEM)
    many = isinstance(shapes, list)
    outs = []
    for i, shape in enumerate(shapes if many else [shapes]):
        make = pltpu.HBM if i in far_out else pltpu.VMEM if i in near_out else jax.ShapeDtypeStruct
        outs.append(make(shape, jnp.float32))
    placed = list(args)
    for held, space in ((far, pltpu.HBM), (near, pltpu.VMEM)):
        for i in held:
            placed[i] = pltpu.with_memory_space_constraint(args[i], space)
    specs = [hbm if i in far_out else vmem for i in range(len(outs))]
    return pl.pallas_call(
        body,
        out_shape=outs if many else outs[0],
        in_specs=[smem if i < scalars else hbm if i in far else vmem for i in range(len(args))],
        out_specs=specs if many else specs[0],
        compiler_params=pltpu.CompilerParams(vmem_limit_bytes=VMEM_BYTES),
        **more,
    )(*placed)


def swap_rows(edges):
    count = lax.axis_size("space")
    if count == 2:
        return (lax.ppermute(edges, "space", [(0, 1), (1, 0)]),)
    below = lax.ppermute(edges[0], "space", [((i + 1) % count, i) for i in range(count)])
    above = lax.ppermute(edges[1], "space", [(i, (i + 1) % count) for i in range(count)])
    return below, above


def per_device(fine_nodes, init_state, mean_depth):
    nodes = fine_nodes[0]
    rows, cols = nodes.shape[-2:]
    outer, inner, spaces = lax.axis_size("outer"), lax.axis_size("inner"), lax.axis_size("space")
    group = ("inner", "space")
    owners = inner * spaces
    half = cols // 2
    width = half // owners
    slices = outer * inner * 2
    reach = slices - 2
    span = -(-(width + 2 * reach) // LANES) * LANES
    wide = rows + TILE
    at_outer, at_inner, at_core, at_space = (
        lax.axis_index(name) for name in ("outer", "inner", "core", "space")
    )
    first = at_outer + at_inner + at_core == 0
    place = jnp.stack([first.astype(jnp.int32), (at_outer == 0).astype(jnp.int32), at_core, at_inner, at_space])
    state, spread = (3, rows, cols), (3, wide, cols)
    swapped = [(0, 1), (1, 0)]
    plan = (spaces, rows, width, reach)

    onward = [(i, i + 1) for i in range(slices - 1)]
    last_shapes = [(3, rows, half + 2 * LANES), (3, rows, half)]
    paired = spaces == 2 and dense(width, reach, rows)
    if paired:
        own_rows = 4 * rows * span // LANES
        soon, late, own, edges = kernel(
            functools.partial(begin_body, width, reach),
            last_shapes + [(own_rows, LANES), (own_rows + 2 * DEEP * cols // LANES, LANES)],
            place, nodes, mean_depth, init_state, scalars=1, far=(1, 2, 3),
            scratch_shapes=[
                pltpu.VMEM((rows, cols), jnp.float32),
                pltpu.VMEM((2, 4, rows, width + 2 * LANES), jnp.float32),
                pltpu.SemaphoreType.DMA((25,)),
                pltpu.SemaphoreType.DMA((4,)),
            ],
        )
    else:
        soon, late = kernel(
            last_body, last_shapes, place, nodes, scalars=1, far=(1,),
            scratch_shapes=[pltpu.SemaphoreType.DMA((4,))],
        )
    prev = lax.ppermute(soon, ("outer", "inner", "core"), onward)
    prev_late = lax.ppermute(late, ("outer", "inner", "core"), onward)
    if paired:
        edges = lax.ppermute(edges, "space", swapped)
        windows, edges = (own, edges), (edges,)
    else:
        windows = all_windows(mean_depth, init_state, at_core * half, at_inner, spaces, width, reach, span)
        windows = (lax.all_to_all(windows, "space", 0, 0, tiled=True),)
        edges = jnp.stack([mean_depth[:DEEP, None], mean_depth[rows - DEEP :, None]])
        edges = swap_rows(edges)

    base, fk, bare = kernel(
        blend_body, [state, spread, (wide, cols)], nodes, mean_depth, far=(0, 1),
        scratch_shapes=[
            pltpu.VMEM(spread, jnp.float32),
            pltpu.VMEM((3,) + state, jnp.float32),
            pltpu.VMEM((rows, cols), jnp.float32),
            pltpu.SemaphoreType.DMA((4,)),
        ],
    )
    ffk, depth = kernel(second_body, [spread, (wide, cols)], fk, bare, *edges)
    fine_shapes = [(3 * wide, half + 2 * LANES), (3 * wide, half)]
    fine_args = (place, base, init_state, fk, ffk, depth, prev)
    give, v_give = kernel(functools.partial(fine_body, False), fine_shapes, *fine_args, scalars=1)
    got = lax.ppermute(give, "core", swapped)
    keep, v_keep = kernel(functools.partial(fine_body, True), fine_shapes, *fine_args, prev_late, scalars=1)
    tight = packed_rows(wide, width, reach)
    msg_shape = (owners, tight, LANES) if tight else (owners, 3 * wide, span)
    msgs, v_keep, v_give = kernel(
        functools.partial(pair_body, width, reach), [msg_shape, v_keep.shape, v_give.shape],
        place, depth, got, keep, v_keep, v_give, scalars=1, far_out=(0, 1, 2),
        scratch_shapes=[pltpu.VMEM(msg_shape, jnp.float32), pltpu.SemaphoreType.DMA((3,))],
    )
    recv = lax.all_to_all(msgs, group, 0, 0, tiled=True)
    spill, keep, give = kernel(
        spill_body, [(2, 2, 18, 1, half), keep.shape, give.shape], keep, give, v_keep, v_give,
        far=(2, 3), far_out=(1, 2),
        scratch_shapes=[pltpu.VMEM((2, 3, TILE, half), jnp.float32), pltpu.SemaphoreType.DMA((8,))],
    )
    far_parts = (keep, give, v_keep, v_give)
    ahead = kernel(
        functools.partial(ahead_body, inner, rows), (3, spaces * rows, span),
        place, *windows, scalars=1,
    )
    spill = swap_rows(spill)
    b_own, vee = kernel(
        mend_body, [spread, state], place, *far_parts, *spill, scalars=1,
        far=range(1, 5), far_out=(1,),
        scratch_shapes=[pltpu.VMEM(state, jnp.float32)]
        + [pltpu.VMEM(x.shape, jnp.float32) for x in far_parts]
        + [pltpu.SemaphoreType.DMA((5,))],
    )
    b_lent = lax.ppermute(b_own, "core", [(0, 1)])

    tight = packed_rows(spaces * rows, width, reach)
    total_shape = (tight, LANES) if tight else (3 * spaces * rows, span)
    total = kernel(functools.partial(total_body, *plan), total_shape, place, recv, ahead, *windows, scalars=1)
    carry = lax.ppermute(total, "outer", [(i, i + 1) for i in range(outer - 1)])
    back = kernel(
        functools.partial(chain_body, *plan), (owners, 3 * rows + 2 * TILE, width),
        place, recv, carry, *windows, scalars=1, far_out=(0,),
        scratch_shapes=[
            pltpu.VMEM((owners, 3 * rows + 2 * TILE, width), jnp.float32),
            pltpu.SemaphoreType.DMA((owners,)),
        ],
    )
    mine = lax.all_to_all(back, group, 0, 0, tiled=True)
    if width % LANES:
        mine = mine.transpose(1, 0, 2).reshape(1, 3 * rows + 2 * TILE, half)
    other = lax.ppermute(mine, "core", swapped)

    def finish(near, cols_held, *args, **more):
        held = (3, wide, cols_held)
        return kernel(
            functools.partial(finish_body, near), (3,) + state,
            place, *args, scalars=1, far_out=(0,),
            scratch_shapes=[
                pltpu.VMEM(held, jnp.float32),
                pltpu.VMEM(held, jnp.float32),
                pltpu.VMEM((3, rows, cols_held), jnp.float32),
                pltpu.VMEM((3, 3, rows, cols_held), jnp.float32),
                pltpu.SemaphoreType.DMA((33,)),
            ],
            **more,
        )

    out = finish(True, half, mine, b_own, b_lent, vee, depth, far=(2, 4))
    out = finish(
        False, half + 4 * LANES, mine, other, b_own, b_lent, vee, depth, out,
        far=(3, 5, 7), input_output_aliases={7: 0},
    )
    return out[None]


def all_windows(depth, init, offset, at_inner, spaces, width, reach, span):
    fixed = jnp.concatenate([depth[None], init], axis=0)
    _, rows, cols = fixed.shape
    onward = jnp.concatenate([fixed, fixed[..., :span]], axis=-1)
    behind = jnp.concatenate([fixed[..., cols - span :], fixed], axis=-1)
    lane = lax.broadcasted_iota(jnp.int32, (4, rows, span), 2)
    windows = []
    for y in range(spaces):
        start = offset + (at_inner * spaces + y) * width
        ahead = lax.dynamic_slice_in_dim(onward, start, span, axis=2)
        back = lax.dynamic_slice_in_dim(behind, start, span, axis=2)
        windows.append(jnp.where(lane < span - reach, ahead, back).reshape(4 * rows, span))
    return jnp.stack(windows)


def solution(mesh):
    slices, spaces = mesh.shape["tm"], mesh.shape["space"]
    split = Mesh(mesh.devices.reshape(2, slices // 4, 2, spaces), ("outer", "inner", "core", "space"))
    nodes = P(("outer", "inner", "core"), None, None, "space", None)
    return jax.shard_map(
        per_device,
        mesh=split,
        in_specs=(nodes, P(None, "space", None), P("space", None)),
        out_specs=nodes,
        check_vma=False,
    )
```
